32 devices in a mesh: section: 2 (over core), expert: 16 (over z, y, x).
Axes of the slice: x: 2, y: 2, z: 4, core: 2. Of those that a mesh axis runs over, the one named last changes fastest.
Arguments:
- grad_out: bfloat16 [2, 2048, 4096], P('section', 'expert'), may hold values from -6 to 6
- saved_hidden: bfloat16 [2, 2048, 8, 1024], P('section', 'expert'), may hold values from -6 to 6
- routes: int32 [2, 2048, 8], P('section', 'expert'), may hold values from 0 to 15, all different within a row; in each aligned block of 128 rows (0 to 127, 128 to 255, ..., all dimensions but the last counted through in order) at most 96 rows name the same one
- scores: float32 [2, 2048, 8], P('section', 'expert'), may hold values from 0.02 to 0.98
- down_weight: bfloat16 [2, 16, 1024, 4096], P('section', 'expert'), may hold values from -0.1875 to 0.1875
- router: bfloat16 [2, 16, 4096], P('section'), may hold values from -0.59765625 to 0.59765625
Outputs:
- weight_grad: bfloat16 [2, 16, 1024, 4096], P('section', 'expert')
- handed: bfloat16 [2, 2048, 4096], P('section', 'expert')
The draws below stay inside these ranges and needn't reach their ends.
Inputs may be any that keep to these rules, and one draw needn't show every extreme that they name: `routes`: each token names 8 different experts. Among the 128 tokens of one index of expert (aligned blocks), no expert is named more than 96 times, and in every draw some expert is named exactly 96 times in some block.
All inputs are finite; a program needn't handle non-finite values.
Results may differ from the reference program's by a relative error of at most 0.007.
Values may be sent and summed in bfloat16 or wider, within the bound.
A program may use at most 128 MiB of HBM per device.

```python
import math
import jax
import jax.numpy as jnp
import numpy as np
from jax import lax

D = 4096
FF = 1024
TOP = 8
TOK_DEV = 128
SECTIONS = 2
EXPERTS = 16
TOKENS = 2048
CAP = 96


def levels(stream_key, dims, shards, smallest, high):
    gain, own = 1.0, jax.random.fold_in(stream_key, 6)
    for axis_at, shards_of in shards:
        heights = jnp.exp(jax.random.uniform(jax.random.fold_in(own, axis_at), (shards_of,), jnp.float32, smallest / len(shards), high / len(shards)))
        gain = gain * jnp.repeat(heights, dims[axis_at] // shards_of).reshape([-1 if axis == axis_at else 1 for axis in range(len(dims))])
    return gain


def deal_out(stream_key, own, number, rows, amount, top, bound, skew):
    sequence = jax.random.permutation(stream_key, amount)
    packed, ordinary = load_shares(amount, rows * top, bound, skew, True), load_shares(amount, rows * top, bound, skew, False)
    places = jnp.arange(amount)

    def named(lengths, offset_by):
        used = int((lengths > 0).sum())
        fixed = max(1, used // 4)
        moved = fixed + (places - fixed + offset_by * (used - fixed)) % max(1, amount - fixed)
        return jnp.zeros((amount,), jnp.int32).at[sequence[jnp.where(places < fixed, places, moved)]].set(jnp.asarray(lengths, jnp.int32))

    lengths = jnp.where(number % 4 == 0, named(packed, number // 4), named(ordinary, number - number // 4 - 1))
    mixed = jax.random.permutation(jax.random.fold_in(own, 3), amount)
    source_of, sink = mixed[0:amount // 2 * 2:2], mixed[1:amount // 2 * 2:2]
    room = jnp.minimum(lengths[source_of] - 1, bound - lengths[sink]) // 2
    room = jnp.where((source_of == sequence[0]) | (sink == sequence[0]) | (lengths[sink] == 0), 0, jnp.maximum(room, 0))
    moved = jax.random.randint(jax.random.fold_in(own, 4), (amount // 2,), 0, 1 << 20) % (room + 1)
    lengths = lengths.at[source_of].add(-moved).at[sink].add(moved)
    items = jnp.searchsorted(jnp.cumsum(lengths), jnp.arange(rows * top), side="right").astype(jnp.int32)
    table = items.reshape(top, rows).T
    table = table[jax.random.permutation(jax.random.fold_in(own, 1), rows)]
    offset_by = jax.random.randint(jax.random.fold_in(own, 2), (rows, 1), 0, top)
    return jnp.take_along_axis(table, (jnp.arange(top)[None, :] + offset_by) % top, axis=1)


def load_shares(count, total, most, slope, full):
    portions = [(1 << 20) // math.isqrt(grade ** slope) + 1 for grade in range(1, count + 1)]
    largest = most if full else min(most, max(-(-total // count), total * portions[0] // sum(portions)))
    least = 1 if total - largest >= count - 1 else 0
    holding, rest = [largest] + [least] * (count - 1), total - largest - least * (count - 1)
    while rest > 0:
        free = [i for i in range(1, count) if holding[i] < largest] or [i for i in range(1, count) if holding[i] < most]
        mass, budget = sum([portions[i] for i in free]), rest
        for i in free:
            extra = min(most - holding[i], max(1, budget * portions[i] // mass), rest)
            holding[i] = holding[i] + extra
            rest = rest - extra
    return np.array(holding)


def centred(own_key, extent, width, most, shards=(), kind=jnp.bfloat16):
    result = jax.random.normal(own_key, extent, jnp.float32) * width
    if len(shards) > 0:
        result = levels(own_key, extent, shards, -0.22, 0.18) * result
    return jnp.clip(result, min=-most, max=most).astype(kind)


def setup_inputs(seed: int = 0) -> dict:
    key_of = jax.random.split(jax.random.key(seed), 7)
    grad_out = centred(key_of[0], (SECTIONS, TOKENS, D), 1.0, 6.0, ((0, 2), (1, 16)))
    saved_hidden = centred(key_of[1], (SECTIONS, TOKENS, TOP, FF), 1.0, 6.0, ((0, 2), (1, 16)))
    routes_keys = jax.random.split(jax.random.fold_in(key_of[2], 1), SECTIONS * TOKENS // TOK_DEV)
    routes_turns = jax.random.permutation(jax.random.fold_in(key_of[2], 3), SECTIONS * TOKENS // TOK_DEV)
    routes = jax.vmap(lambda own, number: deal_out(jax.random.fold_in(key_of[2], 2), own, number, TOK_DEV, EXPERTS, TOP, CAP, 2))(routes_keys, routes_turns).reshape((SECTIONS, TOKENS, TOP))
    scores = jnp.clip(0.02 + 0.96000002 * jax.random.uniform(key_of[3], (SECTIONS, TOKENS, TOP), jnp.float32) ** levels(key_of[3], (SECTIONS, TOKENS, TOP), ((0, 2), (1, 16)), -0.2, 0.2), 0.02, 0.98)
    down_weight = centred(key_of[4], (SECTIONS, EXPERTS, FF, D), FF ** -0.5, 0.1875, ((0, 2), (1, 16)))
    router = centred(key_of[5], (SECTIONS, EXPERTS, D), 0.1, 0.59765625, ((0, 2),))
    return dict(grad_out=grad_out, saved_hidden=saved_hidden, routes=routes, scores=scores, down_weight=down_weight, router=router)


def slot_rows(route_ids, n_experts, per_block, capacity):
    flat_routes = route_ids.reshape(-1)
    entries = flat_routes.shape[0]
    n_blocks = entries // per_block
    onehot = (flat_routes[:, None] == jnp.arange(n_experts, dtype=jnp.int32)[None, :]).astype(jnp.int32)
    running = jnp.cumsum(onehot.reshape(n_blocks, per_block, n_experts), axis=1).astype(jnp.int32)
    running = running.reshape(entries, n_experts)
    slot_index = jnp.sum(running * onehot, axis=1).astype(jnp.int32) - 1
    block_index = jnp.arange(entries, dtype=jnp.int32) // per_block
    row_index = (block_index * capacity + slot_index).astype(jnp.int32)
    source = jnp.full((n_experts, n_blocks * capacity), entries, jnp.int32)
    source = source.at[flat_routes, row_index].set(jnp.arange(entries, dtype=jnp.int32))
    return flat_routes, row_index, source


def section_pass(grad_rows, hidden_rows, route_ids, score_rows, down_all, router_rows):
    n_tokens, n_routes = route_ids.shape
    n_experts = router_rows.shape[0]
    entries = n_tokens * n_routes
    flat_routes, row_index, source = slot_rows(route_ids, n_experts, TOK_DEV * n_routes, CAP)
    score_total = jnp.sum(score_rows, axis=1, keepdims=True)
    weights = score_rows / score_total
    weights_low = weights.astype(jnp.bfloat16).reshape(-1)
    hidden_flat = hidden_rows.reshape(entries, hidden_rows.shape[2])

    def one_expert(operands):
        slot_source, expert_down = operands
        filled = slot_source < entries
        safe_index = jnp.minimum(slot_source, entries - 1)
        grad_in = jnp.where(filled[:, None], grad_rows[safe_index // n_routes], jnp.zeros((), jnp.bfloat16))
        hidden_in = jnp.where(filled[:, None], hidden_flat[safe_index], jnp.zeros((), jnp.bfloat16))
        weight_in = jnp.where(filled, weights_low[safe_index], jnp.zeros((), jnp.bfloat16))
        projected = lax.dot_general(grad_in, expert_down, (((1,), (1,)), ((), ())), preferred_element_type=jnp.float32)
        derivs = jnp.sum(projected * hidden_in.astype(jnp.float32), axis=1)
        scaled = (weight_in.astype(jnp.float32)[:, None] * grad_in.astype(jnp.float32)).astype(jnp.bfloat16)
        weight_grads = lax.dot_general(hidden_in, scaled, (((0,), (0,)), ((), ())), preferred_element_type=jnp.float32)
        return weight_grads.astype(jnp.bfloat16), derivs

    weight_grads, derivs = lax.map(one_expert, (source, down_all))
    derivs_home = derivs[flat_routes, row_index].reshape(n_tokens, n_routes)
    center = jnp.sum(weights * derivs_home, axis=1, keepdims=True)
    logit_grad = score_rows * (1.0 - score_rows) / score_total * (derivs_home - center)
    expert_ids = jnp.arange(n_experts, dtype=jnp.int32)
    dense_grad = jnp.sum(jnp.where(route_ids[:, :, None] == expert_ids[None, None, :], logit_grad[:, :, None], 0.0), axis=1)
    input_grad = grad_rows.astype(jnp.float32) + jnp.dot(dense_grad, router_rows.astype(jnp.float32), precision=lax.Precision.HIGHEST)
    return weight_grads, input_grad.astype(jnp.bfloat16)


def reference(grad_out, saved_hidden, routes, scores, down_weight, router):
    weight_list = []
    input_list = []
    for section_index in range(SECTIONS):
        weight_grads, input_grad = section_pass(grad_out[section_index], saved_hidden[section_index], routes[section_index], scores[section_index], down_weight[section_index], router[section_index])
        weight_list.append(weight_grads)
        input_list.append(input_grad)
    handed = jnp.roll(jnp.stack(input_list), -1, axis=0)
    return jnp.stack(weight_list), handed
```

```python
import functools

import jax
import jax.numpy as jnp
from jax import lax
from jax.experimental import pallas as pl
from jax.experimental.pallas import tpu as pltpu
from jax.sharding import PartitionSpec as P

MESH = pl.DeviceIdType.MESH


def torus_dims(n):
    dims = [1, 1, 1]
    at = 0
    while n > 1:
        factor = next(f for f in range(2, n + 1) if n % f == 0)
        dims[at % 3] *= factor
        n //= factor
        at += 1
    return tuple(dims)


def tree_edges(dims, order, flip):
    reached = [(0, 0, 0)]
    edges = []
    for axis in order:
        size = dims[axis]
        fresh = []
        for count, start in enumerate(reached):
            extra = (count + flip) % 2 if size % 2 == 0 else 0
            plus = (size - 1) // 2 + (1 - extra if size > 2 and size % 2 == 0 else 0)
            if size == 2:
                plus = 1
            minus = size - 1 - plus
            for step, hops in ((1, plus), (-1, minus)):
                place = start
                for _ in range(hops):
                    after = list(place)
                    after[axis] = (after[axis] + step) % size
                    after = tuple(after)
                    edges.append((place, axis, step, after))
                    fresh.append(after)
                    place = after
        reached = reached + fresh
    return edges


def plan(dims, orders):
    waiting = []
    for chunk, (order, flip) in enumerate(orders):
        edges = tree_edges(dims, order, flip)
        below = {}
        for parent, axis, step, child in reversed(edges):
            below[parent] = max(below.get(parent, 0), below.get(child, 0) + 1)
        for parent, axis, step, child in edges:
            waiting.append((chunk, parent, axis, step, child, below.get(child, 0)))
    arrival = {(chunk, (0, 0, 0)): 0 for chunk in range(len(orders))}
    free = {}
    issued = []
    while waiting:
        best = None
        for item in waiting:
            chunk, parent, axis, step, child, depth = item
            if (chunk, parent) not in arrival:
                continue
            begin = max(arrival[(chunk, parent)], free.get((axis, step), 0))
            key = (begin, -depth, chunk)
            if best is None or key < best[0]:
                best = (key, item)
        (begin, _, _), item = best
        waiting.remove(item)
        chunk, parent, axis, step, child, depth = item
        free[(axis, step)] = begin + 1
        arrival[(chunk, child)] = begin + 1.5
        issued.append((begin, item[:5]))
    issued.sort(key=lambda pair: pair[0])
    return [item for _, item in issued]


def flat(offset, dims):
    return (offset[0] * dims[1] + offset[1]) * dims[2] + offset[2]


def exchange_kernel(dims, sends, grad_ref, dense_ref, all_ref, got_ref, own, own_dense, g_send, g_recv, h_send, h_recv, local):
    n = dims[0] * dims[1] * dims[2]
    me = lax.axis_index("expert")
    here = (me // (dims[1] * dims[2]), (me // dims[2]) % dims[1], me % dims[2])

    def at(offset, sign):
        c = [(here[i] + sign * offset[i] + dims[i]) % dims[i] for i in range(3)]
        return (c[0] * dims[1] + c[1]) * dims[2] + c[2]

    load = pltpu.make_async_copy(grad_ref, own, local.at[0])
    load.start()
    load_dense = pltpu.make_async_copy(dense_ref.at[me], own_dense, local.at[1])
    load_dense.start()
    barrier = pltpu.get_barrier_semaphore()
    for i in range(1, n):
        pl.semaphore_signal(barrier, inc=1, device_id={"expert": (me + i) % n}, device_id_type=MESH)
    pl.semaphore_wait(barrier, n - 1)
    load.wait()

    offsets = [(a, b, c) for a in range(dims[0]) for b in range(dims[1]) for c in range(dims[2])]
    offsets = [o for o in offsets if o != (0, 0, 0)]

    def dense_copy(offset):
        k = flat(offset, dims)
        return pltpu.make_async_remote_copy(
            src_ref=dense_ref.at[at(offset, 1)],
            dst_ref=got_ref.at[me],
            send_sem=h_send.at[k],
            recv_sem=h_recv.at[k],
            device_id={"expert": at(offset, 1)},
            device_id_type=MESH,
        )

    def grad_copy(item):
        chunk, parent, axis, step, child = item
        source = at(parent, -1)
        move = [0, 0, 0]
        move[axis] = step
        k = flat(child, dims)
        return pltpu.make_async_remote_copy(
            src_ref=own.at[chunk] if parent == (0, 0, 0) else all_ref.at[source, chunk],
            dst_ref=all_ref.at[source, chunk],
            send_sem=g_send.at[k, chunk],
            recv_sem=g_recv.at[k, chunk],
            device_id={"expert": at(move, 1)},
            device_id_type=MESH,
        )

    def arrived(chunk, offset):
        k = flat(offset, dims)
        source = at(offset, -1)
        pltpu.make_async_copy(all_ref.at[source, chunk], all_ref.at[source, chunk], g_recv.at[k, chunk]).wait()

    seen = set()
    pending = list(offsets)
    copies = []
    dense_copies = []
    stores = []
    own_sends = sum(1 for item in sends if item[1] == (0, 0, 0))
    every = max(1, (len(sends) * 2 // 3 - own_sends) // max(1, len(pending)))
    for count, item in enumerate(sends):
        chunk, parent = item[0], item[1]
        if parent != (0, 0, 0) and (chunk, parent) not in seen:
            arrived(chunk, parent)
            seen.add((chunk, parent))
        copy = grad_copy(item)
        copy.start()
        copies.append(copy)
        if count >= own_sends and (count - own_sends) % every == 0 and pending:
            extra = dense_copy(pending.pop(0))
            extra.start()
            dense_copies.append(extra)
        if count == own_sends:
            store = pltpu.make_async_copy(own, all_ref.at[me], local.at[2])
            store.start()
            load_dense.wait()
            store_dense = pltpu.make_async_copy(own_dense, got_ref.at[me], local.at[3])
            store_dense.start()
            stores = [store, store_dense]
    for offset in pending:
        extra = dense_copy(offset)
        extra.start()
        dense_copies.append(extra)
    for offset in offsets:
        for chunk in range(own.shape[0]):
            if (chunk, offset) not in seen:
                arrived(chunk, offset)
    for copy in dense_copies:
        copy.wait_recv()
    for copy in dense_copies:
        copy.wait_send()
    for copy in copies:
        copy.wait_send()
    for store in stores:
        store.wait()


def line_kernel(dims, orders, grad_ref, dense_ref, all_ref, got_ref, own, own_dense, g_send, g_recv, h_send, h_recv, local):
    n = dims[0] * dims[1] * dims[2]
    chunks = len(orders)
    me = lax.axis_index("expert")
    here = [me // (dims[1] * dims[2]), (me // dims[2]) % dims[1], me % dims[2]]

    def number(c):
        return (c[0] * dims[1] + c[1]) * dims[2] + c[2]

    load = pltpu.make_async_copy(grad_ref, own, local.at[0])
    load.start()
    load_dense = pltpu.make_async_copy(dense_ref.at[me], own_dense, local.at[1])
    load_dense.start()
    barrier = pltpu.get_barrier_semaphore()
    for i in range(1, n):
        pl.semaphore_signal(barrier, inc=1, device_id={"expert": (me + i) % n}, device_id_type=MESH)
    pl.semaphore_wait(barrier, n - 1)
    load.wait()

    def start(source, chunk, axis, step, home):
        target = list(here)
        target[axis] = (here[axis] + step) % dims[axis]
        pltpu.make_async_remote_copy(
            src_ref=own.at[chunk] if home else all_ref.at[source, chunk],
            dst_ref=all_ref.at[source, chunk],
            send_sem=g_send.at[source, chunk, axis, (step + 1) // 2],
            recv_sem=g_recv.at[source, chunk],
            device_id={"expert": number(target)},
            device_id_type=MESH,
        ).start()

    def finish(source, chunk, axis, step, home):
        piece = own.at[chunk] if home else all_ref.at[source, chunk]
        pltpu.make_async_copy(piece, piece, g_send.at[source, chunk, axis, (step + 1) // 2]).wait()

    def moves(offset, order):
        last = max([i for i in range(3) if offset[order[i]] != 0], default=-1)
        steps = []
        if last >= 0 and dims[order[last]] > 2:
            steps.append((order[last], 1 if offset[order[last]] > 0 else -1))
        for axis in order[last + 1 :]:
            if dims[axis] == 2:
                steps.append((axis, 1))
            elif dims[axis] > 2:
                steps += [(axis, 1), (axis, -1)]
        return steps

    def each_move(offset, order, chunk, act):
        source = number([(here[i] - offset[i] + dims[i]) % dims[i] for i in range(3)])
        home = offset == (0, 0, 0)
        for axis, step in moves(offset, order):
            if dims[axis] == 2:
                act(source, chunk, axis, step, home)
            else:
                inside = here[axis] < dims[axis] - 1 if step > 0 else here[axis] > 0
                pl.when(inside)(functools.partial(act, source, chunk, axis, step, home))

    def on_slice(offset, act):
        valid = None
        for i in range(3):
            if dims[i] > 2 and offset[i] != 0:
                inside = here[i] >= offset[i] if offset[i] > 0 else here[i] < dims[i] + offset[i]
                valid = inside if valid is None else valid & inside
        if valid is None:
            act()
        else:
            pl.when(valid)(act)

    spans = [range(size) if size <= 2 else range(1 - size, size) for size in dims]
    offsets = [(a, b, c) for a in spans[0] for b in spans[1] for c in spans[2] if (a, b, c) != (0, 0, 0)]

    for chunk in range(chunks):
        each_move((0, 0, 0), orders[chunk], chunk, start)

    def dense_copy(k):
        return pltpu.make_async_remote_copy(
            src_ref=dense_ref.at[(me + k) % n],
            dst_ref=got_ref.at[me],
            send_sem=h_send.at[k],
            recv_sem=h_recv.at[k],
            device_id={"expert": (me + k) % n},
            device_id_type=MESH,
        )

    store = pltpu.make_async_copy(own, all_ref.at[me], local.at[2])
    store.start()
    load_dense.wait()
    store_dense = pltpu.make_async_copy(own_dense, got_ref.at[me], local.at[3])
    store_dense.start()

    arrivals = []
    for chunk in range(chunks):
        for offset in offsets:
            hops = [abs(offset[axis]) for axis in orders[chunk]]
            arrivals.append((hops[0] * WEIGHTS[0] + hops[1] * WEIGHTS[1] + hops[2] * WEIGHTS[2], chunk, offset))
    arrivals.sort()
    far = sorted(range(1, n), key=lambda k: -min(k, n - k))
    every = max(1, (len(arrivals) * SHARE // 4) // len(far))
    for count, (_, chunk, offset) in enumerate(arrivals):
        if count % every == 0 and far:
            dense_copy(far.pop(0)).start()

        def arrive(chunk=chunk, offset=offset):
            source = number([(here[i] - offset[i] + dims[i]) % dims[i] for i in range(3)])
            piece = all_ref.at[source, chunk]
            pltpu.make_async_copy(piece, piece, g_recv.at[source, chunk]).wait()
            each_move(offset, orders[chunk], chunk, start)

        on_slice(offset, arrive)
    for k in far:
        dense_copy(k).start()
    for k in range(1, n):
        dense_copy(k).wait()
    for chunk in range(chunks):
        each_move((0, 0, 0), orders[chunk], chunk, finish)
        for offset in offsets:
            if moves(offset, orders[chunk]):
                on_slice(offset, functools.partial(each_move, offset, orders[chunk], chunk, finish))
    store.wait()
    store_dense.wait()


WEIGHTS = (2, 3, 3)
SHARE = 3
LINE_ORDERS = ((0, 2, 1), (0, 1, 2), (0, 2, 1), (0, 1, 2))


def exchange(grad_rows, dense):
    n, n_tokens, hidden_width = dense.shape
    width = grad_rows.shape[1]
    dims = torus_dims(n)
    on_line = 2 in dims
    orders = [((2, 1, 0), 0), ((1, 2, 0), 1), ((0, 2, 1), 0), ((0, 1, 2), 1)]
    if on_line:
        kernel, chunks = functools.partial(line_kernel, dims, LINE_ORDERS), len(LINE_ORDERS)
    else:
        kernel, chunks = functools.partial(exchange_kernel, dims, plan(dims, orders)), len(orders)
    rows = n_tokens // chunks
    grad_chunks = grad_rows.reshape(chunks, rows, width)
    got, dense_got = pl.pallas_call(
        kernel,
        out_shape=(
            jax.ShapeDtypeStruct((n, chunks, rows, width), grad_rows.dtype),
            jax.ShapeDtypeStruct(dense.shape, dense.dtype),
        ),
        in_specs=[pl.BlockSpec(memory_space=pl.ANY)] * 2,
        out_specs=(pl.BlockSpec(memory_space=pl.ANY), pl.BlockSpec(memory_space=pl.ANY)),
        scratch_shapes=[
            pltpu.VMEM((chunks, rows, width), grad_rows.dtype),
            pltpu.VMEM((n_tokens, hidden_width), dense.dtype),
            pltpu.SemaphoreType.DMA((n, chunks, 3, 2) if on_line else (n, chunks)),
            pltpu.SemaphoreType.DMA((n, chunks)),
            pltpu.SemaphoreType.DMA((n,)),
            pltpu.SemaphoreType.DMA((n,)),
            pltpu.SemaphoreType.DMA((4,)),
        ],
        compiler_params=pltpu.CompilerParams(collective_id=0, has_side_effects=True),
        name="exchange",
    )(grad_chunks, dense)
    return got.reshape(n * n_tokens, width), dense_got.reshape(n * n_tokens, hidden_width)


def spread_kernel(n_experts, group, top, hidden_ref, weight_ref, route_ref, out_ref):
    rows, cols = n_experts * group, group * top
    row = lax.broadcasted_iota(jnp.int32, (rows, cols), 0)
    col = lax.broadcasted_iota(jnp.int32, (rows, cols), 1)
    named = (row % group == col // top) & (row // group == route_ref[0])
    mix = jnp.where(named, weight_ref[0], 0.0).astype(jnp.bfloat16)
    for e in range(n_experts):
        part = jnp.dot(
            mix[e * group : (e + 1) * group], hidden_ref[...], preferred_element_type=jnp.float32
        )
        out_ref[e] = part.astype(jnp.bfloat16)


def spread(hidden_rows, weights_low, route_ids, n_experts):
    n_tokens, top, width = hidden_rows.shape
    group = 16
    steps = n_tokens // group
    cols = group * top
    return pl.pallas_call(
        functools.partial(spread_kernel, n_experts, group, top),
        grid=(steps,),
        out_shape=jax.ShapeDtypeStruct((n_experts, n_tokens, width), jnp.bfloat16),
        in_specs=[
            pl.BlockSpec((cols, width), lambda i: (i, 0)),
            pl.BlockSpec((1, 1, cols), lambda i: (i, 0, 0)),
            pl.BlockSpec((1, 1, cols), lambda i: (i, 0, 0)),
        ],
        out_specs=pl.BlockSpec((n_experts, group, width), lambda i: (0, i, 0)),
        name="spread",
    )(
        hidden_rows.reshape(n_tokens * top, width),
        weights_low.astype(jnp.float32).reshape(steps, 1, cols),
        route_ids.reshape(steps, 1, cols),
    )


def deriv_kernel(grad_ref, hidden_ref, down_ref, out_ref):
    projected = lax.dot_general(
        grad_ref[...], down_ref[...], (((1,), (1,)), ((), ())), preferred_element_type=jnp.float32
    )
    out_ref[...] = jnp.sum(projected * hidden_ref[...].astype(jnp.float32), axis=1, keepdims=True)


def derivs_of(grads, hidden, down):
    rows, width = grads.shape
    hidden_width = hidden.shape[1]
    tile = 512
    return pl.pallas_call(
        deriv_kernel,
        grid=(rows // tile,),
        out_shape=jax.ShapeDtypeStruct((rows, 1), jnp.float32),
        in_specs=[
            pl.BlockSpec((tile, width), lambda i: (i, 0)),
            pl.BlockSpec((tile, hidden_width), lambda i: (i, 0)),
            pl.BlockSpec((hidden_width, width), lambda i: (0, 0)),
        ],
        out_specs=pl.BlockSpec((tile, 1), lambda i: (i, 0)),
        compiler_params=pltpu.CompilerParams(vmem_limit_bytes=50 * 1024 * 1024),
        cost_estimate=pl.CostEstimate(
            flops=2 * rows * width * hidden_width, bytes_accessed=2 * rows * width, transcendentals=0
        ),
        name="derivs",
    )(grads, hidden, down)


OWN, ROWS, GET = 0, 1, 2
SPREAD, KEEP, DERIVE, PRODUCT = 0, 1, 2, 3
SHAPE = (4, 2, 2)
ORDERS = ((0, 2, 1), (2, 0, 1), (0, 1, 2), (1, 0, 2))
WIDTHS = (1, 1, 1, 1)
GROUPS = (
    ((0, 0), (0, 1), (1, 0), (2, 0), (1, 1), (2, 1), (3, 0), (3, 1)),
    ((1, 0), (0, 0), (1, 1), (2, 0), (0, 1), (2, 1), (3, 0), (3, 1)),
)
WORK = (
    (SPREAD,),
    (KEEP,),
    (DERIVE, 0),
    (DERIVE, 1),
    (DERIVE, 2),
    (DERIVE, 3),
    (DERIVE, 4),
    (DERIVE, 5),
    (DERIVE, 6),
    (PRODUCT, 0),
    (DERIVE, 7),
    (PRODUCT, 1),
    (PRODUCT, 2),
    (PRODUCT, 3),
    (PRODUCT, 4),
    (PRODUCT, 5),
    (PRODUCT, 6),
    (PRODUCT, 7),
    (PRODUCT, 8),
    (PRODUCT, 9),
    (PRODUCT, 10),
    (PRODUCT, 11),
    (PRODUCT, 12),
    (PRODUCT, 13),
    (PRODUCT, 14),
    (PRODUCT, 15),
)
SCHEDULE = (
    (
        (
            (OWN, 0, 0, 1),
            (OWN, 0, 2, 1),
            (OWN, 0, 1, 1),
            (OWN, 1, 2, 1),
            (OWN, 1, 0, 1),
            (OWN, 1, 1, 1),
            (OWN, 2, 0, 1),
            (OWN, 2, 1, 1),
            (OWN, 2, 2, 1),
            (OWN, 3, 1, 1),
            (OWN, 3, 0, 1),
            (OWN, 3, 2, 1),
        ),
        (
            (GET, 0, 0, 1, 0),
            (GET, 0, 1, 0, 0),
            (GET, 1, 0, 0, 0),
        ),
        (
            (ROWS, 0, 1, 0),
            (GET, 0, 0, 1, 1),
            (GET, 0, 1, 0, 1),
            (GET, 1, 0, 0, 1),
            (ROWS, 0, 0, 1),
            (GET, 0, 0, 1, 2),
            (GET, 0, 1, 0, 2),
            (GET, 1, 0, 0, 2),
            (ROWS, 0, 1, 1),
            (GET, 0, 0, 1, 3),
            (GET, 0, 1, 0, 3),
            (GET, 1, 0, 0, 3),
            (ROWS, 1, 0, 0),
            (GET, 1, 0, 1, 0),
            (GET, 0, 1, 1, 0),
            (GET, 2, 0, 0, 0),
            (ROWS, 1, 1, 0),
            (GET, 1, 1, 0, 0),
            (GET, 1, 0, 1, 1),
            (GET, 0, 1, 1, 2),
        ),
        (
            (GET, 2, 0, 0, 1),
            (ROWS, 1, 0, 1),
            (GET, 1, 0, 1, 2),
            (GET, 0, 1, 1, 1),
            (GET, 2, 0, 0, 2),
            (ROWS, 1, 1, 1),
            (GET, 1, 1, 0, 3),
            (ROWS, 2, 0, 0),
            (GET, 1, 1, 0, 1),
            (GET, 2, 0, 0, 3),
            (GET, 0, 1, 1, 3),
            (ROWS, 2, 1, 0),
            (GET, 1, 1, 0, 2),
            (GET, 1, 0, 1, 3),
            (ROWS, 2, 0, 1),
            (GET, 1, 1, 1, 0),
            (GET, 3, 0, 0, 0),
            (GET, 2, 0, 1, 0),
            (ROWS, 2, 1, 1),
            (GET, 2, 1, 0, 0),
            (GET, 2, 0, 1, 1),
            (GET, 2, 0, 1, 2),
            (GET, 1, 1, 1, 1),
            (ROWS, 3, 0, 0),
            (GET, 3, 0, 0, 1),
        ),
        (
            (GET, 1, 1, 1, 3),
            (ROWS, 3, 1, 0),
            (GET, 2, 1, 0, 1),
            (GET, 2, 0, 1, 3),
            (ROWS, 3, 0, 1),
            (GET, 1, 1, 1, 2),
            (GET, 2, 1, 0, 2),
            (GET, 3, 0, 0, 2),
            (ROWS, 3, 1, 1),
            (GET, 3, 0, 1, 0),
            (GET, 3, 1, 0, 0),
            (GET, 2, 1, 0, 3),
            (GET, 2, 1, 1, 0),
        ),
        (
            (GET, 2, 1, 1, 2),
            (GET, 2, 1, 1, 1),
            (GET, 3, 0, 1, 2),
            (GET, 3, 1, 0, 1),
            (GET, 2, 1, 1, 3),
            (GET, 3, 0, 0, 3),
            (GET, 3, 1, 0, 2),
            (GET, 3, 0, 1, 3),
            (GET, 3, 1, 1, 0),
            (GET, 3, 0, 1, 1),
            (GET, 3, 1, 1, 2),
        ),
        (),
        (
            (GET, 3, 1, 1, 1),
        ),
        (
            (GET, 3, 1, 0, 3),
        ),
        (),
        (
            (GET, 3, 1, 1, 3),
        ),
        (),
        (),
        (),
        (),
        (),
        (),
        (),
        (),
        (),
        (),
        (),
        (),
        (),
        (),
        (),
    ),
    (
        (
            (OWN, 0, 0, 1),
            (OWN, 0, 0, -1),
            (OWN, 0, 2, 1),
            (OWN, 0, 1, 1),
            (OWN, 1, 2, 1),
            (OWN, 1, 0, 1),
            (OWN, 1, 0, -1),
            (OWN, 1, 1, 1),
            (OWN, 2, 0, 1),
            (OWN, 2, 0, -1),
            (OWN, 2, 1, 1),
            (OWN, 2, 2, 1),
            (OWN, 3, 1, 1),
            (OWN, 3, 0, 1),
            (OWN, 3, 0, -1),
            (OWN, 3, 2, 1),
        ),
        (
            (GET, 0, 0, 0, 0),
            (GET, 1, 0, 1, 0),
            (GET, 1, 1, 0, 0),
            (GET, 2, 0, 0, 0),
        ),
        (
            (ROWS, 1, 1, 0),
            (GET, 0, 0, 0, 1),
            (GET, 1, 0, 1, 1),
            (GET, 1, 1, 0, 1),
            (GET, 2, 0, 0, 1),
            (ROWS, 1, 0, 1),
            (GET, 0, 0, 0, 2),
            (GET, 1, 0, 1, 2),
            (GET, 1, 1, 0, 2),
            (GET, 2, 0, 0, 2),
            (ROWS, 1, 1, 1),
            (GET, 0, 0, 0, 3),
            (GET, 1, 0, 1, 3),
            (GET, 1, 1, 0, 3),
            (GET, 2, 0, 0, 3),
            (ROWS, 0, 0, 0),
            (GET, 0, 0, 1, 1),
            (GET, 0, 0, 1, 0),
            (GET, 0, 1, 0, 0),
            (GET, 3, 0, 0, 0),
            (ROWS, 2, 0, 0),
            (GET, 0, 1, 0, 3),
            (GET, 2, 0, 1, 0),
            (GET, 1, 1, 1, 0),
            (GET, 2, 0, 1, 1),
        ),
        (
            (GET, 3, 0, 0, 1),
            (ROWS, 0, 1, 0),
            (GET, 2, 1, 0, 0),
            (GET, 0, 0, 1, 2),
            (GET, 3, 0, 0, 2),
            (ROWS, 2, 1, 0),
            (GET, 2, 1, 0, 3),
            (ROWS, 0, 0, 1),
            (GET, 1, 1, 1, 2),
            (GET, 0, 1, 0, 1),
            (GET, 3, 0, 0, 3),
            (ROWS, 2, 0, 1),
            (GET, 3, 0, 1, 1),
            (GET, 2, 0, 1, 2),
            (GET, 1, 1, 1, 1),
            (ROWS, 0, 1, 1),
            (ROWS, 2, 1, 1),
            (GET, 2, 1, 0, 1),
            (ROWS, 3, 0, 0),
            (GET, 0, 0, 1, 3),
        ),
        (
            (GET, 3, 1, 0, 3),
            (ROWS, 3, 1, 0),
            (GET, 1, 1, 1, 3),
            (GET, 0, 1, 0, 2),
            (ROWS, 3, 0, 1),
            (GET, 2, 1, 0, 2),
            (ROWS, 3, 1, 1),
            (GET, 2, 0, 1, 3),
            (GET, 0, 1, 1, 1),
        ),
        (
            (GET, 3, 0, 1, 0),
            (GET, 0, 1, 1, 0),
            (GET, 0, 1, 1, 3),
            (GET, 3, 1, 0, 0),
            (GET, 3, 0, 1, 2),
            (GET, 2, 1, 1, 0),
            (GET, 2, 1, 1, 3),
            (GET, 2, 1, 1, 1),
            (GET, 3, 0, 1, 3),
            (GET, 3, 1, 0, 1),
            (GET, 3, 1, 1, 3),
            (GET, 3, 1, 0, 2),
            (GET, 0, 1, 1, 2),
            (GET, 3, 1, 1, 1),
        ),
        (
            (GET, 2, 1, 1, 2),
            (GET, 3, 1, 1, 0),
        ),
        (
            (GET, 3, 1, 1, 2),
        ),
        (),
        (),
        (),
        (),
        (),
        (),
        (),
        (),
        (),
        (),
        (),
        (),
        (),
        (),
        (),
        (),
        (),
        (),
    ),
)

def near_index(z, y, x, dims):
    return (z * dims[1] + y) * dims[2] + x


def onward(dims, here, source, order):
    offset = [here[i] - source[i] for i in range(3)]
    last = max([i for i in range(3) if offset[order[i]] != 0], default=-1)
    steps = []
    if last >= 0 and order[last] == 0:
        steps.append((0, 1 if offset[0] > 0 else -1))
    for axis in order[last + 1 :]:
        steps += [(axis, 1), (axis, -1)] if axis == 0 else [(axis, 1)]
    return [(a, d) for a, d in steps if a != 0 or 0 <= here[0] + d < dims[0]]


def relay_kernel(
    dims, cap, top, grad_ref, hidden_ref, slots_ref, meta_ref, stats_ref, down_ref, router_ref,
    part_ref, ht_ref, far_ref, logit_ref, next_ref, next_router_ref,
    gall, hid, down, hsend, hgot, mgot, ht, stage, dsend, home, logit,
    g_send, g_recv, h_send, h_recv, m_send, m_recv, d_send, d_recv, s_send, s_recv, local,
):
    n = dims[0] * dims[1] * dims[2]
    rows = grad_ref.shape[0]
    width = grad_ref.shape[1]
    hidden_width = hid.shape[1]
    cols = hid.shape[0]
    me = lax.axis_index("expert")
    section = lax.axis_index("section")
    z, y, x = me // (dims[1] * dims[2]), (me // dims[2]) % dims[1], me % dims[2]
    lower = z < dims[0] // 2
    at_end = (z == 0) | (z == dims[0] - 1)
    sign = jnp.where(lower, 1, -1)
    pair = dims[2] * rows

    load = pltpu.make_async_copy(grad_ref, gall.at[pl.ds(me * rows, rows)], local.at[0])
    load.start()
    load_hidden = pltpu.make_async_copy(hidden_ref, hid, local.at[1])
    load_hidden.start()
    load_down = pltpu.make_async_copy(down_ref, down, local.at[2])
    load_down.start()

    barrier = pltpu.get_barrier_semaphore()
    for i in range(1, n):
        pl.semaphore_signal(barrier, inc=1, device_id={"expert": (me + i) % n}, device_id_type=MESH)
    pl.semaphore_signal(barrier, inc=1, device_id={"section": 1 - section}, device_id_type=MESH)
    pl.semaphore_wait(barrier, n)
    load.wait()

    def plane(mirrored):
        return jnp.where(lower, mirrored, dims[0] - 1 - mirrored)

    def number(rel):
        return near_index(plane(rel[0]), (y + rel[1]) % 2, (x + rel[2]) % 2, dims)

    def piece(source, chunk):
        begin = sum(WIDTHS[:chunk]) * width // sum(WIDTHS)
        size = WIDTHS[chunk] * width // sum(WIDTHS)
        return gall.at[pl.ds(source * rows, rows), pl.ds(begin, size)]

    def grad_copy(source, chunk, axis, step):
        target = [z, y, x]
        target[axis] = z + step * sign if axis == 0 else (target[axis] + 1) % 2
        block = piece(source, chunk)
        return pltpu.make_async_remote_copy(
            src_ref=block,
            dst_ref=block,
            send_sem=g_send.at[source, chunk, axis, (step + 1) // 2],
            recv_sem=g_recv.at[source, chunk],
            device_id={"expert": near_index(*target, dims)},
            device_id_type=MESH,
        )

    def hidden_copy(k):
        return pltpu.make_async_remote_copy(
            src_ref=hsend.at[pl.ds(k * cap, cap)],
            dst_ref=hgot.at[me],
            send_sem=h_send.at[k],
            recv_sem=h_recv.at[me],
            device_id={"expert": k},
            device_id_type=MESH,
        )

    def meta_copy(k):
        return pltpu.make_async_remote_copy(
            src_ref=meta_ref.at[k],
            dst_ref=mgot.at[me],
            send_sem=m_send.at[k],
            recv_sem=m_recv.at[me],
            device_id={"expert": k},
            device_id_type=MESH,
        )

    def home_copy(k):
        return pltpu.make_async_remote_copy(
            src_ref=dsend.at[k],
            dst_ref=home.at[me],
            send_sem=d_send.at[k],
            recv_sem=d_recv.at[me],
            device_id={"expert": k},
            device_id_type=MESH,
        )

    def beside(src, dst, k):
        return pltpu.make_async_remote_copy(
            src_ref=src,
            dst_ref=dst,
            send_sem=s_send.at[k],
            recv_sem=s_recv.at[k],
            device_id={"section": 1 - section},
            device_id_type=MESH,
        )

    mine = gall.at[pl.ds(me * rows, rows)]

    def issue(kind, event):
        here = (kind, 0, 0)
        if event[0] == OWN:
            grad_copy(me, event[1], event[2], event[3]).start()
        elif event[0] == ROWS:
            hidden_copy(number(event[1:])).start()
        else:
            source, chunk = number(event[1:4]), event[4]
            block = piece(source, chunk)
            pltpu.make_async_copy(block, block, g_recv.at[source, chunk]).wait()
            for axis, step in onward(dims, here, event[1:4], ORDERS[chunk]):
                grad_copy(source, chunk, axis, step).start()

    def events(segment):
        for kind in range(2):
            if SCHEDULE[kind][segment]:

                @pl.when(at_end if kind == 0 else jnp.logical_not(at_end))
                def _(kind=kind):
                    for event in SCHEDULE[kind][segment]:
                        issue(kind, event)

    def spread_rows():
        load_hidden.wait()
        expand = jnp.where(
            lax.broadcasted_iota(jnp.int32, (rows, cols), 1) // top
            == lax.broadcasted_iota(jnp.int32, (rows, cols), 0),
            1.0,
            0.0,
        ).astype(jnp.bfloat16)
        wide = jnp.dot(slots_ref[...].astype(jnp.bfloat16), expand, preferred_element_type=jnp.float32)
        lane = lax.broadcasted_iota(jnp.int32, (top, cols), 1) % top
        own = lane == lax.broadcasted_iota(jnp.int32, (top, cols), 0)
        slot = jnp.sum(jnp.where(own, wide[:top], 0.0), axis=0, keepdims=True)
        route = jnp.sum(jnp.where(own, wide[top:], 0.0), axis=0, keepdims=True)
        place = (route * cap + slot).astype(jnp.int32)
        block = 256 if (n * cap) % 256 == 0 else cap

        def one(b, _):
            begin = pl.multiple_of(b * block, block)
            want = lax.broadcasted_iota(jnp.int32, (block, cols), 0) + begin
            pick = jnp.where(want == place, 1.0, 0.0).astype(jnp.bfloat16)
            part = jnp.dot(pick, hid[...], preferred_element_type=jnp.float32)
            hsend[pl.ds(begin, block), :] = part.astype(jnp.bfloat16)
            return 0

        lax.fori_loop(0, n * cap // block, one, 0)

    def keep_own():
        own = pltpu.make_async_copy(hsend.at[pl.ds(me * cap, cap)], hgot.at[me], local.at[3])
        own.start()
        own.wait()

    def group_base(group):
        table = GROUPS[0][group], GROUPS[1][group]
        zm = jnp.where(at_end, table[0][0], table[1][0])
        dy = jnp.where(at_end, table[0][1], table[1][1])
        zz = jnp.where(lower, zm, dims[0] - 1 - zm)
        return near_index(zz, (y + dy) % 2, 0, dims)

    def derive(group):
        first = group_base(group)
        for j in range(dims[2]):
            source = first + j

            @pl.when(source != me)
            def _(source=source):
                pltpu.make_async_copy(hgot.at[source], hgot.at[source], h_recv.at[source]).wait()
                pltpu.make_async_copy(mgot.at[source], mgot.at[source], m_recv.at[source]).wait()

            @pl.when(source == me)
            def _():
                mgot[me] = meta_ref[me]

            info = mgot[source]
            want = lax.broadcasted_iota(jnp.int32, (cap, rows), 0).astype(jnp.float32)
            pick = jnp.where(want == info[0:1], info[1:2], 0.0).astype(jnp.bfloat16)
            full = lax.dot_general(
                hgot[source], pick, (((0,), (0,)), ((), ())), preferred_element_type=jnp.float32
            )
            ht[:, pl.ds(pl.multiple_of(source * rows, rows), rows)] = full.astype(jnp.bfloat16)
        begin = pl.multiple_of(first * rows, pair)
        block = 256

        def one(m, total):
            at = pl.multiple_of(m * block, block)
            projected = lax.dot_general(
                down[pl.ds(at, block), :],
                gall[pl.ds(begin, pair), :],
                (((1,), (1,)), ((), ())),
                preferred_element_type=jnp.float32,
            )
            held = ht[pl.ds(at, block), pl.ds(begin, pair)].astype(jnp.float32)
            return total + jnp.sum(projected * held, axis=0, keepdims=True)

        total = lax.fori_loop(0, hidden_width // block, one, jnp.zeros((1, pair), jnp.float32))
        for j in range(dims[2]):
            dsend[first + j] = total[:, j * rows : (j + 1) * rows]

            @pl.when(first + j == me)
            def _(j=j):
                home[me] = total[:, j * rows : (j + 1) * rows]

    def send_home(group):
        first = group_base(group)
        for j in range(dims[2]):

            @pl.when(first + j != me)
            def _(source=first + j):
                home_copy(source).start()

    most = (dims[0] - 1) * dims[1] * pair
    begin_most = pl.multiple_of(jnp.where(lower, 0, dims[1] * pair), pair)
    tile = stage.shape[2]

    def part_copy(step):
        return pltpu.make_async_copy(
            stage.at[step % 2], part_ref.at[:, pl.ds(step * tile, tile)], local.at[4 + step % 2]
        )

    def product(step):
        if step >= 2:
            part_copy(step - 2).wait()
        stage[step % 2] = jnp.dot(
            ht[:, pl.ds(begin_most, most)],
            gall[pl.ds(begin_most, most), pl.ds(step * tile, tile)],
            preferred_element_type=jnp.float32,
        )
        part_copy(step).start()

    beside(mine, next_ref, 0).start()
    beside(router_ref, next_router_ref, 1).start()
    late = None
    for segment, op in enumerate(WORK):
        events(segment)
        if late is not None:
            send_home(late)
            late = None
        if op[0] == SPREAD:
            for i in range(1, n):
                meta_copy((me + i) % n).start()
            spread_rows()
        elif op[0] == KEEP:
            keep_own()
            load_down.wait()
        elif op[0] == DERIVE:
            derive(op[1])
            late = op[1]
        elif op[0] == PRODUCT:
            product(op[1])
    last = pl.multiple_of(jnp.where(lower, (dims[0] - 1) * dims[1] * pair, 0), pair)
    far = dims[1] * pair
    keep_grad = pltpu.make_async_copy(gall.at[pl.ds(last, far)], far_ref, local.at[6])
    keep_grad.start()
    keep_hidden = pltpu.make_async_copy(ht.at[:, pl.ds(last, far)], ht_ref, local.at[7])
    keep_hidden.start()
    if late is not None:
        send_home(late)

    for i in range(1, n):
        source = (me + i) % n
        pltpu.make_async_copy(home.at[source], home.at[source], d_recv.at[source]).wait()
    score = stats_ref[0:n]
    fix = stats_ref[n : 2 * n]
    ratio = stats_ref[2 * n : 3 * n]
    weighted = home[:, 0, :] * fix
    center = jnp.sum(weighted, axis=0, keepdims=True)
    logit[...] = (1.0 - score) * (weighted - ratio * center)
    keep_grad.wait()
    keep_hidden.wait()
    steps = width // tile
    for step in range(max(0, steps - 2), steps):
        part_copy(step).wait()
    give = beside(logit, logit_ref, 2)
    give.start()
    for i in range(1, n):
        k = (me + i) % n
        hidden_copy(k).wait_send()
        meta_copy(k).wait_send()
        home_copy(k).wait_send()
    for kind in range(2):

        @pl.when(at_end if kind == 0 else jnp.logical_not(at_end))
        def _(kind=kind):
            for segment in SCHEDULE[kind]:
                for event in segment:
                    if event[0] == OWN:
                        grad_copy(me, event[1], event[2], event[3]).wait_send()
                    elif event[0] != ROWS:
                        for axis, step in onward(dims, (kind, 0, 0), event[1:4], ORDERS[event[4]]):
                            grad_copy(number(event[1:4]), event[4], axis, step).wait_send()

    beside(mine, next_ref, 0).wait()
    beside(router_ref, next_router_ref, 1).wait()
    give.wait()


def relay(grad_rows, hidden_rows, slots, meta, stats, down, router_rows, cap):
    n = meta.shape[0]
    n_tokens, width = grad_rows.shape
    top = slots.shape[0] // 2
    entries, hidden_width = hidden_rows.shape
    dims = torus_dims(n)
    far = n_tokens * dims[1] * dims[2]
    low = jnp.bfloat16
    any_space = pl.BlockSpec(memory_space=pl.ANY)
    vmem = pl.BlockSpec(memory_space=pltpu.VMEM)
    dma = pltpu.SemaphoreType.DMA
    return pl.pallas_call(
        functools.partial(relay_kernel, dims, cap, top),
        out_shape=(
            jax.ShapeDtypeStruct((hidden_width, width), jnp.float32),
            jax.ShapeDtypeStruct((hidden_width, far), low),
            jax.ShapeDtypeStruct((far, width), low),
            jax.ShapeDtypeStruct((n, n_tokens), jnp.float32),
            jax.ShapeDtypeStruct((n_tokens, width), low),
            jax.ShapeDtypeStruct(router_rows.shape, low),
        ),
        in_specs=[any_space, any_space, vmem, vmem, vmem, any_space, any_space],
        out_specs=(any_space,) * 6,
        scratch_shapes=[
            pltpu.VMEM((n * n_tokens, width), low),
            pltpu.VMEM((entries, hidden_width), low),
            pltpu.VMEM((hidden_width, width), low),
            pltpu.VMEM((n * cap, hidden_width), low),
            pltpu.VMEM((n, cap, hidden_width), low),
            pltpu.VMEM(meta.shape, jnp.float32),
            pltpu.VMEM((hidden_width, n * n_tokens), low),
            pltpu.VMEM((2, hidden_width, 256), jnp.float32),
            pltpu.VMEM((n, 1, n_tokens), jnp.float32),
            pltpu.VMEM((n, 1, n_tokens), jnp.float32),
            pltpu.VMEM((n, n_tokens), jnp.float32),
            dma((n, len(ORDERS), 3, 2)),
            dma((n, len(ORDERS))),
            dma((n,)),
            dma((n,)),
            dma((n,)),
            dma((n,)),
            dma((n,)),
            dma((n,)),
            dma((3,)),
            dma((3,)),
            dma((8,)),
        ],
        compiler_params=pltpu.CompilerParams(
            collective_id=1, has_side_effects=True, vmem_limit_bytes=60 * 1024 * 1024
        ),
        name="relay",
    )(grad_rows, hidden_rows, slots, meta, stats, down, router_rows)


def finish_kernel(part_ref, ht_ref, far_ref, logit_ref, next_ref, router_ref, weight_ref, handed_ref):
    weight_ref[...] = (
        part_ref[...] + jnp.dot(ht_ref[...], far_ref[...], preferred_element_type=jnp.float32)
    ).astype(weight_ref.dtype)
    extra = lax.dot_general(
        logit_ref[...],
        router_ref[...].astype(jnp.float32),
        (((0,), (0,)), ((), ())),
        precision=lax.Precision.HIGHEST,
        preferred_element_type=jnp.float32,
    )
    handed_ref[...] = (next_ref[...].astype(jnp.float32) + extra).astype(handed_ref.dtype)


def finish(part, ht, far, logit, next_grad, next_router):
    hidden_width, width = part.shape
    tile = 512
    whole = lambda a: pl.BlockSpec(a.shape, lambda i: (0, 0))
    column = lambda a: pl.BlockSpec((a.shape[0], tile), lambda i: (0, i))
    return pl.pallas_call(
        finish_kernel,
        grid=(width // tile,),
        out_shape=(
            jax.ShapeDtypeStruct(part.shape, jnp.bfloat16),
            jax.ShapeDtypeStruct(next_grad.shape, jnp.bfloat16),
        ),
        in_specs=[column(part), whole(ht), column(far), whole(logit), column(next_grad), column(next_router)],
        out_specs=(column(part), column(next_grad)),
        compiler_params=pltpu.CompilerParams(vmem_limit_bytes=50 * 1024 * 1024),
        name="finish",
    )(part, ht, far, logit, next_grad, next_router)


def close_body(grad_out, saved_hidden, routes, scores, down_weight, router):
    grad_rows = grad_out[0]
    hidden_rows = saved_hidden[0]
    n_tokens, top, hidden_width = hidden_rows.shape
    n = router.shape[1]
    cap = 3 * n_tokens * top // (2 * n)
    route_t = routes[0].T
    score_t = scores[0].T
    total = jnp.sum(score_t, axis=0, keepdims=True)
    named = route_t[None] == jnp.arange(n, dtype=jnp.int32)[:, None, None]
    score_dense = jnp.sum(jnp.where(named, score_t[None], 0.0), axis=1)
    is_named = jnp.any(named, axis=1)
    weights = score_t / total
    low_t = weights.astype(jnp.bfloat16).astype(jnp.float32)
    fix_dense = jnp.sum(jnp.where(named, (weights / low_t)[None], 0.0), axis=1)
    low_dense = jnp.sum(jnp.where(named, low_t[None], 0.0), axis=1)
    earlier = jnp.arange(n_tokens)[:, None] < jnp.arange(n_tokens)[None, :]
    rank = jnp.dot(
        is_named.astype(jnp.bfloat16), earlier.astype(jnp.bfloat16), preferred_element_type=jnp.float32
    )
    slot_dense = jnp.where(is_named, rank, -1.0)
    slot_t = jnp.sum(jnp.where(named, rank[:, None, :], 0.0), axis=0)
    slots = jnp.concatenate([slot_t, route_t.astype(jnp.float32)], axis=0)
    meta = jnp.stack([slot_dense, low_dense] + [jnp.zeros_like(rank)] * 6, axis=1)
    stats = jnp.concatenate([score_dense, fix_dense, score_dense / total], axis=0)
    part, ht, far, logit, next_grad, next_router = relay(
        grad_rows, hidden_rows.reshape(n_tokens * top, hidden_width), slots, meta, stats, down_weight[0, 0], router[0], cap
    )
    weight_out, handed = finish(part, ht, far, logit, next_grad, next_router)
    return (weight_out[None, None], handed[None])


def passed_along(array, axis, by):
    size = lax.axis_size(axis)
    return lax.ppermute(array, axis, [(i, (i + by) % size) for i in range(size)])


def body(grad_out, saved_hidden, routes, scores, down_weight, router):
    grad_rows = grad_out[0]
    hidden_rows = saved_hidden[0]
    route_ids = routes[0]
    score_rows = scores[0]
    n_tokens = grad_rows.shape[0]
    n_experts = router.shape[1]
    score_total = jnp.sum(score_rows, axis=1, keepdims=True)
    weights = score_rows / score_total
    weights_low = weights.astype(jnp.bfloat16)

    next_grad = passed_along(grad_rows, "section", -1)
    next_router = passed_along(router[0], "section", -1)
    dense = spread(hidden_rows, weights_low, route_ids, n_experts)
    grads, hidden = exchange(grad_rows, dense)
    derivs = derivs_of(grads, hidden, down_weight[0, 0])
    home = lax.all_to_all(
        derivs.reshape(n_experts, n_tokens), "expert", split_axis=0, concat_axis=0, tiled=True
    )
    weight_out = lax.dot_general(
        hidden, grads, (((0,), (0,)), ((), ())), preferred_element_type=jnp.float32
    ).astype(jnp.bfloat16)

    named = route_ids.T[None] == jnp.arange(n_experts, dtype=jnp.int32)[:, None, None]
    low = weights_low.astype(jnp.float32)
    score_dense = jnp.sum(jnp.where(named, score_rows.T[None], 0.0), axis=1)
    fix_dense = jnp.sum(jnp.where(named, (weights / low).T[None], 0.0), axis=1)
    weighted = home * fix_dense
    center = jnp.sum(weighted, axis=0, keepdims=True)
    total_row = score_total.T
    logit_dense = (1.0 - score_dense) * (weighted - score_dense / total_row * center)
    next_logit = passed_along(logit_dense, "section", -1)
    handed = next_grad.astype(jnp.float32) + lax.dot_general(
        next_logit,
        next_router.astype(jnp.float32),
        (((0,), (0,)), ((), ())),
        precision=lax.Precision.HIGHEST,
    )
    return (weight_out[None, None], handed.astype(jnp.bfloat16)[None])


def solution(mesh):
    close = mesh.shape["section"] == 2 and torus_dims(mesh.shape["expert"]) == SHAPE
    return jax.shard_map(
        close_body if close else body,
        mesh=mesh,
        in_specs=(
            P("section", "expert", None),
            P("section", "expert", None, None),
            P("section", "expert", None),
            P("section", "expert", None),
            P("section", "expert", None, None),
            P("section", None, None),
        ),
        out_specs=(P("section", "expert", None, None), P("section", "expert", None)),
        check_vma=False,
    )
```

```python
import functools

import jax
import jax.numpy as jnp
from jax import lax
from jax.experimental import pallas as pl
from jax.experimental.pallas import tpu as pltpu
from jax.sharding import PartitionSpec as P

MESH = pl.DeviceIdType.MESH


def torus_dims(n):
    dims = [1, 1, 1]
    at = 0
    while n > 1:
        factor = next(f for f in range(2, n + 1) if n % f == 0)
        dims[at % 3] *= factor
        n //= factor
        at += 1
    return tuple(dims)


def tree_edges(dims, order, flip):
    reached = [(0, 0, 0)]
    edges = []
    for axis in order:
        size = dims[axis]
        fresh = []
        for count, start in enumerate(reached):
            extra = (count + flip) % 2 if size % 2 == 0 else 0
            plus = (size - 1) // 2 + (1 - extra if size > 2 and size % 2 == 0 else 0)
            if size == 2:
                plus = 1
            minus = size - 1 - plus
            for step, hops in ((1, plus), (-1, minus)):
                place = start
                for _ in range(hops):
                    after = list(place)
                    after[axis] = (after[axis] + step) % size
                    after = tuple(after)
                    edges.append((place, axis, step, after))
                    fresh.append(after)
                    place = after
        reached = reached + fresh
    return edges


def plan(dims, orders):
    waiting = []
    for chunk, (order, flip) in enumerate(orders):
        edges = tree_edges(dims, order, flip)
        below = {}
        for parent, axis, step, child in reversed(edges):
            below[parent] = max(below.get(parent, 0), below.get(child, 0) + 1)
        for parent, axis, step, child in edges:
            waiting.append((chunk, parent, axis, step, child, below.get(child, 0)))
    arrival = {(chunk, (0, 0, 0)): 0 for chunk in range(len(orders))}
    free = {}
    issued = []
    while waiting:
        best = None
        for item in waiting:
            chunk, parent, axis, step, child, depth = item
            if (chunk, parent) not in arrival:
                continue
            begin = max(arrival[(chunk, parent)], free.get((axis, step), 0))
            key = (begin, -depth, chunk)
            if best is None or key < best[0]:
                best = (key, item)
        (begin, _, _), item = best
        waiting.remove(item)
        chunk, parent, axis, step, child, depth = item
        free[(axis, step)] = begin + 1
        arrival[(chunk, child)] = begin + 1.5
        issued.append((begin, item[:5]))
    issued.sort(key=lambda pair: pair[0])
    return [item for _, item in issued]


def flat(offset, dims):
    return (offset[0] * dims[1] + offset[1]) * dims[2] + offset[2]


def exchange_kernel(dims, sends, grad_ref, dense_ref, all_ref, got_ref, own, own_dense, g_send, g_recv, h_send, h_recv, local):
    n = dims[0] * dims[1] * dims[2]
    me = lax.axis_index("expert")
    here = (me // (dims[1] * dims[2]), (me // dims[2]) % dims[1], me % dims[2])

    def at(offset, sign):
        c = [(here[i] + sign * offset[i] + dims[i]) % dims[i] for i in range(3)]
        return (c[0] * dims[1] + c[1]) * dims[2] + c[2]

    load = pltpu.make_async_copy(grad_ref, own, local.at[0])
    load.start()
    load_dense = pltpu.make_async_copy(dense_ref.at[me], own_dense, local.at[1])
    load_dense.start()
    barrier = pltpu.get_barrier_semaphore()
    for i in range(1, n):
        pl.semaphore_signal(barrier, inc=1, device_id={"expert": (me + i) % n}, device_id_type=MESH)
    pl.semaphore_wait(barrier, n - 1)
    load.wait()

    offsets = [(a, b, c) for a in range(dims[0]) for b in range(dims[1]) for c in range(dims[2])]
    offsets = [o for o in offsets if o != (0, 0, 0)]

    def dense_copy(offset):
        k = flat(offset, dims)
        return pltpu.make_async_remote_copy(
            src_ref=dense_ref.at[at(offset, 1)],
            dst_ref=got_ref.at[me],
            send_sem=h_send.at[k],
            recv_sem=h_recv.at[k],
            device_id={"expert": at(offset, 1)},
            device_id_type=MESH,
        )

    def grad_copy(item):
        chunk, parent, axis, step, child = item
        source = at(parent, -1)
        move = [0, 0, 0]
        move[axis] = step
        k = flat(child, dims)
        return pltpu.make_async_remote_copy(
            src_ref=own.at[chunk] if parent == (0, 0, 0) else all_ref.at[source, chunk],
            dst_ref=all_ref.at[source, chunk],
            send_sem=g_send.at[k, chunk],
            recv_sem=g_recv.at[k, chunk],
            device_id={"expert": at(move, 1)},
            device_id_type=MESH,
        )

    def arrived(chunk, offset):
        k = flat(offset, dims)
        source = at(offset, -1)
        pltpu.make_async_copy(all_ref.at[source, chunk], all_ref.at[source, chunk], g_recv.at[k, chunk]).wait()

    seen = set()
    pending = list(offsets)
    copies = []
    dense_copies = []
    stores = []
    own_sends = sum(1 for item in sends if item[1] == (0, 0, 0))
    every = max(1, (len(sends) * 2 // 3 - own_sends) // max(1, len(pending)))
    for count, item in enumerate(sends):
        chunk, parent = item[0], item[1]
        if parent != (0, 0, 0) and (chunk, parent) not in seen:
            arrived(chunk, parent)
            seen.add((chunk, parent))
        copy = grad_copy(item)
        copy.start()
        copies.append(copy)
        if count >= own_sends and (count - own_sends) % every == 0 and pending:
            extra = dense_copy(pending.pop(0))
            extra.start()
            dense_copies.append(extra)
        if count == own_sends:
            store = pltpu.make_async_copy(own, all_ref.at[me], local.at[2])
            store.start()
            load_dense.wait()
            store_dense = pltpu.make_async_copy(own_dense, got_ref.at[me], local.at[3])
            store_dense.start()
            stores = [store, store_dense]
    for offset in pending:
        extra = dense_copy(offset)
        extra.start()
        dense_copies.append(extra)
    for offset in offsets:
        for chunk in range(own.shape[0]):
            if (chunk, offset) not in seen:
                arrived(chunk, offset)
    for copy in dense_copies:
        copy.wait_recv()
    for copy in dense_copies:
        copy.wait_send()
    for copy in copies:
        copy.wait_send()
    for store in stores:
        store.wait()


def line_kernel(dims, orders, grad_ref, dense_ref, all_ref, got_ref, own, own_dense, g_send, g_recv, h_send, h_recv, local):
    n = dims[0] * dims[1] * dims[2]
    chunks = len(orders)
    me = lax.axis_index("expert")
    here = [me // (dims[1] * dims[2]), (me // dims[2]) % dims[1], me % dims[2]]

    def number(c):
        return (c[0] * dims[1] + c[1]) * dims[2] + c[2]

    load = pltpu.make_async_copy(grad_ref, own, local.at[0])
    load.start()
    load_dense = pltpu.make_async_copy(dense_ref.at[me], own_dense, local.at[1])
    load_dense.start()
    barrier = pltpu.get_barrier_semaphore()
    for i in range(1, n):
        pl.semaphore_signal(barrier, inc=1, device_id={"expert": (me + i) % n}, device_id_type=MESH)
    pl.semaphore_wait(barrier, n - 1)
    load.wait()

    def start(source, chunk, axis, step, home):
        target = list(here)
        target[axis] = (here[axis] + step) % dims[axis]
        pltpu.make_async_remote_copy(
            src_ref=own.at[chunk] if home else all_ref.at[source, chunk],
            dst_ref=all_ref.at[source, chunk],
            send_sem=g_send.at[source, chunk, axis, (step + 1) // 2],
            recv_sem=g_recv.at[source, chunk],
            device_id={"expert": number(target)},
            device_id_type=MESH,
        ).start()

    def finish(source, chunk, axis, step, home):
        piece = own.at[chunk] if home else all_ref.at[source, chunk]
        pltpu.make_async_copy(piece, piece, g_send.at[source, chunk, axis, (step + 1) // 2]).wait()

    def moves(offset, order):
        last = max([i for i in range(3) if offset[order[i]] != 0], default=-1)
        steps = []
        if last >= 0 and dims[order[last]] > 2:
            steps.append((order[last], 1 if offset[order[last]] > 0 else -1))
        for axis in order[last + 1 :]:
            if dims[axis] == 2:
                steps.append((axis, 1))
            elif dims[axis] > 2:
                steps += [(axis, 1), (axis, -1)]
        return steps

    def each_move(offset, order, chunk, act):
        source = number([(here[i] - offset[i] + dims[i]) % dims[i] for i in range(3)])
        home = offset == (0, 0, 0)
        for axis, step in moves(offset, order):
            if dims[axis] == 2:
                act(source, chunk, axis, step, home)
            else:
                inside = here[axis] < dims[axis] - 1 if step > 0 else here[axis] > 0
                pl.when(inside)(functools.partial(act, source, chunk, axis, step, home))

    def on_slice(offset, act):
        valid = None
        for i in range(3):
            if dims[i] > 2 and offset[i] != 0:
                inside = here[i] >= offset[i] if offset[i] > 0 else here[i] < dims[i] + offset[i]
                valid = inside if valid is None else valid & inside
        if valid is None:
            act()
        else:
            pl.when(valid)(act)

    spans = [range(size) if size <= 2 else range(1 - size, size) for size in dims]
    offsets = [(a, b, c) for a in spans[0] for b in spans[1] for c in spans[2] if (a, b, c) != (0, 0, 0)]

    for chunk in range(chunks):
        each_move((0, 0, 0), orders[chunk], chunk, start)

    def dense_copy(k):
        return pltpu.make_async_remote_copy(
            src_ref=dense_ref.at[(me + k) % n],
            dst_ref=got_ref.at[me],
            send_sem=h_send.at[k],
            recv_sem=h_recv.at[k],
            device_id={"expert": (me + k) % n},
            device_id_type=MESH,
        )

    store = pltpu.make_async_copy(own, all_ref.at[me], local.at[2])
    store.start()
    load_dense.wait()
    store_dense = pltpu.make_async_copy(own_dense, got_ref.at[me], local.at[3])
    store_dense.start()

    arrivals = []
    for chunk in range(chunks):
        for offset in offsets:
            hops = [abs(offset[axis]) for axis in orders[chunk]]
            arrivals.append((hops[0] * WEIGHTS[0] + hops[1] * WEIGHTS[1] + hops[2] * WEIGHTS[2], chunk, offset))
    arrivals.sort()
    far = sorted(range(1, n), key=lambda k: -min(k, n - k))
    every = max(1, (len(arrivals) * SHARE // 4) // len(far))
    for count, (_, chunk, offset) in enumerate(arrivals):
        if count % every == 0 and far:
            dense_copy(far.pop(0)).start()

        def arrive(chunk=chunk, offset=offset):
            source = number([(here[i] - offset[i] + dims[i]) % dims[i] for i in range(3)])
            piece = all_ref.at[source, chunk]
            pltpu.make_async_copy(piece, piece, g_recv.at[source, chunk]).wait()
            each_move(offset, orders[chunk], chunk, start)

        on_slice(offset, arrive)
    for k in far:
        dense_copy(k).start()
    for k in range(1, n):
        dense_copy(k).wait()
    for chunk in range(chunks):
        each_move((0, 0, 0), orders[chunk], chunk, finish)
        for offset in offsets:
            if moves(offset, orders[chunk]):
                on_slice(offset, functools.partial(each_move, offset, orders[chunk], chunk, finish))
    store.wait()
    store_dense.wait()


WEIGHTS = (2, 3, 3)
SHARE = 3
LINE_ORDERS = ((0, 2, 1), (0, 1, 2), (0, 2, 1), (0, 1, 2))


def exchange(grad_rows, dense):
    n, n_tokens, hidden_width = dense.shape
    width = grad_rows.shape[1]
    dims = torus_dims(n)
    on_line = 2 in dims
    orders = [((2, 1, 0), 0), ((1, 2, 0), 1), ((0, 2, 1), 0), ((0, 1, 2), 1)]
    if on_line:
        kernel, chunks = functools.partial(line_kernel, dims, LINE_ORDERS), len(LINE_ORDERS)
    else:
        kernel, chunks = functools.partial(exchange_kernel, dims, plan(dims, orders)), len(orders)
    rows = n_tokens // chunks
    grad_chunks = grad_rows.reshape(chunks, rows, width)
    got, dense_got = pl.pallas_call(
        kernel,
        out_shape=(
            jax.ShapeDtypeStruct((n, chunks, rows, width), grad_rows.dtype),
            jax.ShapeDtypeStruct(dense.shape, dense.dtype),
        ),
        in_specs=[pl.BlockSpec(memory_space=pl.ANY)] * 2,
        out_specs=(pl.BlockSpec(memory_space=pl.ANY), pl.BlockSpec(memory_space=pl.ANY)),
        scratch_shapes=[
            pltpu.VMEM((chunks, rows, width), grad_rows.dtype),
            pltpu.VMEM((n_tokens, hidden_width), dense.dtype),
            pltpu.SemaphoreType.DMA((n, chunks, 3, 2) if on_line else (n, chunks)),
            pltpu.SemaphoreType.DMA((n, chunks)),
            pltpu.SemaphoreType.DMA((n,)),
            pltpu.SemaphoreType.DMA((n,)),
            pltpu.SemaphoreType.DMA((4,)),
        ],
        compiler_params=pltpu.CompilerParams(collective_id=0, has_side_effects=True),
        name="exchange",
    )(grad_chunks, dense)
    return got.reshape(n * n_tokens, width), dense_got.reshape(n * n_tokens, hidden_width)


def spread_kernel(n_experts, group, top, hidden_ref, weight_ref, route_ref, out_ref):
    rows, cols = n_experts * group, group * top
    row = lax.broadcasted_iota(jnp.int32, (rows, cols), 0)
    col = lax.broadcasted_iota(jnp.int32, (rows, cols), 1)
    named = (row % group == col // top) & (row // group == route_ref[0])
    mix = jnp.where(named, weight_ref[0], 0.0).astype(jnp.bfloat16)
    for e in range(n_experts):
        part = jnp.dot(
            mix[e * group : (e + 1) * group], hidden_ref[...], preferred_element_type=jnp.float32
        )
        out_ref[e] = part.astype(jnp.bfloat16)


def spread(hidden_rows, weights_low, route_ids, n_experts):
    n_tokens, top, width = hidden_rows.shape
    group = 16
    steps = n_tokens // group
    cols = group * top
    return pl.pallas_call(
        functools.partial(spread_kernel, n_experts, group, top),
        grid=(steps,),
        out_shape=jax.ShapeDtypeStruct((n_experts, n_tokens, width), jnp.bfloat16),
        in_specs=[
            pl.BlockSpec((cols, width), lambda i: (i, 0)),
            pl.BlockSpec((1, 1, cols), lambda i: (i, 0, 0)),
            pl.BlockSpec((1, 1, cols), lambda i: (i, 0, 0)),
        ],
        out_specs=pl.BlockSpec((n_experts, group, width), lambda i: (0, i, 0)),
        name="spread",
    )(
        hidden_rows.reshape(n_tokens * top, width),
        weights_low.astype(jnp.float32).reshape(steps, 1, cols),
        route_ids.reshape(steps, 1, cols),
    )


def deriv_kernel(grad_ref, hidden_ref, down_ref, out_ref):
    projected = lax.dot_general(
        grad_ref[...], down_ref[...], (((1,), (1,)), ((), ())), preferred_element_type=jnp.float32
    )
    out_ref[...] = jnp.sum(projected * hidden_ref[...].astype(jnp.float32), axis=1, keepdims=True)


def derivs_of(grads, hidden, down):
    rows, width = grads.shape
    hidden_width = hidden.shape[1]
    tile = 512
    return pl.pallas_call(
        deriv_kernel,
        grid=(rows // tile,),
        out_shape=jax.ShapeDtypeStruct((rows, 1), jnp.float32),
        in_specs=[
            pl.BlockSpec((tile, width), lambda i: (i, 0)),
            pl.BlockSpec((tile, hidden_width), lambda i: (i, 0)),
            pl.BlockSpec((hidden_width, width), lambda i: (0, 0)),
        ],
        out_specs=pl.BlockSpec((tile, 1), lambda i: (i, 0)),
        compiler_params=pltpu.CompilerParams(vmem_limit_bytes=50 * 1024 * 1024),
        cost_estimate=pl.CostEstimate(
            flops=2 * rows * width * hidden_width, bytes_accessed=2 * rows * width, transcendentals=0
        ),
        name="derivs",
    )(grads, hidden, down)


OWN, ROWS, GET = 0, 1, 2
SPREAD, KEEP, EXPAND, DERIVE, PRODUCT, CLOSE, LOGIT, HANDED = range(8)
SHAPE = (4, 2, 2)
ORDERS = ((0, 2, 1), (2, 0, 1), (0, 1, 2), (1, 0, 2))
WIDTHS = (9, 7, 9, 7)
RELAY_MIB, SETTLE_MIB = 62, 62
PLANES = ((1, 0, 2, 3), (1, 2, 0, 3))
GROUPS = (
    ((1, 0), (1, 1), (0, 0), (0, 1), (2, 0), (2, 1), (3, 0), (3, 1)),
    ((1, 0), (1, 1), (2, 0), (2, 1), (0, 0), (0, 1), (3, 0), (3, 1)),
)
WORK = (
    (SPREAD,),
    (KEEP,),
    (EXPAND, 0),
    (DERIVE, 0),
    (EXPAND, 2),
    (DERIVE, 2),
    (EXPAND, 1),
    (EXPAND, 4),
    (DERIVE, 1),
    (EXPAND, 6),
    (PRODUCT, 0, 0),
    (PRODUCT, 0, 1),
    (PRODUCT, 0, 2),
    (EXPAND, 5),
    (EXPAND, 3),
    (PRODUCT, 0, 3),
    (DERIVE, 3),
    (PRODUCT, 1, 0),
    (PRODUCT, 1, 1),
    (DERIVE, 4),
    (PRODUCT, 1, 2),
    (PRODUCT, 1, 3),
    (DERIVE, 5),
    (PRODUCT, 2, 0),
    (PRODUCT, 2, 1),
    (PRODUCT, 2, 2),
    (EXPAND, 7),
    (PRODUCT, 2, 3),
    (DERIVE, 6),
    (DERIVE, 7),
    (CLOSE, 3, 0),
    (CLOSE, 3, 1),
    (LOGIT,),
    (CLOSE, 3, 2),
    (CLOSE, 3, 3),
    (HANDED,),
)
SCHEDULE = (
    (
        (
            (OWN, 0, 2, 1),
            (OWN, 1, 2, 1),
            (OWN, 2, 1, 1),
        ),
        (
            (OWN, 2, 0, 1),
            (ROWS, 3, 0, 0),
        ),
        (
            (GET, 1, 0, 0, 1),
            (GET, 0, 0, 1, 0),
            (GET, 0, 1, 0, 2),
            (ROWS, 3, 0, 1),
            (ROWS, 3, 1, 1),
            (GET, 0, 0, 1, 1),
            (GET, 1, 1, 0, 1),
            (GET, 1, 0, 0, 0),
            (ROWS, 1, 1, 0),
            (ROWS, 2, 1, 0),
            (GET, 0, 1, 1, 2),
            (ROWS, 0, 1, 1),
            (OWN, 0, 0, 1),
            (ROWS, 2, 0, 0),
            (GET, 0, 1, 1, 0),
            (OWN, 0, 1, 1),
            (OWN, 3, 2, 1),
            (ROWS, 1, 1, 1),
            (GET, 0, 1, 1, 1),
            (GET, 1, 0, 1, 0),
            (GET, 2, 0, 0, 3),
            (OWN, 1, 1, 1),
            (ROWS, 0, 0, 1),
            (GET, 2, 0, 0, 1),
            (ROWS, 1, 0, 0),
            (GET, 1, 1, 0, 0),
            (GET, 1, 0, 0, 3),
            (GET, 0, 0, 1, 3),
            (GET, 0, 1, 0, 0),
            (OWN, 2, 2, 1),
            (GET, 1, 0, 0, 2),
            (GET, 2, 0, 1, 3),
            (ROWS, 3, 1, 0),
            (GET, 1, 1, 1, 0),
            (GET, 1, 0, 1, 1),
            (GET, 1, 0, 1, 3),
            (ROWS, 1, 0, 1),
            (GET, 0, 1, 0, 1),
            (GET, 2, 0, 0, 0),
            (GET, 0, 0, 1, 2),
            (GET, 2, 1, 0, 1),
            (GET, 1, 1, 0, 3),
            (GET, 1, 0, 1, 2),
            (OWN, 1, 0, 1),
            (GET, 1, 1, 0, 2),
            (GET, 3, 0, 0, 2),
            (GET, 1, 1, 1, 1),
            (GET, 2, 0, 1, 0),
            (GET, 2, 0, 1, 1),
            (GET, 2, 1, 0, 0),
            (GET, 1, 1, 1, 3),
            (ROWS, 2, 0, 1),
            (OWN, 3, 1, 1),
            (GET, 3, 1, 0, 2),
            (GET, 1, 1, 1, 2),
            (ROWS, 0, 1, 0),
            (GET, 2, 0, 0, 2),
            (GET, 2, 1, 1, 0),
            (GET, 3, 0, 1, 2),
        ),
        (),
        (
            (OWN, 3, 0, 1),
        ),
        (),
        (
            (GET, 2, 1, 1, 1),
        ),
        (),
        (
            (GET, 3, 1, 1, 2),
        ),
        (
            (GET, 0, 1, 0, 3),
        ),
        (),
        (),
        (
            (GET, 2, 1, 0, 3),
        ),
        (),
        (),
        (
            (GET, 2, 0, 1, 2),
        ),
        (
            (GET, 3, 0, 1, 1),
            (GET, 0, 1, 1, 3),
        ),
        (
            (GET, 2, 1, 0, 2),
        ),
        (
            (GET, 3, 0, 0, 0),
        ),
        (
            (GET, 2, 1, 1, 3),
            (GET, 3, 1, 1, 1),
        ),
        (
            (ROWS, 2, 1, 1),
            (GET, 3, 0, 0, 1),
        ),
        (),
        (
            (GET, 2, 1, 1, 2),
            (GET, 3, 1, 0, 0),
        ),
        (
            (GET, 3, 0, 0, 3),
        ),
        (),
        (
            (GET, 3, 1, 0, 1),
            (GET, 3, 0, 1, 0),
        ),
        (
            (GET, 3, 1, 0, 3),
        ),
        (),
        (
            (GET, 3, 0, 1, 3),
        ),
        (
            (GET, 3, 1, 1, 0),
            (GET, 3, 1, 1, 3),
        ),
        (),
        (),
        (),
        (),
        (),
        (),
    ),
    (
        (
            (OWN, 1, 0, -1),
            (OWN, 1, 1, 1),
            (OWN, 2, 2, 1),
            (OWN, 3, 0, 1),
        ),
        (
            (OWN, 1, 0, 1),
            (OWN, 0, 0, -1),
            (ROWS, 1, 1, 1),
            (ROWS, 0, 1, 0),
            (ROWS, 2, 1, 0),
            (ROWS, 2, 0, 1),
        ),
        (
            (GET, 1, 1, 0, 1),
            (GET, 2, 0, 0, 3),
            (GET, 1, 0, 1, 2),
            (OWN, 1, 2, 1),
            (OWN, 0, 0, 1),
            (GET, 0, 0, 0, 2),
            (GET, 2, 0, 0, 1),
            (GET, 2, 0, 1, 3),
            (OWN, 3, 2, 1),
            (OWN, 3, 0, -1),
            (GET, 0, 1, 0, 2),
            (OWN, 2, 0, -1),
            (GET, 1, 0, 1, 1),
            (ROWS, 3, 1, 0),
            (OWN, 2, 0, 1),
            (ROWS, 2, 1, 1),
            (GET, 2, 1, 0, 1),
            (OWN, 2, 1, 1),
            (OWN, 3, 1, 1),
            (GET, 1, 1, 1, 1),
            (GET, 0, 0, 1, 2),
            (ROWS, 3, 0, 1),
            (GET, 1, 0, 1, 3),
            (GET, 2, 0, 0, 0),
            (GET, 1, 1, 0, 2),
            (ROWS, 1, 1, 0),
            (GET, 1, 1, 0, 3),
            (GET, 0, 0, 1, 1),
            (GET, 0, 1, 1, 2),
            (GET, 3, 0, 0, 2),
            (OWN, 0, 2, 1),
            (GET, 2, 0, 1, 1),
            (GET, 2, 0, 1, 0),
            (GET, 2, 1, 0, 0),
            (GET, 1, 1, 1, 2),
            (ROWS, 1, 0, 1),
            (GET, 1, 1, 1, 3),
            (ROWS, 0, 0, 1),
            (GET, 2, 0, 0, 2),
            (GET, 0, 0, 0, 0),
            (GET, 0, 1, 1, 1),
            (GET, 3, 0, 1, 2),
            (ROWS, 0, 0, 0),
            (GET, 3, 1, 0, 2),
            (OWN, 0, 1, 1),
            (GET, 1, 0, 1, 0),
            (ROWS, 0, 1, 1),
            (GET, 2, 1, 1, 1),
            (GET, 2, 1, 0, 3),
            (ROWS, 2, 0, 0),
            (ROWS, 3, 0, 0),
            (GET, 2, 0, 1, 2),
            (GET, 2, 1, 1, 0),
            (GET, 3, 0, 1, 1),
            (GET, 2, 1, 0, 2),
            (ROWS, 3, 1, 1),
            (GET, 0, 0, 1, 0),
            (GET, 3, 0, 0, 0),
            (GET, 0, 1, 0, 0),
        ),
        (),
        (),
        (),
        (
            (GET, 3, 1, 1, 2),
            (GET, 0, 0, 0, 1),
            (GET, 1, 1, 0, 0),
        ),
        (),
        (
            (GET, 1, 1, 1, 0),
        ),
        (
            (GET, 2, 1, 1, 3),
        ),
        (),
        (),
        (
            (GET, 0, 0, 0, 3),
            (GET, 3, 1, 1, 1),
        ),
        (
            (GET, 2, 1, 1, 2),
        ),
        (),
        (),
        (
            (GET, 0, 1, 0, 3),
            (GET, 3, 0, 0, 1),
            (GET, 0, 1, 1, 0),
            (GET, 3, 0, 1, 0),
        ),
        (
            (GET, 3, 0, 0, 3),
        ),
        (
            (GET, 3, 1, 0, 0),
        ),
        (
            (GET, 0, 0, 1, 3),
        ),
        (
            (GET, 3, 1, 0, 3),
        ),
        (
            (GET, 0, 1, 0, 1),
        ),
        (
            (GET, 0, 1, 1, 3),
        ),
        (),
        (),
        (),
        (
            (GET, 3, 1, 0, 1),
            (GET, 3, 0, 1, 3),
        ),
        (),
        (),
        (
            (GET, 3, 1, 1, 3),
            (GET, 3, 1, 1, 0),
        ),
        (),
        (),
        (),
        (),
        (),
        (),
    ),
)

def near_index(z, y, x, dims):
    return (z * dims[1] + y) * dims[2] + x


def onward(dims, here, source, order):
    offset = [here[i] - source[i] for i in range(3)]
    last = max([i for i in range(3) if offset[order[i]] != 0], default=-1)
    steps = []
    if last >= 0 and order[last] == 0:
        steps.append((0, 1 if offset[0] > 0 else -1))
    for axis in order[last + 1 :]:
        steps += [(axis, 1), (axis, -1)] if axis == 0 else [(axis, 1)]
    return [(a, d) for a, d in steps if a != 0 or 0 <= here[0] + d < dims[0]]


def relay_kernel(
    dims, cap, grad_ref, hidden_ref, routes_ref, scores_ref, down_ref, router_ref,
    weight_ref, handed_ref,
    gall, down, hsend, hgot, meta, mgot, slots, stats, ht, acc, stage, dsend, home, logit,
    next_grad, next_router, next_logit,
    g_send, g_recv, h_send, h_recv, m_send, m_recv, d_send, d_recv, s_send, s_recv, local,
):
    n = dims[0] * dims[1] * dims[2]
    rows = grad_ref.shape[0]
    width = grad_ref.shape[1]
    hidden_width = hidden_ref.shape[1]
    cols = hidden_ref.shape[0]
    top = cols // rows
    me = lax.axis_index("expert")
    section = lax.axis_index("section")
    z, y, x = me // (dims[1] * dims[2]), (me // dims[2]) % dims[1], me % dims[2]
    lower = z < dims[0] // 2
    at_end = (z == 0) | (z == dims[0] - 1)
    sign = jnp.where(lower, 1, -1)
    pair = dims[2] * rows
    hid = ht.at[pl.ds(0, cols), pl.ds(0, hidden_width)]

    load = pltpu.make_async_copy(grad_ref, gall.at[pl.ds(me * rows, rows)], local.at[0])
    load.start()
    load_hidden = pltpu.make_async_copy(hidden_ref, hid, local.at[1])
    load_hidden.start()
    load_down = pltpu.make_async_copy(down_ref, down, local.at[2])
    load_down.start()

    barrier = pltpu.get_barrier_semaphore()
    for i in range(1, n):
        pl.semaphore_signal(barrier, inc=1, device_id={"expert": (me + i) % n}, device_id_type=MESH)
    pl.semaphore_signal(barrier, inc=1, device_id={"section": 1 - section}, device_id_type=MESH)
    pl.semaphore_wait(barrier, n)
    load.wait()

    def plane(mirrored):
        return jnp.where(lower, mirrored, dims[0] - 1 - mirrored)

    def number(rel):
        return near_index(plane(rel[0]), (y + rel[1]) % 2, (x + rel[2]) % 2, dims)

    def piece(source, chunk):
        begin = sum(WIDTHS[:chunk]) * width // sum(WIDTHS)
        size = WIDTHS[chunk] * width // sum(WIDTHS)
        return gall.at[pl.ds(source * rows, rows), pl.ds(begin, size)]

    def grad_copy(source, chunk, axis, step):
        target = [z, y, x]
        target[axis] = z + step * sign if axis == 0 else (target[axis] + 1) % 2
        block = piece(source, chunk)
        return pltpu.make_async_remote_copy(
            src_ref=block,
            dst_ref=block,
            send_sem=g_send.at[source, chunk, axis, (step + 1) // 2],
            recv_sem=g_recv.at[source, chunk],
            device_id={"expert": near_index(*target, dims)},
            device_id_type=MESH,
        )

    def hidden_copy(k):
        return pltpu.make_async_remote_copy(
            src_ref=hsend.at[pl.ds(k * cap, cap)],
            dst_ref=hgot.at[me],
            send_sem=h_send.at[k],
            recv_sem=h_recv.at[me],
            device_id={"expert": k},
            device_id_type=MESH,
        )

    def meta_copy(k):
        return pltpu.make_async_remote_copy(
            src_ref=meta.at[k],
            dst_ref=mgot.at[me],
            send_sem=m_send.at[k],
            recv_sem=m_recv.at[me],
            device_id={"expert": k},
            device_id_type=MESH,
        )

    def home_copy(k):
        return pltpu.make_async_remote_copy(
            src_ref=dsend.at[k],
            dst_ref=home.at[me],
            send_sem=d_send.at[k],
            recv_sem=d_recv.at[me],
            device_id={"expert": k},
            device_id_type=MESH,
        )

    def beside(src, dst, k):
        return pltpu.make_async_remote_copy(
            src_ref=src,
            dst_ref=dst,
            send_sem=s_send.at[k],
            recv_sem=s_recv.at[k],
            device_id={"section": 1 - section},
            device_id_type=MESH,
        )

    mine = gall.at[pl.ds(me * rows, rows)]

    def issue(kind, event):
        here = (kind, 0, 0)
        if event[0] == OWN:
            grad_copy(me, event[1], event[2], event[3]).start()
        elif event[0] == ROWS:
            hidden_copy(number(event[1:])).start()
        else:
            source, chunk = number(event[1:4]), event[4]
            block = piece(source, chunk)
            pltpu.make_async_copy(block, block, g_recv.at[source, chunk]).wait()
            for axis, step in onward(dims, here, event[1:4], ORDERS[chunk]):
                grad_copy(source, chunk, axis, step).start()

    def events(segment):
        for kind in range(2):
            if SCHEDULE[kind][segment]:

                @pl.when(at_end if kind == 0 else jnp.logical_not(at_end))
                def _(kind=kind):
                    for event in SCHEDULE[kind][segment]:
                        issue(kind, event)

    def tables():
        before = lax.broadcasted_iota(jnp.int32, (rows, rows), 0) < lax.broadcasted_iota(jnp.int32, (rows, rows), 1)
        score = scores_ref[...]
        route = routes_ref[...].astype(jnp.float32)
        total = jnp.sum(score, axis=0, keepdims=True)
        weight = score / total
        low = weight.astype(jnp.bfloat16).astype(jnp.float32)
        fix = weight / low
        expert = lax.broadcasted_iota(jnp.int32, (n, rows), 0).astype(jnp.float32)
        hit = [route[k : k + 1] == expert for k in range(top)]
        dense = lambda value: sum(jnp.where(hit[k], value[k : k + 1], 0.0) for k in range(top))
        named = dense(jnp.ones_like(route))
        rank = jnp.dot(
            named.astype(jnp.bfloat16),
            jnp.where(before, 1.0, 0.0).astype(jnp.bfloat16),
            preferred_element_type=jnp.float32,
        )
        score_dense = dense(score)
        stats[0] = score_dense
        stats[1] = dense(fix)
        stats[2] = score_dense / total
        place = jnp.where(named > 0.0, rank, -1.0)
        low_dense = dense(low)
        for e in range(n):
            meta[e, 0:1] = place[e : e + 1]
            meta[e, 1:2] = low_dense[e : e + 1]
        for k in range(top):
            slots[k : k + 1] = jnp.sum(jnp.where(hit[k], rank, 0.0), axis=0, keepdims=True)
        slots[top : 2 * top] = route

    def spread_rows():
        tables()
        load_hidden.wait()
        expand = jnp.where(
            lax.broadcasted_iota(jnp.int32, (rows, cols), 1) // top
            == lax.broadcasted_iota(jnp.int32, (rows, cols), 0),
            1.0,
            0.0,
        ).astype(jnp.bfloat16)
        wide = jnp.dot(slots[...].astype(jnp.bfloat16), expand, preferred_element_type=jnp.float32)
        lane = lax.broadcasted_iota(jnp.int32, (top, cols), 1) % top
        own = lane == lax.broadcasted_iota(jnp.int32, (top, cols), 0)
        slot = jnp.sum(jnp.where(own, wide[:top], 0.0), axis=0, keepdims=True)
        route = jnp.sum(jnp.where(own, wide[top:], 0.0), axis=0, keepdims=True)
        place = (route * cap + slot).astype(jnp.int32)
        block = 256 if (n * cap) % 256 == 0 else cap

        def one(b, _):
            begin = pl.multiple_of(b * block, block)
            want = lax.broadcasted_iota(jnp.int32, (block, cols), 0) + begin
            pick = jnp.where(want == place, 1.0, 0.0).astype(jnp.bfloat16)
            part = jnp.dot(pick, ht[:cols, :hidden_width], preferred_element_type=jnp.float32)
            hsend[pl.ds(begin, block), :] = part.astype(jnp.bfloat16)
            return 0

        lax.fori_loop(0, n * cap // block, one, 0)

    def keep_own():
        own = pltpu.make_async_copy(hsend.at[pl.ds(me * cap, cap)], hgot.at[me], local.at[3])
        own.start()
        own.wait()

    def group_base(group):
        table = GROUPS[0][group], GROUPS[1][group]
        zm = jnp.where(at_end, table[0][0], table[1][0])
        dy = jnp.where(at_end, table[0][1], table[1][1])
        zz = jnp.where(lower, zm, dims[0] - 1 - zm)
        return near_index(zz, (y + dy) % 2, 0, dims)

    def enlarge(group):
        first = group_base(group)
        for j in range(dims[2]):
            source = first + j

            @pl.when(source != me)
            def _(source=source):
                pltpu.make_async_copy(hgot.at[source], hgot.at[source], h_recv.at[source]).wait()
                pltpu.make_async_copy(mgot.at[source], mgot.at[source], m_recv.at[source]).wait()

            @pl.when(source == me)
            def _():
                mgot[me] = meta[me]

            info = mgot[source]
            want = lax.broadcasted_iota(jnp.int32, (cap, rows), 0).astype(jnp.float32)
            pick = jnp.where(want == info[0:1], info[1:2], 0.0).astype(jnp.bfloat16)
            full = lax.dot_general(
                hgot[source], pick, (((0,), (0,)), ((), ())), preferred_element_type=jnp.float32
            )
            ht[:, pl.ds(pl.multiple_of(source * rows, rows), rows)] = full.astype(jnp.bfloat16)

    def derive(group):
        first = group_base(group)
        begin = pl.multiple_of(first * rows, pair)
        block = 512

        def one(m, total):
            at = pl.multiple_of(m * block, block)
            projected = lax.dot_general(
                down[pl.ds(at, block), :],
                gall[pl.ds(begin, pair), :],
                (((1,), (1,)), ((), ())),
                preferred_element_type=jnp.float32,
            )
            held = ht[pl.ds(at, block), pl.ds(begin, pair)].astype(jnp.float32)
            return total + jnp.sum(projected * held, axis=0, keepdims=True)

        total = lax.fori_loop(0, hidden_width // block, one, jnp.zeros((1, pair), jnp.float32))
        for j in range(dims[2]):
            dsend[first + j] = total[:, j * rows : (j + 1) * rows]

            @pl.when(first + j == me)
            def _(j=j):
                home[me] = total[:, j * rows : (j + 1) * rows]

    def send_home(group):
        first = group_base(group)
        for j in range(dims[2]):

            @pl.when(first + j != me)
            def _(source=first + j):
                home_copy(source).start()

    tile = stage.shape[2]
    layer = dims[1] * pair

    def plane_rows(p):
        zm = jnp.where(at_end, PLANES[0][p], PLANES[1][p])
        return pl.ds(pl.multiple_of(jnp.where(lower, zm, dims[0] - 1 - zm) * layer, layer), layer)

    def partial(p, column):
        return jnp.dot(ht[:, plane_rows(p)], gall[plane_rows(p), column], preferred_element_type=jnp.float32)

    def product(p, step):
        def one(j, _):
            column = pl.ds(pl.multiple_of((step * 2 + j) * tile, tile), tile)
            if p == 0:
                acc[:, column] = partial(p, column)
            else:
                acc[:, column] += partial(p, column)
            return 0

        lax.fori_loop(0, 2, one, 0)

    def weight_copy(j, step):
        column = pl.ds(pl.multiple_of((step * 2 + j) * tile, tile), tile)
        return pltpu.make_async_copy(stage.at[j], weight_ref.at[:, column], local.at[4 + j])

    def close(p, step):
        def one(j, _):
            column = pl.ds(pl.multiple_of((step * 2 + j) * tile, tile), tile)
            if step > 0:
                weight_copy(j, step - 1).wait()
            stage[j] = (acc[:, column] + partial(p, column)).astype(stage.dtype)
            weight_copy(j, step).start()
            return 0

        lax.fori_loop(0, 2, one, 0)

    def logits():
        for i in range(1, n):
            source = (me + i) % n
            pltpu.make_async_copy(home.at[source], home.at[source], d_recv.at[source]).wait()
        weighted = home[:, 0, :] * stats[1]
        center = jnp.sum(weighted, axis=0, keepdims=True)
        logit[...] = (1.0 - stats[0]) * (weighted - stats[2] * center)
        beside(logit, next_logit, 2).start()

    def hand_on():
        beside(mine, next_grad, 0).wait()
        beside(router_ref, next_router, 1).wait()
        beside(logit, next_logit, 2).wait()
        value = next_logit[...]
        parts = []
        for _ in range(3):
            parts.append(value.astype(jnp.bfloat16))
            value = value - parts[-1].astype(jnp.float32)
        parts = jnp.concatenate(parts, axis=0)
        size = 1024 if width % 1024 == 0 else width

        def one(j, _):
            column = pl.ds(pl.multiple_of(j * size, size), size)
            extra = lax.dot_general(
                parts,
                jnp.concatenate([next_router[:, column]] * 3, axis=0),
                (((0,), (0,)), ((), ())),
                preferred_element_type=jnp.float32,
            )
            next_grad[:, column] = (next_grad[:, column].astype(jnp.float32) + extra).astype(next_grad.dtype)
            return 0

        lax.fori_loop(0, width // size, one, 0)
        hand_copy.start()

    hand_copy = pltpu.make_async_copy(next_grad, handed_ref, local.at[6])
    steps = width // (2 * tile)

    beside(mine, next_grad, 0).start()
    beside(router_ref, next_router, 1).start()
    late = None
    for segment, op in enumerate(WORK):
        events(segment)
        if late is not None:
            send_home(late)
            late = None
        if op[0] == SPREAD:
            spread_rows()
        elif op[0] == KEEP:
            for i in range(1, n):
                meta_copy((me + i) % n).start()
            keep_own()
            load_down.wait()
        elif op[0] == EXPAND:
            enlarge(op[1])
        elif op[0] == DERIVE:
            derive(op[1])
            late = op[1]
        elif op[0] == PRODUCT:
            product(op[1], op[2])
        elif op[0] == CLOSE:
            close(op[1], op[2])
        elif op[0] == LOGIT:
            logits()
        else:
            hand_on()

    for i in range(1, n):
        k = (me + i) % n
        hidden_copy(k).wait_send()
        meta_copy(k).wait_send()
        home_copy(k).wait_send()
    for kind in range(2):

        @pl.when(at_end if kind == 0 else jnp.logical_not(at_end))
        def _(kind=kind):
            for segment in SCHEDULE[kind]:
                for event in segment:
                    if event[0] == OWN:
                        grad_copy(me, event[1], event[2], event[3]).wait_send()
                    elif event[0] != ROWS:
                        for axis, step in onward(dims, (kind, 0, 0), event[1:4], ORDERS[event[4]]):
                            grad_copy(number(event[1:4]), event[4], axis, step).wait_send()

    for j in range(2):
        weight_copy(j, steps - 1).wait()
    hand_copy.wait()


def relay(grad_rows, hidden_rows, routes, scores, down, router_rows, cap):
    n = router_rows.shape[0]
    n_tokens, width = grad_rows.shape
    top = routes.shape[0]
    entries, hidden_width = hidden_rows.shape
    dims = torus_dims(n)
    low = jnp.bfloat16
    any_space = pl.BlockSpec(memory_space=pl.ANY)
    vmem = pl.BlockSpec(memory_space=pltpu.VMEM)
    hbm = pl.BlockSpec(memory_space=pltpu.HBM)
    dma = pltpu.SemaphoreType.DMA
    return pl.pallas_call(
        functools.partial(relay_kernel, dims, cap),
        out_shape=(
            jax.ShapeDtypeStruct((hidden_width, width), low),
            jax.ShapeDtypeStruct((n_tokens, width), low),
        ),
        in_specs=[hbm, hbm, vmem, vmem, hbm, hbm],
        out_specs=(any_space,) * 2,
        scratch_shapes=[
            pltpu.VMEM((n * n_tokens, width), low),
            pltpu.VMEM((hidden_width, width), low),
            pltpu.VMEM((n * cap, hidden_width), low),
            pltpu.VMEM((n, cap, hidden_width), low),
            pltpu.VMEM((n, 2, n_tokens), jnp.float32),
            pltpu.VMEM((n, 2, n_tokens), jnp.float32),
            pltpu.VMEM((2 * top, n_tokens), jnp.float32),
            pltpu.VMEM((3, n, n_tokens), jnp.float32),
            pltpu.VMEM((hidden_width, n * n_tokens), low),
            pltpu.VMEM((hidden_width, width), jnp.float32),
            pltpu.VMEM((2, hidden_width, 512), low),
            pltpu.VMEM((n, 1, n_tokens), jnp.float32),
            pltpu.VMEM((n, 1, n_tokens), jnp.float32),
            pltpu.VMEM((n, n_tokens), jnp.float32),
            pltpu.VMEM((n_tokens, width), low),
            pltpu.VMEM(router_rows.shape, low),
            pltpu.VMEM((n, n_tokens), jnp.float32),
            dma((n, len(ORDERS), 3, 2)),
            dma((n, len(ORDERS))),
            dma((n,)),
            dma((n,)),
            dma((n,)),
            dma((n,)),
            dma((n,)),
            dma((n,)),
            dma((3,)),
            dma((3,)),
            dma((8,)),
        ],
        compiler_params=pltpu.CompilerParams(
            collective_id=1, has_side_effects=True, vmem_limit_bytes=RELAY_MIB * 1024 * 1024
        ),
        name="relay",
    )(grad_rows, hidden_rows, routes, scores, down, router_rows)


def settle_kernel(parts, weight_ref, handed_ref, weight_out, handed_out, held, kept, arrive, leave):
    size = weight_ref.shape[0] // parts
    first = [pltpu.make_async_copy(handed_ref, kept, arrive.at[parts])]
    second = [pltpu.make_async_copy(kept, handed_out, leave.at[parts])]
    for i in range(parts):
        rows = pl.ds(i * size, size)
        first.append(pltpu.make_async_copy(weight_ref.at[rows], held.at[rows], arrive.at[i]))
        second.append(pltpu.make_async_copy(held.at[rows], weight_out.at[rows], leave.at[i]))
    for copy in first:
        copy.start()
    for copy, onward_copy in zip(first, second):
        copy.wait()
        onward_copy.start()
    for copy in second:
        copy.wait()


def settle(weight, handed):
    parts = 8
    hbm = pl.BlockSpec(memory_space=pl.ANY)
    return pl.pallas_call(
        functools.partial(settle_kernel, parts),
        out_shape=(
            jax.ShapeDtypeStruct(weight.shape, weight.dtype),
            jax.ShapeDtypeStruct(handed.shape, handed.dtype),
        ),
        in_specs=[hbm] * 2,
        out_specs=(hbm,) * 2,
        scratch_shapes=[
            pltpu.VMEM(weight.shape, weight.dtype),
            pltpu.VMEM(handed.shape, handed.dtype),
            pltpu.SemaphoreType.DMA((parts + 1,)),
            pltpu.SemaphoreType.DMA((parts + 1,)),
        ],
        compiler_params=pltpu.CompilerParams(vmem_limit_bytes=SETTLE_MIB * 1024 * 1024),
        name="settle",
    )(weight, handed)


def close_body(grad_out, saved_hidden, routes, scores, down_weight, router):
    grad_rows = grad_out[0]
    hidden_rows = saved_hidden[0]
    n_tokens, top, hidden_width = hidden_rows.shape
    n = router.shape[1]
    cap = 3 * n_tokens * top // (2 * n)
    weight_out, handed = relay(
        grad_rows,
        hidden_rows.reshape(n_tokens * top, hidden_width),
        routes[0].T,
        scores[0].T,
        down_weight[0, 0],
        router[0],
        cap,
    )
    weight_out, handed = settle(weight_out, handed)
    return (weight_out[None, None], handed[None])


def passed_along(array, axis, by):
    size = lax.axis_size(axis)
    return lax.ppermute(array, axis, [(i, (i + by) % size) for i in range(size)])


def body(grad_out, saved_hidden, routes, scores, down_weight, router):
    grad_rows = grad_out[0]
    hidden_rows = saved_hidden[0]
    route_ids = routes[0]
    score_rows = scores[0]
    n_tokens = grad_rows.shape[0]
    n_experts = router.shape[1]
    score_total = jnp.sum(score_rows, axis=1, keepdims=True)
    weights = score_rows / score_total
    weights_low = weights.astype(jnp.bfloat16)

    next_grad = passed_along(grad_rows, "section", -1)
    next_router = passed_along(router[0], "section", -1)
    dense = spread(hidden_rows, weights_low, route_ids, n_experts)
    grads, hidden = exchange(grad_rows, dense)
    derivs = derivs_of(grads, hidden, down_weight[0, 0])
    home = lax.all_to_all(
        derivs.reshape(n_experts, n_tokens), "expert", split_axis=0, concat_axis=0, tiled=True
    )
    weight_out = lax.dot_general(
        hidden, grads, (((0,), (0,)), ((), ())), preferred_element_type=jnp.float32
    ).astype(jnp.bfloat16)

    named = route_ids.T[None] == jnp.arange(n_experts, dtype=jnp.int32)[:, None, None]
    low = weights_low.astype(jnp.float32)
    score_dense = jnp.sum(jnp.where(named, score_rows.T[None], 0.0), axis=1)
    fix_dense = jnp.sum(jnp.where(named, (weights / low).T[None], 0.0), axis=1)
    weighted = home * fix_dense
    center = jnp.sum(weighted, axis=0, keepdims=True)
    total_row = score_total.T
    logit_dense = (1.0 - score_dense) * (weighted - score_dense / total_row * center)
    next_logit = passed_along(logit_dense, "section", -1)
    handed = next_grad.astype(jnp.float32) + lax.dot_general(
        next_logit,
        next_router.astype(jnp.float32),
        (((0,), (0,)), ((), ())),
        precision=lax.Precision.HIGHEST,
    )
    return (weight_out[None, None], handed.astype(jnp.bfloat16)[None])


def solution(mesh):
    close = mesh.shape["section"] == 2 and torus_dims(mesh.shape["expert"]) == SHAPE
    return jax.shard_map(
        close_body if close else body,
        mesh=mesh,
        in_specs=(
            P("section", "expert", None),
            P("section", "expert", None, None),
            P("section", "expert", None),
            P("section", "expert", None),
            P("section", "expert", None, None),
            P("section", None, None),
        ),
        out_specs=(P("section", "expert", None, None), P("section", "expert", None)),
        check_vma=False,
    )
```

```python
import functools

import jax
import jax.numpy as jnp
from jax import lax
from jax.experimental import pallas as pl
from jax.experimental.pallas import tpu as pltpu
from jax.sharding import PartitionSpec as P

MESH = pl.DeviceIdType.MESH


def torus_dims(n):
    dims = [1, 1, 1]
    at = 0
    while n > 1:
        factor = next(f for f in range(2, n + 1) if n % f == 0)
        dims[at % 3] *= factor
        n //= factor
        at += 1
    return tuple(dims)


def tree_edges(dims, order, flip):
    reached = [(0, 0, 0)]
    edges = []
    for axis in order:
        size = dims[axis]
        fresh = []
        for count, start in enumerate(reached):
            extra = (count + flip) % 2 if size % 2 == 0 else 0
            plus = (size - 1) // 2 + (1 - extra if size > 2 and size % 2 == 0 else 0)
            if size == 2:
                plus = 1
            minus = size - 1 - plus
            for step, hops in ((1, plus), (-1, minus)):
                place = start
                for _ in range(hops):
                    after = list(place)
                    after[axis] = (after[axis] + step) % size
                    after = tuple(after)
                    edges.append((place, axis, step, after))
                    fresh.append(after)
                    place = after
        reached = reached + fresh
    return edges


def plan(dims, orders):
    waiting = []
    for chunk, (order, flip) in enumerate(orders):
        edges = tree_edges(dims, order, flip)
        below = {}
        for parent, axis, step, child in reversed(edges):
            below[parent] = max(below.get(parent, 0), below.get(child, 0) + 1)
        for parent, axis, step, child in edges:
            waiting.append((chunk, parent, axis, step, child, below.get(child, 0)))
    arrival = {(chunk, (0, 0, 0)): 0 for chunk in range(len(orders))}
    free = {}
    issued = []
    while waiting:
        best = None
        for item in waiting:
            chunk, parent, axis, step, child, depth = item
            if (chunk, parent) not in arrival:
                continue
            begin = max(arrival[(chunk, parent)], free.get((axis, step), 0))
            key = (begin, -depth, chunk)
            if best is None or key < best[0]:
                best = (key, item)
        (begin, _, _), item = best
        waiting.remove(item)
        chunk, parent, axis, step, child, depth = item
        free[(axis, step)] = begin + 1
        arrival[(chunk, child)] = begin + 1.5
        issued.append((begin, item[:5]))
    issued.sort(key=lambda pair: pair[0])
    return [item for _, item in issued]


def flat(offset, dims):
    return (offset[0] * dims[1] + offset[1]) * dims[2] + offset[2]


def exchange_kernel(dims, sends, grad_ref, dense_ref, all_ref, got_ref, own, own_dense, g_send, g_recv, h_send, h_recv, local):
    n = dims[0] * dims[1] * dims[2]
    me = lax.axis_index("expert")
    here = (me // (dims[1] * dims[2]), (me // dims[2]) % dims[1], me % dims[2])

    def at(offset, sign):
        c = [(here[i] + sign * offset[i] + dims[i]) % dims[i] for i in range(3)]
        return (c[0] * dims[1] + c[1]) * dims[2] + c[2]

    load = pltpu.make_async_copy(grad_ref, own, local.at[0])
    load.start()
    load_dense = pltpu.make_async_copy(dense_ref.at[me], own_dense, local.at[1])
    load_dense.start()
    barrier = pltpu.get_barrier_semaphore()
    for i in range(1, n):
        pl.semaphore_signal(barrier, inc=1, device_id={"expert": (me + i) % n}, device_id_type=MESH)
    pl.semaphore_wait(barrier, n - 1)
    load.wait()

    offsets = [(a, b, c) for a in range(dims[0]) for b in range(dims[1]) for c in range(dims[2])]
    offsets = [o for o in offsets if o != (0, 0, 0)]

    def dense_copy(offset):
        k = flat(offset, dims)
        return pltpu.make_async_remote_copy(
            src_ref=dense_ref.at[at(offset, 1)],
            dst_ref=got_ref.at[me],
            send_sem=h_send.at[k],
            recv_sem=h_recv.at[k],
            device_id={"expert": at(offset, 1)},
            device_id_type=MESH,
        )

    def grad_copy(item):
        chunk, parent, axis, step, child = item
        source = at(parent, -1)
        move = [0, 0, 0]
        move[axis] = step
        k = flat(child, dims)
        return pltpu.make_async_remote_copy(
            src_ref=own.at[chunk] if parent == (0, 0, 0) else all_ref.at[source, chunk],
            dst_ref=all_ref.at[source, chunk],
            send_sem=g_send.at[k, chunk],
            recv_sem=g_recv.at[k, chunk],
            device_id={"expert": at(move, 1)},
            device_id_type=MESH,
        )

    def arrived(chunk, offset):
        k = flat(offset, dims)
        source = at(offset, -1)
        pltpu.make_async_copy(all_ref.at[source, chunk], all_ref.at[source, chunk], g_recv.at[k, chunk]).wait()

    seen = set()
    pending = list(offsets)
    copies = []
    dense_copies = []
    stores = []
    own_sends = sum(1 for item in sends if item[1] == (0, 0, 0))
    every = max(1, (len(sends) * 2 // 3 - own_sends) // max(1, len(pending)))
    for count, item in enumerate(sends):
        chunk, parent = item[0], item[1]
        if parent != (0, 0, 0) and (chunk, parent) not in seen:
            arrived(chunk, parent)
            seen.add((chunk, parent))
        copy = grad_copy(item)
        copy.start()
        copies.append(copy)
        if count >= own_sends and (count - own_sends) % every == 0 and pending:
            extra = dense_copy(pending.pop(0))
            extra.start()
            dense_copies.append(extra)
        if count == own_sends:
            store = pltpu.make_async_copy(own, all_ref.at[me], local.at[2])
            store.start()
            load_dense.wait()
            store_dense = pltpu.make_async_copy(own_dense, got_ref.at[me], local.at[3])
            store_dense.start()
            stores = [store, store_dense]
    for offset in pending:
        extra = dense_copy(offset)
        extra.start()
        dense_copies.append(extra)
    for offset in offsets:
        for chunk in range(own.shape[0]):
            if (chunk, offset) not in seen:
                arrived(chunk, offset)
    for copy in dense_copies:
        copy.wait_recv()
    for copy in dense_copies:
        copy.wait_send()
    for copy in copies:
        copy.wait_send()
    for store in stores:
        store.wait()


def line_kernel(dims, orders, grad_ref, dense_ref, all_ref, got_ref, own, own_dense, g_send, g_recv, h_send, h_recv, local):
    n = dims[0] * dims[1] * dims[2]
    chunks = len(orders)
    me = lax.axis_index("expert")
    here = [me // (dims[1] * dims[2]), (me // dims[2]) % dims[1], me % dims[2]]

    def number(c):
        return (c[0] * dims[1] + c[1]) * dims[2] + c[2]

    load = pltpu.make_async_copy(grad_ref, own, local.at[0])
    load.start()
    load_dense = pltpu.make_async_copy(dense_ref.at[me], own_dense, local.at[1])
    load_dense.start()
    barrier = pltpu.get_barrier_semaphore()
    for i in range(1, n):
        pl.semaphore_signal(barrier, inc=1, device_id={"expert": (me + i) % n}, device_id_type=MESH)
    pl.semaphore_wait(barrier, n - 1)
    load.wait()

    def start(source, chunk, axis, step, home):
        target = list(here)
        target[axis] = (here[axis] + step) % dims[axis]
        pltpu.make_async_remote_copy(
            src_ref=own.at[chunk] if home else all_ref.at[source, chunk],
            dst_ref=all_ref.at[source, chunk],
            send_sem=g_send.at[source, chunk, axis, (step + 1) // 2],
            recv_sem=g_recv.at[source, chunk],
            device_id={"expert": number(target)},
            device_id_type=MESH,
        ).start()

    def finish(source, chunk, axis, step, home):
        piece = own.at[chunk] if home else all_ref.at[source, chunk]
        pltpu.make_async_copy(piece, piece, g_send.at[source, chunk, axis, (step + 1) // 2]).wait()

    def moves(offset, order):
        last = max([i for i in range(3) if offset[order[i]] != 0], default=-1)
        steps = []
        if last >= 0 and dims[order[last]] > 2:
            steps.append((order[last], 1 if offset[order[last]] > 0 else -1))
        for axis in order[last + 1 :]:
            if dims[axis] == 2:
                steps.append((axis, 1))
            elif dims[axis] > 2:
                steps += [(axis, 1), (axis, -1)]
        return steps

    def each_move(offset, order, chunk, act):
        source = number([(here[i] - offset[i] + dims[i]) % dims[i] for i in range(3)])
        home = offset == (0, 0, 0)
        for axis, step in moves(offset, order):
            if dims[axis] == 2:
                act(source, chunk, axis, step, home)
            else:
                inside = here[axis] < dims[axis] - 1 if step > 0 else here[axis] > 0
                pl.when(inside)(functools.partial(act, source, chunk, axis, step, home))

    def on_slice(offset, act):
        valid = None
        for i in range(3):
            if dims[i] > 2 and offset[i] != 0:
                inside = here[i] >= offset[i] if offset[i] > 0 else here[i] < dims[i] + offset[i]
                valid = inside if valid is None else valid & inside
        if valid is None:
            act()
        else:
            pl.when(valid)(act)

    spans = [range(size) if size <= 2 else range(1 - size, size) for size in dims]
    offsets = [(a, b, c) for a in spans[0] for b in spans[1] for c in spans[2] if (a, b, c) != (0, 0, 0)]

    for chunk in range(chunks):
        each_move((0, 0, 0), orders[chunk], chunk, start)

    def dense_copy(k):
        return pltpu.make_async_remote_copy(
            src_ref=dense_ref.at[(me + k) % n],
            dst_ref=got_ref.at[me],
            send_sem=h_send.at[k],
            recv_sem=h_recv.at[k],
            device_id={"expert": (me + k) % n},
            device_id_type=MESH,
        )

    store = pltpu.make_async_copy(own, all_ref.at[me], local.at[2])
    store.start()
    load_dense.wait()
    store_dense = pltpu.make_async_copy(own_dense, got_ref.at[me], local.at[3])
    store_dense.start()

    arrivals = []
    for chunk in range(chunks):
        for offset in offsets:
            hops = [abs(offset[axis]) for axis in orders[chunk]]
            arrivals.append((hops[0] * WEIGHTS[0] + hops[1] * WEIGHTS[1] + hops[2] * WEIGHTS[2], chunk, offset))
    arrivals.sort()
    far = sorted(range(1, n), key=lambda k: -min(k, n - k))
    every = max(1, (len(arrivals) * SHARE // 4) // len(far))
    for count, (_, chunk, offset) in enumerate(arrivals):
        if count % every == 0 and far:
            dense_copy(far.pop(0)).start()

        def arrive(chunk=chunk, offset=offset):
            source = number([(here[i] - offset[i] + dims[i]) % dims[i] for i in range(3)])
            piece = all_ref.at[source, chunk]
            pltpu.make_async_copy(piece, piece, g_recv.at[source, chunk]).wait()
            each_move(offset, orders[chunk], chunk, start)

        on_slice(offset, arrive)
    for k in far:
        dense_copy(k).start()
    for k in range(1, n):
        dense_copy(k).wait()
    for chunk in range(chunks):
        each_move((0, 0, 0), orders[chunk], chunk, finish)
        for offset in offsets:
            if moves(offset, orders[chunk]):
                on_slice(offset, functools.partial(each_move, offset, orders[chunk], chunk, finish))
    store.wait()
    store_dense.wait()


WEIGHTS = (2, 3, 3)
SHARE = 3
LINE_ORDERS = ((0, 2, 1), (0, 1, 2), (0, 2, 1), (0, 1, 2))


def exchange(grad_rows, dense):
    n, n_tokens, hidden_width = dense.shape
    width = grad_rows.shape[1]
    dims = torus_dims(n)
    on_line = 2 in dims
    orders = [((2, 1, 0), 0), ((1, 2, 0), 1), ((0, 2, 1), 0), ((0, 1, 2), 1)]
    if on_line:
        kernel, chunks = functools.partial(line_kernel, dims, LINE_ORDERS), len(LINE_ORDERS)
    else:
        kernel, chunks = functools.partial(exchange_kernel, dims, plan(dims, orders)), len(orders)
    rows = n_tokens // chunks
    grad_chunks = grad_rows.reshape(chunks, rows, width)
    got, dense_got = pl.pallas_call(
        kernel,
        out_shape=(
            jax.ShapeDtypeStruct((n, chunks, rows, width), grad_rows.dtype),
            jax.ShapeDtypeStruct(dense.shape, dense.dtype),
        ),
        in_specs=[pl.BlockSpec(memory_space=pl.ANY)] * 2,
        out_specs=(pl.BlockSpec(memory_space=pl.ANY), pl.BlockSpec(memory_space=pl.ANY)),
        scratch_shapes=[
            pltpu.VMEM((chunks, rows, width), grad_rows.dtype),
            pltpu.VMEM((n_tokens, hidden_width), dense.dtype),
            pltpu.SemaphoreType.DMA((n, chunks, 3, 2) if on_line else (n, chunks)),
            pltpu.SemaphoreType.DMA((n, chunks)),
            pltpu.SemaphoreType.DMA((n,)),
            pltpu.SemaphoreType.DMA((n,)),
            pltpu.SemaphoreType.DMA((4,)),
        ],
        compiler_params=pltpu.CompilerParams(collective_id=0, has_side_effects=True),
        name="exchange",
    )(grad_chunks, dense)
    return got.reshape(n * n_tokens, width), dense_got.reshape(n * n_tokens, hidden_width)


def spread_kernel(n_experts, group, top, hidden_ref, weight_ref, route_ref, out_ref):
    rows, cols = n_experts * group, group * top
    row = lax.broadcasted_iota(jnp.int32, (rows, cols), 0)
    col = lax.broadcasted_iota(jnp.int32, (rows, cols), 1)
    named = (row % group == col // top) & (row // group == route_ref[0])
    mix = jnp.where(named, weight_ref[0], 0.0).astype(jnp.bfloat16)
    for e in range(n_experts):
        part = jnp.dot(
            mix[e * group : (e + 1) * group], hidden_ref[...], preferred_element_type=jnp.float32
        )
        out_ref[e] = part.astype(jnp.bfloat16)


def spread(hidden_rows, weights_low, route_ids, n_experts):
    n_tokens, top, width = hidden_rows.shape
    group = 16
    steps = n_tokens // group
    cols = group * top
    return pl.pallas_call(
        functools.partial(spread_kernel, n_experts, group, top),
        grid=(steps,),
        out_shape=jax.ShapeDtypeStruct((n_experts, n_tokens, width), jnp.bfloat16),
        in_specs=[
            pl.BlockSpec((cols, width), lambda i: (i, 0)),
            pl.BlockSpec((1, 1, cols), lambda i: (i, 0, 0)),
            pl.BlockSpec((1, 1, cols), lambda i: (i, 0, 0)),
        ],
        out_specs=pl.BlockSpec((n_experts, group, width), lambda i: (0, i, 0)),
        name="spread",
    )(
        hidden_rows.reshape(n_tokens * top, width),
        weights_low.astype(jnp.float32).reshape(steps, 1, cols),
        route_ids.reshape(steps, 1, cols),
    )


def deriv_kernel(grad_ref, hidden_ref, down_ref, out_ref):
    projected = lax.dot_general(
        grad_ref[...], down_ref[...], (((1,), (1,)), ((), ())), preferred_element_type=jnp.float32
    )
    out_ref[...] = jnp.sum(projected * hidden_ref[...].astype(jnp.float32), axis=1, keepdims=True)


def derivs_of(grads, hidden, down):
    rows, width = grads.shape
    hidden_width = hidden.shape[1]
    tile = 512
    return pl.pallas_call(
        deriv_kernel,
        grid=(rows // tile,),
        out_shape=jax.ShapeDtypeStruct((rows, 1), jnp.float32),
        in_specs=[
            pl.BlockSpec((tile, width), lambda i: (i, 0)),
            pl.BlockSpec((tile, hidden_width), lambda i: (i, 0)),
            pl.BlockSpec((hidden_width, width), lambda i: (0, 0)),
        ],
        out_specs=pl.BlockSpec((tile, 1), lambda i: (i, 0)),
        compiler_params=pltpu.CompilerParams(vmem_limit_bytes=50 * 1024 * 1024),
        cost_estimate=pl.CostEstimate(
            flops=2 * rows * width * hidden_width, bytes_accessed=2 * rows * width, transcendentals=0
        ),
        name="derivs",
    )(grads, hidden, down)


OWN, ROWS, GET, SEND = range(4)
SPREAD, KEEP, EXPAND, DERIVE, PRODUCT, CLOSE, LOGIT, PART = range(8)
SHAPE = (4, 2, 2)
ORDERS = ((0, 2, 1), (2, 0, 1), (0, 1, 2), (1, 0, 2))
WIDTHS = (9, 7, 9, 7)
RELAY_MIB, SETTLE_MIB = 62, 62
PLANES = ((1, 0, 2, 3), (1, 2, 0, 3))
GROUPS = (
    ((1, 0), (1, 1), (0, 0), (0, 1), (2, 0), (2, 1), (3, 0), (3, 1)),
    ((1, 0), (1, 1), (2, 0), (2, 1), (0, 0), (0, 1), (3, 0), (3, 1)),
)
WORK = (
    (SPREAD,),
    (KEEP,),
    (EXPAND, 0),
    (DERIVE, 0),
    (EXPAND, 2),
    (DERIVE, 2),
    (EXPAND, 1),
    (PRODUCT, 0, 2),
    (EXPAND, 4),
    (PRODUCT, 0, 3),
    (EXPAND, 6),
    (PART, 6, 2, 1, 0),
    (DERIVE, 1),
    (PRODUCT, 0, 0),
    (PRODUCT, 0, 1),
    (EXPAND, 5),
    (EXPAND, 3),
    (PRODUCT, 1, 0),
    (PRODUCT, 1, 1),
    (PRODUCT, 1, 2),
    (DERIVE, 3),
    (PRODUCT, 1, 3),
    (DERIVE, 4),
    (PRODUCT, 2, 0),
    (PART, 6, 1, 0, 0),
    (PRODUCT, 2, 1),
    (DERIVE, 5),
    (PRODUCT, 2, 2),
    (PRODUCT, 2, 3),
    (PART, 6, 0, 0, 0),
    (EXPAND, 7),
    (PART, 7, 2, 1, 0),
    (PART, 7, 1, 0, 0),
    (CLOSE, 3, 2),
    (PART, 6, 3, 0, 1),
    (PART, 7, 0, 0, 0),
    (CLOSE, 3, 0),
    (PART, 7, 3, 0, 1),
    (CLOSE, 3, 1),
    (CLOSE, 3, 3),
    (LOGIT,),
)
SCHEDULE = (
    (
        (
            (OWN, 0, 2, 1),
            (OWN, 1, 2, 1),
            (OWN, 2, 1, 1),
        ),
        (
            (OWN, 2, 0, 1),
            (ROWS, 3, 0, 0),
        ),
        (
            (GET, 1, 0, 0, 1),
            (SEND, 1, 0, 0, 1, 1, 1),
            (GET, 0, 0, 1, 0),
            (GET, 0, 1, 0, 2),
            (SEND, 0, 0, 1, 0, 1, 1),
            (SEND, 0, 1, 0, 2, 2, 1),
            (ROWS, 3, 0, 1),
            (ROWS, 3, 1, 1),
            (GET, 0, 0, 1, 1),
            (GET, 1, 1, 0, 1),
            (SEND, 0, 0, 1, 1, 0, 1),
            (SEND, 0, 0, 1, 1, 1, 1),
            (GET, 1, 0, 0, 0),
            (SEND, 1, 0, 0, 0, 2, 1),
            (SEND, 1, 0, 0, 0, 1, 1),
            (ROWS, 1, 1, 0),
            (ROWS, 2, 1, 0),
            (GET, 0, 1, 1, 2),
            (ROWS, 0, 1, 1),
            (OWN, 0, 0, 1),
            (ROWS, 2, 0, 0),
            (GET, 0, 1, 1, 0),
            (OWN, 0, 1, 1),
            (OWN, 3, 2, 1),
            (ROWS, 1, 1, 1),
            (GET, 0, 1, 1, 1),
            (GET, 1, 0, 1, 0),
            (SEND, 1, 0, 1, 0, 1, 1),
            (GET, 2, 0, 0, 3),
            (SEND, 2, 0, 0, 3, 2, 1),
            (OWN, 1, 1, 1),
            (ROWS, 0, 0, 1),
            (GET, 2, 0, 0, 1),
            (SEND, 2, 0, 0, 1, 1, 1),
            (ROWS, 1, 0, 0),
            (GET, 1, 1, 0, 0),
            (GET, 1, 0, 0, 3),
            (SEND, 1, 0, 0, 3, 2, 1),
            (GET, 0, 0, 1, 3),
            (GET, 0, 1, 0, 0),
            (OWN, 2, 2, 1),
            (GET, 1, 0, 0, 2),
            (SEND, 1, 0, 0, 2, 1, 1),
            (SEND, 1, 0, 0, 2, 2, 1),
            (GET, 2, 0, 1, 3),
            (ROWS, 3, 1, 0),
            (GET, 1, 1, 1, 0),
            (GET, 1, 0, 1, 1),
            (SEND, 1, 0, 1, 1, 1, 1),
            (GET, 1, 0, 1, 3),
            (ROWS, 1, 0, 1),
            (GET, 0, 1, 0, 1),
            (GET, 2, 0, 0, 0),
            (SEND, 2, 0, 0, 0, 2, 1),
            (SEND, 2, 0, 0, 0, 1, 1),
            (GET, 0, 0, 1, 2),
            (GET, 2, 1, 0, 1),
            (GET, 1, 1, 0, 3),
            (SEND, 1, 1, 0, 3, 2, 1),
            (GET, 1, 0, 1, 2),
            (OWN, 1, 0, 1),
            (GET, 1, 1, 0, 2),
            (SEND, 1, 1, 0, 2, 2, 1),
            (GET, 3, 0, 0, 2),
            (SEND, 3, 0, 0, 2, 1, 1),
            (SEND, 3, 0, 0, 2, 2, 1),
            (GET, 1, 1, 1, 1),
            (GET, 2, 0, 1, 0),
            (SEND, 2, 0, 1, 0, 1, 1),
            (GET, 2, 0, 1, 1),
            (SEND, 2, 0, 1, 1, 1, 1),
            (GET, 2, 1, 0, 0),
            (GET, 1, 1, 1, 3),
            (ROWS, 2, 0, 1),
            (OWN, 3, 1, 1),
            (GET, 3, 1, 0, 2),
            (SEND, 3, 1, 0, 2, 2, 1),
            (GET, 1, 1, 1, 2),
            (ROWS, 0, 1, 0),
            (GET, 2, 0, 0, 2),
            (SEND, 2, 0, 0, 2, 1, 1),
            (SEND, 2, 0, 0, 2, 2, 1),
            (GET, 2, 1, 1, 0),
            (GET, 3, 0, 1, 2),
        ),
        (),
        (
            (OWN, 3, 0, 1),
        ),
        (),
        (
            (GET, 2, 1, 1, 1),
        ),
        (),
        (
            (GET, 3, 1, 1, 2),
        ),
        (),
        (),
        (
            (GET, 0, 1, 0, 3),
            (SEND, 0, 1, 0, 3, 0, 1),
            (SEND, 0, 1, 0, 3, 2, 1),
        ),
        (),
        (),
        (
            (GET, 2, 1, 0, 3),
            (SEND, 2, 1, 0, 3, 2, 1),
        ),
        (),
        (
            (GET, 2, 0, 1, 2),
        ),
        (),
        (),
        (
            (GET, 3, 0, 1, 1),
            (SEND, 3, 0, 1, 1, 1, 1),
        ),
        (
            (GET, 0, 1, 1, 3),
        ),
        (
            (GET, 2, 1, 0, 2),
            (SEND, 2, 1, 0, 2, 2, 1),
        ),
        (
            (GET, 3, 0, 0, 0),
            (SEND, 3, 0, 0, 0, 2, 1),
            (SEND, 3, 0, 0, 0, 1, 1),
            (GET, 2, 1, 1, 3),
        ),
        (
            (GET, 3, 1, 1, 1),
            (ROWS, 2, 1, 1),
        ),
        (
            (GET, 3, 0, 0, 1),
            (SEND, 3, 0, 0, 1, 1, 1),
        ),
        (),
        (
            (GET, 2, 1, 1, 2),
        ),
        (
            (GET, 3, 1, 0, 0),
            (GET, 3, 0, 0, 3),
            (SEND, 3, 0, 0, 3, 2, 1),
        ),
        (),
        (
            (GET, 3, 1, 0, 1),
            (GET, 3, 0, 1, 0),
            (SEND, 3, 0, 1, 0, 1, 1),
        ),
        (
            (GET, 3, 1, 0, 3),
            (SEND, 3, 1, 0, 3, 2, 1),
        ),
        (),
        (),
        (),
        (
            (GET, 3, 0, 1, 3),
        ),
        (
            (GET, 3, 1, 1, 0),
        ),
        (),
        (
            (GET, 3, 1, 1, 3),
        ),
        (),
        (),
        (),
    ),
    (
        (
            (OWN, 1, 0, -1),
            (OWN, 1, 1, 1),
            (OWN, 2, 2, 1),
            (OWN, 3, 0, 1),
        ),
        (
            (OWN, 1, 0, 1),
            (OWN, 0, 0, -1),
            (ROWS, 1, 1, 1),
            (ROWS, 0, 1, 0),
            (ROWS, 2, 1, 0),
            (ROWS, 2, 0, 1),
        ),
        (
            (GET, 1, 1, 0, 1),
            (GET, 2, 0, 0, 3),
            (SEND, 2, 0, 0, 3, 0, -1),
            (SEND, 2, 0, 0, 3, 2, 1),
            (GET, 1, 0, 1, 2),
            (OWN, 1, 2, 1),
            (OWN, 0, 0, 1),
            (GET, 0, 0, 0, 2),
            (SEND, 0, 0, 0, 2, 0, 1),
            (SEND, 0, 0, 0, 2, 1, 1),
            (SEND, 0, 0, 0, 2, 2, 1),
            (GET, 2, 0, 0, 1),
            (SEND, 2, 0, 0, 1, 0, -1),
            (SEND, 2, 0, 0, 1, 1, 1),
            (GET, 2, 0, 1, 3),
            (OWN, 3, 2, 1),
            (OWN, 3, 0, -1),
            (GET, 0, 1, 0, 2),
            (SEND, 0, 1, 0, 2, 2, 1),
            (OWN, 2, 0, -1),
            (GET, 1, 0, 1, 1),
            (SEND, 1, 0, 1, 1, 0, 1),
            (SEND, 1, 0, 1, 1, 0, -1),
            (SEND, 1, 0, 1, 1, 1, 1),
            (ROWS, 3, 1, 0),
            (OWN, 2, 0, 1),
            (ROWS, 2, 1, 1),
            (GET, 2, 1, 0, 1),
            (OWN, 2, 1, 1),
            (OWN, 3, 1, 1),
            (GET, 1, 1, 1, 1),
            (GET, 0, 0, 1, 2),
            (ROWS, 3, 0, 1),
            (GET, 1, 0, 1, 3),
            (GET, 2, 0, 0, 0),
            (SEND, 2, 0, 0, 0, 0, -1),
            (SEND, 2, 0, 0, 0, 2, 1),
            (SEND, 2, 0, 0, 0, 1, 1),
            (GET, 1, 1, 0, 2),
            (SEND, 1, 1, 0, 2, 2, 1),
            (ROWS, 1, 1, 0),
            (GET, 1, 1, 0, 3),
            (SEND, 1, 1, 0, 3, 0, 1),
            (SEND, 1, 1, 0, 3, 0, -1),
            (SEND, 1, 1, 0, 3, 2, 1),
            (GET, 0, 0, 1, 1),
            (SEND, 0, 0, 1, 1, 0, 1),
            (SEND, 0, 0, 1, 1, 1, 1),
            (GET, 0, 1, 1, 2),
            (GET, 3, 0, 0, 2),
            (SEND, 3, 0, 0, 2, 0, -1),
            (SEND, 3, 0, 0, 2, 1, 1),
            (SEND, 3, 0, 0, 2, 2, 1),
            (OWN, 0, 2, 1),
            (GET, 2, 0, 1, 1),
            (SEND, 2, 0, 1, 1, 0, -1),
            (SEND, 2, 0, 1, 1, 1, 1),
            (GET, 2, 0, 1, 0),
            (SEND, 2, 0, 1, 0, 1, 1),
            (GET, 2, 1, 0, 0),
            (GET, 1, 1, 1, 2),
            (ROWS, 1, 0, 1),
            (GET, 1, 1, 1, 3),
            (ROWS, 0, 0, 1),
            (GET, 2, 0, 0, 2),
            (SEND, 2, 0, 0, 2, 0, -1),
            (SEND, 2, 0, 0, 2, 1, 1),
            (SEND, 2, 0, 0, 2, 2, 1),
            (GET, 0, 0, 0, 0),
            (SEND, 0, 0, 0, 0, 0, 1),
            (SEND, 0, 0, 0, 0, 2, 1),
            (SEND, 0, 0, 0, 0, 1, 1),
            (GET, 0, 1, 1, 1),
            (GET, 3, 0, 1, 2),
            (ROWS, 0, 0, 0),
            (GET, 3, 1, 0, 2),
            (SEND, 3, 1, 0, 2, 2, 1),
            (OWN, 0, 1, 1),
            (GET, 1, 0, 1, 0),
            (SEND, 1, 0, 1, 0, 1, 1),
            (ROWS, 0, 1, 1),
            (GET, 2, 1, 1, 1),
            (GET, 2, 1, 0, 3),
            (SEND, 2, 1, 0, 3, 0, -1),
            (SEND, 2, 1, 0, 3, 2, 1),
            (ROWS, 2, 0, 0),
            (ROWS, 3, 0, 0),
            (GET, 2, 0, 1, 2),
            (GET, 2, 1, 1, 0),
            (GET, 3, 0, 1, 1),
            (SEND, 3, 0, 1, 1, 0, -1),
            (SEND, 3, 0, 1, 1, 1, 1),
            (GET, 2, 1, 0, 2),
            (SEND, 2, 1, 0, 2, 2, 1),
            (ROWS, 3, 1, 1),
            (GET, 0, 0, 1, 0),
            (SEND, 0, 0, 1, 0, 1, 1),
            (GET, 3, 0, 0, 0),
            (SEND, 3, 0, 0, 0, 0, -1),
            (SEND, 3, 0, 0, 0, 2, 1),
            (SEND, 3, 0, 0, 0, 1, 1),
            (GET, 0, 1, 0, 0),
        ),
        (),
        (),
        (),
        (
            (GET, 3, 1, 1, 2),
            (GET, 0, 0, 0, 1),
            (SEND, 0, 0, 0, 1, 0, 1),
            (SEND, 0, 0, 0, 1, 1, 1),
            (GET, 1, 1, 0, 0),
        ),
        (),
        (),
        (),
        (
            (GET, 1, 1, 1, 0),
            (GET, 2, 1, 1, 3),
        ),
        (),
        (),
        (
            (GET, 0, 0, 0, 3),
            (SEND, 0, 0, 0, 3, 0, 1),
            (SEND, 0, 0, 0, 3, 2, 1),
            (GET, 3, 1, 1, 1),
        ),
        (),
        (
            (GET, 2, 1, 1, 2),
        ),
        (),
        (),
        (
            (GET, 0, 1, 0, 3),
            (SEND, 0, 1, 0, 3, 0, 1),
            (SEND, 0, 1, 0, 3, 2, 1),
            (GET, 3, 0, 0, 1),
            (SEND, 3, 0, 0, 1, 0, -1),
            (SEND, 3, 0, 0, 1, 1, 1),
        ),
        (
            (GET, 0, 1, 1, 0),
        ),
        (
            (GET, 3, 0, 1, 0),
            (SEND, 3, 0, 1, 0, 1, 1),
        ),
        (
            (GET, 3, 0, 0, 3),
            (SEND, 3, 0, 0, 3, 0, -1),
            (SEND, 3, 0, 0, 3, 2, 1),
        ),
        (
            (GET, 3, 1, 0, 0),
            (GET, 0, 0, 1, 3),
        ),
        (
            (GET, 3, 1, 0, 3),
            (SEND, 3, 1, 0, 3, 0, -1),
            (SEND, 3, 1, 0, 3, 2, 1),
        ),
        (
            (GET, 0, 1, 0, 1),
        ),
        (),
        (
            (GET, 0, 1, 1, 3),
        ),
        (),
        (),
        (),
        (
            (GET, 3, 1, 0, 1),
        ),
        (
            (GET, 3, 0, 1, 3),
        ),
        (),
        (),
        (),
        (
            (GET, 3, 1, 1, 3),
            (GET, 3, 1, 1, 0),
        ),
        (),
        (),
        (),
        (),
        (),
    ),
)

def near_index(z, y, x, dims):
    return (z * dims[1] + y) * dims[2] + x


def relay_kernel(
    dims, cap, grad_ref, hidden_ref, routes_ref, scores_ref, down_ref, router_ref,
    weight_ref, next_grad, next_router, next_logit,
    gall, down, hsend, hgot, meta, mgot, slots, stats, ht, acc, stage, dsend, dpart, home, logit,
    g_send, g_recv, h_send, h_recv, m_send, m_recv, d_send, d_recv, s_send, s_recv, local,
):
    n = dims[0] * dims[1] * dims[2]
    rows = grad_ref.shape[0]
    width = grad_ref.shape[1]
    hidden_width = hidden_ref.shape[1]
    cols = hidden_ref.shape[0]
    top = cols // rows
    me = lax.axis_index("expert")
    section = lax.axis_index("section")
    z, y, x = me // (dims[1] * dims[2]), (me // dims[2]) % dims[1], me % dims[2]
    lower = z < dims[0] // 2
    at_end = (z == 0) | (z == dims[0] - 1)
    sign = jnp.where(lower, 1, -1)
    pair = dims[2] * rows
    hid = ht.at[pl.ds(0, cols), pl.ds(0, hidden_width)]

    load = pltpu.make_async_copy(grad_ref, gall.at[pl.ds(me * rows, rows)], local.at[0])
    load.start()
    load_hidden = pltpu.make_async_copy(hidden_ref, hid, local.at[1])
    load_hidden.start()
    load_down = pltpu.make_async_copy(down_ref, down, local.at[2])
    load_down.start()

    barrier = pltpu.get_barrier_semaphore()
    for i in range(1, n):
        pl.semaphore_signal(barrier, inc=1, device_id={"expert": (me + i) % n}, device_id_type=MESH)
    pl.semaphore_signal(barrier, inc=1, device_id={"section": 1 - section}, device_id_type=MESH)
    pl.semaphore_wait(barrier, n)
    load.wait()

    def plane(mirrored):
        return jnp.where(lower, mirrored, dims[0] - 1 - mirrored)

    def number(rel):
        return near_index(plane(rel[0]), (y + rel[1]) % 2, (x + rel[2]) % 2, dims)

    def span(chunk):
        return sum(WIDTHS[:chunk]) * width // sum(WIDTHS), WIDTHS[chunk] * width // sum(WIDTHS)

    def piece(source, chunk):
        begin, size = span(chunk)
        return gall.at[pl.ds(source * rows, rows), pl.ds(begin, size)]

    def grad_copy(source, chunk, axis, step):
        target = [z, y, x]
        target[axis] = z + step * sign if axis == 0 else (target[axis] + 1) % 2
        block = piece(source, chunk)
        return pltpu.make_async_remote_copy(
            src_ref=block,
            dst_ref=block,
            send_sem=g_send.at[source, chunk, axis, (step + 1) // 2],
            recv_sem=g_recv.at[source, chunk],
            device_id={"expert": near_index(*target, dims)},
            device_id_type=MESH,
        )

    def hidden_copy(k):
        return pltpu.make_async_remote_copy(
            src_ref=hsend.at[pl.ds(k * cap, cap)],
            dst_ref=hgot.at[me],
            send_sem=h_send.at[k],
            recv_sem=h_recv.at[me],
            device_id={"expert": k},
            device_id_type=MESH,
        )

    def meta_copy(k):
        return pltpu.make_async_remote_copy(
            src_ref=meta.at[k],
            dst_ref=mgot.at[me],
            send_sem=m_send.at[k],
            recv_sem=m_recv.at[me],
            device_id={"expert": k},
            device_id_type=MESH,
        )

    def home_copy(k):
        return pltpu.make_async_remote_copy(
            src_ref=dsend.at[k],
            dst_ref=home.at[me],
            send_sem=d_send.at[k],
            recv_sem=d_recv.at[me],
            device_id={"expert": k},
            device_id_type=MESH,
        )

    def beside(src, dst, k):
        return pltpu.make_async_remote_copy(
            src_ref=src,
            dst_ref=dst,
            send_sem=s_send.at[k],
            recv_sem=s_recv.at[k],
            device_id={"section": 1 - section},
            device_id_type=MESH,
        )

    mine = gall.at[pl.ds(me * rows, rows)]

    def issue(event):
        if event[0] == OWN:
            grad_copy(me, event[1], event[2], event[3]).start()
        elif event[0] == ROWS:
            hidden_copy(number(event[1:])).start()
        else:
            source, chunk = number(event[1:4]), event[4]
            block = piece(source, chunk)
            if event[0] == GET:
                pltpu.make_async_copy(block, block, g_recv.at[source, chunk]).wait()
            else:
                grad_copy(source, chunk, event[5], event[6]).start()

    def events(segment):
        for kind in range(2):
            if SCHEDULE[kind][segment]:

                @pl.when(at_end if kind == 0 else jnp.logical_not(at_end))
                def _(kind=kind):
                    for event in SCHEDULE[kind][segment]:
                        issue(event)

    def tables():
        before = lax.broadcasted_iota(jnp.int32, (rows, rows), 0) < lax.broadcasted_iota(jnp.int32, (rows, rows), 1)
        score = scores_ref[...]
        route = routes_ref[...].astype(jnp.float32)
        total = jnp.sum(score, axis=0, keepdims=True)
        weight = score / total
        low = weight.astype(jnp.bfloat16).astype(jnp.float32)
        fix = weight / low
        expert = lax.broadcasted_iota(jnp.int32, (n, rows), 0).astype(jnp.float32)
        hit = [route[k : k + 1] == expert for k in range(top)]
        dense = lambda value: sum(jnp.where(hit[k], value[k : k + 1], 0.0) for k in range(top))
        named = dense(jnp.ones_like(route))
        rank = jnp.dot(
            named.astype(jnp.bfloat16),
            jnp.where(before, 1.0, 0.0).astype(jnp.bfloat16),
            preferred_element_type=jnp.float32,
        )
        score_dense = dense(score)
        stats[0] = score_dense
        stats[1] = dense(fix)
        stats[2] = score_dense / total
        place = jnp.where(named > 0.0, rank, -1.0)
        low_dense = dense(low)
        for e in range(n):
            meta[e, 0:1] = place[e : e + 1]
            meta[e, 1:2] = low_dense[e : e + 1]
        for k in range(top):
            slots[k : k + 1] = jnp.sum(jnp.where(hit[k], rank, 0.0), axis=0, keepdims=True)
        slots[top : 2 * top] = route

    def spread_rows():
        tables()
        load_hidden.wait()
        expand = jnp.where(
            lax.broadcasted_iota(jnp.int32, (rows, cols), 1) // top
            == lax.broadcasted_iota(jnp.int32, (rows, cols), 0),
            1.0,
            0.0,
        ).astype(jnp.bfloat16)
        wide = jnp.dot(slots[...].astype(jnp.bfloat16), expand, preferred_element_type=jnp.float32)
        lane = lax.broadcasted_iota(jnp.int32, (top, cols), 1) % top
        own = lane == lax.broadcasted_iota(jnp.int32, (top, cols), 0)
        slot = jnp.sum(jnp.where(own, wide[:top], 0.0), axis=0, keepdims=True)
        route = jnp.sum(jnp.where(own, wide[top:], 0.0), axis=0, keepdims=True)
        place = (route * cap + slot).astype(jnp.int32)
        block = 256 if (n * cap) % 256 == 0 else cap

        def one(b, _):
            begin = pl.multiple_of(b * block, block)
            want = lax.broadcasted_iota(jnp.int32, (block, cols), 0) + begin
            pick = jnp.where(want == place, 1.0, 0.0).astype(jnp.bfloat16)
            part = jnp.dot(pick, ht[:cols, :hidden_width], preferred_element_type=jnp.float32)
            hsend[pl.ds(begin, block), :] = part.astype(jnp.bfloat16)
            return 0

        lax.fori_loop(0, n * cap // block, one, 0)

    def keep_own():
        own = pltpu.make_async_copy(hsend.at[pl.ds(me * cap, cap)], hgot.at[me], local.at[3])
        own.start()
        own.wait()

    def group_base(group):
        table = GROUPS[0][group], GROUPS[1][group]
        zm = jnp.where(at_end, table[0][0], table[1][0])
        dy = jnp.where(at_end, table[0][1], table[1][1])
        zz = jnp.where(lower, zm, dims[0] - 1 - zm)
        return near_index(zz, (y + dy) % 2, 0, dims)

    def enlarge(group):
        first = group_base(group)
        for j in range(dims[2]):
            source = first + j

            @pl.when(source != me)
            def _(source=source):
                pltpu.make_async_copy(hgot.at[source], hgot.at[source], h_recv.at[source]).wait()
                pltpu.make_async_copy(mgot.at[source], mgot.at[source], m_recv.at[source]).wait()

            @pl.when(source == me)
            def _():
                mgot[me] = meta[me]

            info = mgot[source]
            want = lax.broadcasted_iota(jnp.int32, (cap, rows), 0).astype(jnp.float32)
            pick = jnp.where(want == info[0:1], info[1:2], 0.0).astype(jnp.bfloat16)
            full = lax.dot_general(
                hgot[source], pick, (((0,), (0,)), ((), ())), preferred_element_type=jnp.float32
            )
            ht[:, pl.ds(pl.multiple_of(source * rows, rows), rows)] = full.astype(jnp.bfloat16)

    def derive(group):
        first = group_base(group)
        begin = pl.multiple_of(first * rows, pair)
        block = 512

        def one(m, total):
            at = pl.multiple_of(m * block, block)
            projected = lax.dot_general(
                down[pl.ds(at, block), :],
                gall[pl.ds(begin, pair), :],
                (((1,), (1,)), ((), ())),
                preferred_element_type=jnp.float32,
            )
            held = ht[pl.ds(at, block), pl.ds(begin, pair)].astype(jnp.float32)
            return total + jnp.sum(projected * held, axis=0, keepdims=True)

        keep_derived(first, lax.fori_loop(0, hidden_width // block, one, jnp.zeros((1, pair), jnp.float32)))

    def derive_part(group, chunk, opening, closing):
        first = group_base(group)
        begin = pl.multiple_of(first * rows, pair)
        block = 512
        start, size = span(chunk)

        def one(m, total):
            at = pl.multiple_of(m * block, block)
            projected = lax.dot_general(
                down[pl.ds(at, block), pl.ds(start, size)],
                gall[pl.ds(begin, pair), pl.ds(start, size)],
                (((1,), (1,)), ((), ())),
                preferred_element_type=jnp.float32,
            )
            held = ht[pl.ds(at, block), pl.ds(begin, pair)].astype(jnp.float32)
            return total + jnp.sum(projected * held, axis=0, keepdims=True)

        total = lax.fori_loop(0, hidden_width // block, one, jnp.zeros((1, pair), jnp.float32))
        if not opening:
            total = total + dpart[group % 2]
        if closing:
            keep_derived(first, total)
        else:
            dpart[group % 2] = total

    def keep_derived(first, total):
        for j in range(dims[2]):
            dsend[first + j] = total[:, j * rows : (j + 1) * rows]

            @pl.when(first + j == me)
            def _(j=j):
                home[me] = total[:, j * rows : (j + 1) * rows]

    def send_home(group):
        first = group_base(group)
        for j in range(dims[2]):

            @pl.when(first + j != me)
            def _(source=first + j):
                home_copy(source).start()

    tile = stage.shape[2]
    layer = dims[1] * pair

    def plane_rows(p):
        zm = jnp.where(at_end, PLANES[0][p], PLANES[1][p])
        return pl.ds(pl.multiple_of(jnp.where(lower, zm, dims[0] - 1 - zm) * layer, layer), layer)

    def partial(p, column):
        return jnp.dot(ht[:, plane_rows(p)], gall[plane_rows(p), column], preferred_element_type=jnp.float32)

    def product(p, step):
        def one(j, _):
            column = pl.ds(pl.multiple_of((step * 2 + j) * tile, tile), tile)
            if p == 0:
                acc[:, column] = partial(p, column)
            else:
                acc[:, column] += partial(p, column)
            return 0

        lax.fori_loop(0, 2, one, 0)

    def weight_copy(j, step):
        column = pl.ds(pl.multiple_of((step * 2 + j) * tile, tile), tile)
        return pltpu.make_async_copy(stage.at[j], weight_ref.at[:, column], local.at[4 + j])

    def close(p, step, before):
        def one(j, _):
            column = pl.ds(pl.multiple_of((step * 2 + j) * tile, tile), tile)
            if before is not None:
                weight_copy(j, before).wait()
            stage[j] = (acc[:, column] + partial(p, column)).astype(stage.dtype)
            weight_copy(j, step).start()
            return 0

        lax.fori_loop(0, 2, one, 0)

    def logits():
        for i in range(1, n):
            source = (me + i) % n
            pltpu.make_async_copy(home.at[source], home.at[source], d_recv.at[source]).wait()
        weighted = home[:, 0, :] * stats[1]
        center = jnp.sum(weighted, axis=0, keepdims=True)
        logit[...] = (1.0 - stats[0]) * (weighted - stats[2] * center)
        beside(logit, next_logit, 2).start()

    beside(mine, next_grad, 0).start()
    beside(router_ref, next_router, 1).start()
    late = None
    closed = None
    for segment, op in enumerate(WORK):
        events(segment)
        if late is not None:
            send_home(late)
            late = None
        if op[0] == SPREAD:
            spread_rows()
        elif op[0] == KEEP:
            for i in range(1, n):
                meta_copy((me + i) % n).start()
            keep_own()
            load_down.wait()
        elif op[0] == EXPAND:
            enlarge(op[1])
        elif op[0] == DERIVE:
            derive(op[1])
            late = op[1]
        elif op[0] == PRODUCT:
            product(op[1], op[2])
        elif op[0] == CLOSE:
            close(op[1], op[2], closed)
            closed = op[2]
        elif op[0] == PART:
            derive_part(*op[1:])
            if op[4]:
                late = op[1]
        elif op[0] == LOGIT:
            logits()

    for i in range(1, n):
        k = (me + i) % n
        hidden_copy(k).wait_send()
        meta_copy(k).wait_send()
        home_copy(k).wait_send()
    for kind in range(2):

        @pl.when(at_end if kind == 0 else jnp.logical_not(at_end))
        def _(kind=kind):
            for segment in SCHEDULE[kind]:
                for event in segment:
                    if event[0] == OWN:
                        grad_copy(me, event[1], event[2], event[3]).wait_send()
                    elif event[0] == SEND:
                        grad_copy(number(event[1:4]), event[4], event[5], event[6]).wait_send()

    for j in range(2):
        weight_copy(j, closed).wait()
    beside(mine, next_grad, 0).wait()
    beside(router_ref, next_router, 1).wait()
    beside(logit, next_logit, 2).wait()


def relay(grad_rows, hidden_rows, routes, scores, down, router_rows, cap):
    n = router_rows.shape[0]
    n_tokens, width = grad_rows.shape
    top = routes.shape[0]
    entries, hidden_width = hidden_rows.shape
    dims = torus_dims(n)
    low = jnp.bfloat16
    any_space = pl.BlockSpec(memory_space=pl.ANY)
    vmem = pl.BlockSpec(memory_space=pltpu.VMEM)
    hbm = pl.BlockSpec(memory_space=pltpu.HBM)
    dma = pltpu.SemaphoreType.DMA
    return pl.pallas_call(
        functools.partial(relay_kernel, dims, cap),
        out_shape=(
            jax.ShapeDtypeStruct((hidden_width, width), low),
            jax.ShapeDtypeStruct((n_tokens, width), low),
            jax.ShapeDtypeStruct(router_rows.shape, low),
            jax.ShapeDtypeStruct((n, n_tokens), jnp.float32),
        ),
        in_specs=[hbm, hbm, vmem, vmem, hbm, hbm],
        out_specs=(any_space,) * 4,
        scratch_shapes=[
            pltpu.VMEM((n * n_tokens, width), low),
            pltpu.VMEM((hidden_width, width), low),
            pltpu.VMEM((n * cap, hidden_width), low),
            pltpu.VMEM((n, cap, hidden_width), low),
            pltpu.VMEM((n, 2, n_tokens), jnp.float32),
            pltpu.VMEM((n, 2, n_tokens), jnp.float32),
            pltpu.VMEM((2 * top, n_tokens), jnp.float32),
            pltpu.VMEM((3, n, n_tokens), jnp.float32),
            pltpu.VMEM((hidden_width, n * n_tokens), low),
            pltpu.VMEM((hidden_width, width), jnp.float32),
            pltpu.VMEM((2, hidden_width, 512), low),
            pltpu.VMEM((n, 1, n_tokens), jnp.float32),
            pltpu.VMEM((2, 1, dims[2] * n_tokens), jnp.float32),
            pltpu.VMEM((n, 1, n_tokens), jnp.float32),
            pltpu.VMEM((n, n_tokens), jnp.float32),
            dma((n, len(ORDERS), 3, 2)),
            dma((n, len(ORDERS))),
            dma((n,)),
            dma((n,)),
            dma((n,)),
            dma((n,)),
            dma((n,)),
            dma((n,)),
            dma((3,)),
            dma((3,)),
            dma((8,)),
        ],
        compiler_params=pltpu.CompilerParams(
            collective_id=1, has_side_effects=True, vmem_limit_bytes=RELAY_MIB * 1024 * 1024
        ),
        name="relay",
    )(grad_rows, hidden_rows, routes, scores, down, router_rows)


def settle_kernel(
    parts, weight_ref, grad_ref, router_ref, logit_ref, weight_out, handed_out, held, kept, rows, value, arrive, leave
):
    size = weight_ref.shape[0] // parts
    tile = grad_ref.shape[1] // parts
    small = [
        pltpu.make_async_copy(grad_ref, kept, arrive.at[parts]),
        pltpu.make_async_copy(router_ref, rows, arrive.at[parts + 1]),
        pltpu.make_async_copy(logit_ref, value, arrive.at[parts + 2]),
    ]
    first, second = [], []
    for i in range(parts):
        block = pl.ds(i * size, size)
        first.append(pltpu.make_async_copy(weight_ref.at[block], held.at[block], arrive.at[i]))
        second.append(pltpu.make_async_copy(held.at[block], weight_out.at[block], leave.at[i]))
    for copy in small + first:
        copy.start()
    for copy in small:
        copy.wait()
    rest = value[...]
    pieces = []
    for _ in range(3):
        pieces.append(rest.astype(jnp.bfloat16))
        rest = rest - pieces[-1].astype(jnp.float32)
    pieces = jnp.concatenate(pieces, axis=0)
    for i in range(parts):
        first[i].wait()
        second[i].start()
        column = pl.ds(i * tile, tile)
        extra = lax.dot_general(
            pieces,
            jnp.concatenate([rows[:, column]] * 3, axis=0),
            (((0,), (0,)), ((), ())),
            preferred_element_type=jnp.float32,
        )
        kept[:, column] = (kept[:, column].astype(jnp.float32) + extra).astype(kept.dtype)
    last = pltpu.make_async_copy(kept, handed_out, leave.at[parts])
    last.start()
    for copy in second:
        copy.wait()
    last.wait()


def settle(weight, next_grad, next_router, next_logit):
    parts = 8
    hbm = pl.BlockSpec(memory_space=pl.ANY)
    return pl.pallas_call(
        functools.partial(settle_kernel, parts),
        out_shape=(
            jax.ShapeDtypeStruct(weight.shape, weight.dtype),
            jax.ShapeDtypeStruct(next_grad.shape, next_grad.dtype),
        ),
        in_specs=[hbm] * 4,
        out_specs=(hbm,) * 2,
        scratch_shapes=[
            pltpu.VMEM(weight.shape, weight.dtype),
            pltpu.VMEM(next_grad.shape, next_grad.dtype),
            pltpu.VMEM(next_router.shape, next_router.dtype),
            pltpu.VMEM(next_logit.shape, next_logit.dtype),
            pltpu.SemaphoreType.DMA((parts + 3,)),
            pltpu.SemaphoreType.DMA((parts + 1,)),
        ],
        compiler_params=pltpu.CompilerParams(vmem_limit_bytes=SETTLE_MIB * 1024 * 1024),
        name="settle",
    )(weight, next_grad, next_router, next_logit)


def close_body(grad_out, saved_hidden, routes, scores, down_weight, router):
    grad_rows = grad_out[0]
    hidden_rows = saved_hidden[0]
    n_tokens, top, hidden_width = hidden_rows.shape
    n = router.shape[1]
    cap = 3 * n_tokens * top // (2 * n)
    results = relay(
        grad_rows,
        hidden_rows.reshape(n_tokens * top, hidden_width),
        routes[0].T,
        scores[0].T,
        down_weight[0, 0],
        router[0],
        cap,
    )
    weight_out, handed = settle(*results)
    return (weight_out[None, None], handed[None])


def passed_along(array, axis, by):
    size = lax.axis_size(axis)
    return lax.ppermute(array, axis, [(i, (i + by) % size) for i in range(size)])


def body(grad_out, saved_hidden, routes, scores, down_weight, router):
    grad_rows = grad_out[0]
    hidden_rows = saved_hidden[0]
    route_ids = routes[0]
    score_rows = scores[0]
    n_tokens = grad_rows.shape[0]
    n_experts = router.shape[1]
    score_total = jnp.sum(score_rows, axis=1, keepdims=True)
    weights = score_rows / score_total
    weights_low = weights.astype(jnp.bfloat16)

    next_grad = passed_along(grad_rows, "section", -1)
    next_router = passed_along(router[0], "section", -1)
    dense = spread(hidden_rows, weights_low, route_ids, n_experts)
    grads, hidden = exchange(grad_rows, dense)
    derivs = derivs_of(grads, hidden, down_weight[0, 0])
    home = lax.all_to_all(
        derivs.reshape(n_experts, n_tokens), "expert", split_axis=0, concat_axis=0, tiled=True
    )
    weight_out = lax.dot_general(
        hidden, grads, (((0,), (0,)), ((), ())), preferred_element_type=jnp.float32
    ).astype(jnp.bfloat16)

    named = route_ids.T[None] == jnp.arange(n_experts, dtype=jnp.int32)[:, None, None]
    low = weights_low.astype(jnp.float32)
    score_dense = jnp.sum(jnp.where(named, score_rows.T[None], 0.0), axis=1)
    fix_dense = jnp.sum(jnp.where(named, (weights / low).T[None], 0.0), axis=1)
    weighted = home * fix_dense
    center = jnp.sum(weighted, axis=0, keepdims=True)
    total_row = score_total.T
    logit_dense = (1.0 - score_dense) * (weighted - score_dense / total_row * center)
    next_logit = passed_along(logit_dense, "section", -1)
    handed = next_grad.astype(jnp.float32) + lax.dot_general(
        next_logit,
        next_router.astype(jnp.float32),
        (((0,), (0,)), ((), ())),
        precision=lax.Precision.HIGHEST,
    )
    return (weight_out[None, None], handed.astype(jnp.bfloat16)[None])


def solution(mesh):
    close = mesh.shape["section"] == 2 and torus_dims(mesh.shape["expert"]) == SHAPE
    return jax.shard_map(
        close_body if close else body,
        mesh=mesh,
        in_specs=(
            P("section", "expert", None),
            P("section", "expert", None, None),
            P("section", "expert", None),
            P("section", "expert", None),
            P("section", "expert", None, None),
            P("section", None, None),
        ),
        out_specs=(P("section", "expert", None, None), P("section", "expert", None)),
        check_vma=False,
    )
```

```python
import functools

import jax
import jax.numpy as jnp
from jax import lax
from jax.experimental import pallas as pl
from jax.experimental.pallas import tpu as pltpu
from jax.sharding import PartitionSpec as P

MESH = pl.DeviceIdType.MESH


def torus_dims(n):
    dims = [1, 1, 1]
    at = 0
    while n > 1:
        factor = next(f for f in range(2, n + 1) if n % f == 0)
        dims[at % 3] *= factor
        n //= factor
        at += 1
    return tuple(dims)


def tree_edges(dims, order, flip):
    reached = [(0, 0, 0)]
    edges = []
    for axis in order:
        size = dims[axis]
        fresh = []
        for count, start in enumerate(reached):
            extra = (count + flip) % 2 if size % 2 == 0 else 0
            plus = (size - 1) // 2 + (1 - extra if size > 2 and size % 2 == 0 else 0)
            if size == 2:
                plus = 1
            minus = size - 1 - plus
            for step, hops in ((1, plus), (-1, minus)):
                place = start
                for _ in range(hops):
                    after = list(place)
                    after[axis] = (after[axis] + step) % size
                    after = tuple(after)
                    edges.append((place, axis, step, after))
                    fresh.append(after)
                    place = after
        reached = reached + fresh
    return edges


def plan(dims, orders):
    waiting = []
    for chunk, (order, flip) in enumerate(orders):
        edges = tree_edges(dims, order, flip)
        below = {}
        for parent, axis, step, child in reversed(edges):
            below[parent] = max(below.get(parent, 0), below.get(child, 0) + 1)
        for parent, axis, step, child in edges:
            waiting.append((chunk, parent, axis, step, child, below.get(child, 0)))
    arrival = {(chunk, (0, 0, 0)): 0 for chunk in range(len(orders))}
    free = {}
    issued = []
    while waiting:
        best = None
        for item in waiting:
            chunk, parent, axis, step, child, depth = item
            if (chunk, parent) not in arrival:
                continue
            begin = max(arrival[(chunk, parent)], free.get((axis, step), 0))
            key = (begin, -depth, chunk)
            if best is None or key < best[0]:
                best = (key, item)
        (begin, _, _), item = best
        waiting.remove(item)
        chunk, parent, axis, step, child, depth = item
        free[(axis, step)] = begin + 1
        arrival[(chunk, child)] = begin + 1.5
        issued.append((begin, item[:5]))
    issued.sort(key=lambda pair: pair[0])
    return [item for _, item in issued]


def flat(offset, dims):
    return (offset[0] * dims[1] + offset[1]) * dims[2] + offset[2]


def exchange_kernel(dims, sends, grad_ref, dense_ref, all_ref, got_ref, own, own_dense, g_send, g_recv, h_send, h_recv, local):
    n = dims[0] * dims[1] * dims[2]
    me = lax.axis_index("expert")
    here = (me // (dims[1] * dims[2]), (me // dims[2]) % dims[1], me % dims[2])

    def at(offset, sign):
        c = [(here[i] + sign * offset[i] + dims[i]) % dims[i] for i in range(3)]
        return (c[0] * dims[1] + c[1]) * dims[2] + c[2]

    load = pltpu.make_async_copy(grad_ref, own, local.at[0])
    load.start()
    load_dense = pltpu.make_async_copy(dense_ref.at[me], own_dense, local.at[1])
    load_dense.start()
    barrier = pltpu.get_barrier_semaphore()
    for i in range(1, n):
        pl.semaphore_signal(barrier, inc=1, device_id={"expert": (me + i) % n}, device_id_type=MESH)
    pl.semaphore_wait(barrier, n - 1)
    load.wait()

    offsets = [(a, b, c) for a in range(dims[0]) for b in range(dims[1]) for c in range(dims[2])]
    offsets = [o for o in offsets if o != (0, 0, 0)]

    def dense_copy(offset):
        k = flat(offset, dims)
        return pltpu.make_async_remote_copy(
            src_ref=dense_ref.at[at(offset, 1)],
            dst_ref=got_ref.at[me],
            send_sem=h_send.at[k],
            recv_sem=h_recv.at[k],
            device_id={"expert": at(offset, 1)},
            device_id_type=MESH,
        )

    def grad_copy(item):
        chunk, parent, axis, step, child = item
        source = at(parent, -1)
        move = [0, 0, 0]
        move[axis] = step
        k = flat(child, dims)
        return pltpu.make_async_remote_copy(
            src_ref=own.at[chunk] if parent == (0, 0, 0) else all_ref.at[source, chunk],
            dst_ref=all_ref.at[source, chunk],
            send_sem=g_send.at[k, chunk],
            recv_sem=g_recv.at[k, chunk],
            device_id={"expert": at(move, 1)},
            device_id_type=MESH,
        )

    def arrived(chunk, offset):
        k = flat(offset, dims)
        source = at(offset, -1)
        pltpu.make_async_copy(all_ref.at[source, chunk], all_ref.at[source, chunk], g_recv.at[k, chunk]).wait()

    seen = set()
    pending = list(offsets)
    copies = []
    dense_copies = []
    stores = []
    own_sends = sum(1 for item in sends if item[1] == (0, 0, 0))
    every = max(1, (len(sends) * 2 // 3 - own_sends) // max(1, len(pending)))
    for count, item in enumerate(sends):
        chunk, parent = item[0], item[1]
        if parent != (0, 0, 0) and (chunk, parent) not in seen:
            arrived(chunk, parent)
            seen.add((chunk, parent))
        copy = grad_copy(item)
        copy.start()
        copies.append(copy)
        if count >= own_sends and (count - own_sends) % every == 0 and pending:
            extra = dense_copy(pending.pop(0))
            extra.start()
            dense_copies.append(extra)
        if count == own_sends:
            store = pltpu.make_async_copy(own, all_ref.at[me], local.at[2])
            store.start()
            load_dense.wait()
            store_dense = pltpu.make_async_copy(own_dense, got_ref.at[me], local.at[3])
            store_dense.start()
            stores = [store, store_dense]
    for offset in pending:
        extra = dense_copy(offset)
        extra.start()
        dense_copies.append(extra)
    for offset in offsets:
        for chunk in range(own.shape[0]):
            if (chunk, offset) not in seen:
                arrived(chunk, offset)
    for copy in dense_copies:
        copy.wait_recv()
    for copy in dense_copies:
        copy.wait_send()
    for copy in copies:
        copy.wait_send()
    for store in stores:
        store.wait()


def line_kernel(dims, orders, grad_ref, dense_ref, all_ref, got_ref, own, own_dense, g_send, g_recv, h_send, h_recv, local):
    n = dims[0] * dims[1] * dims[2]
    chunks = len(orders)
    me = lax.axis_index("expert")
    here = [me // (dims[1] * dims[2]), (me // dims[2]) % dims[1], me % dims[2]]

    def number(c):
        return (c[0] * dims[1] + c[1]) * dims[2] + c[2]

    load = pltpu.make_async_copy(grad_ref, own, local.at[0])
    load.start()
    load_dense = pltpu.make_async_copy(dense_ref.at[me], own_dense, local.at[1])
    load_dense.start()
    barrier = pltpu.get_barrier_semaphore()
    for i in range(1, n):
        pl.semaphore_signal(barrier, inc=1, device_id={"expert": (me + i) % n}, device_id_type=MESH)
    pl.semaphore_wait(barrier, n - 1)
    load.wait()

    def start(source, chunk, axis, step, home):
        target = list(here)
        target[axis] = (here[axis] + step) % dims[axis]
        pltpu.make_async_remote_copy(
            src_ref=own.at[chunk] if home else all_ref.at[source, chunk],
            dst_ref=all_ref.at[source, chunk],
            send_sem=g_send.at[source, chunk, axis, (step + 1) // 2],
            recv_sem=g_recv.at[source, chunk],
            device_id={"expert": number(target)},
            device_id_type=MESH,
        ).start()

    def finish(source, chunk, axis, step, home):
        piece = own.at[chunk] if home else all_ref.at[source, chunk]
        pltpu.make_async_copy(piece, piece, g_send.at[source, chunk, axis, (step + 1) // 2]).wait()

    def moves(offset, order):
        last = max([i for i in range(3) if offset[order[i]] != 0], default=-1)
        steps = []
        if last >= 0 and dims[order[last]] > 2:
            steps.append((order[last], 1 if offset[order[last]] > 0 else -1))
        for axis in order[last + 1 :]:
            if dims[axis] == 2:
                steps.append((axis, 1))
            elif dims[axis] > 2:
                steps += [(axis, 1), (axis, -1)]
        return steps

    def each_move(offset, order, chunk, act):
        source = number([(here[i] - offset[i] + dims[i]) % dims[i] for i in range(3)])
        home = offset == (0, 0, 0)
        for axis, step in moves(offset, order):
            if dims[axis] == 2:
                act(source, chunk, axis, step, home)
            else:
                inside = here[axis] < dims[axis] - 1 if step > 0 else here[axis] > 0
                pl.when(inside)(functools.partial(act, source, chunk, axis, step, home))

    def on_slice(offset, act):
        valid = None
        for i in range(3):
            if dims[i] > 2 and offset[i] != 0:
                inside = here[i] >= offset[i] if offset[i] > 0 else here[i] < dims[i] + offset[i]
                valid = inside if valid is None else valid & inside
        if valid is None:
            act()
        else:
            pl.when(valid)(act)

    spans = [range(size) if size <= 2 else range(1 - size, size) for size in dims]
    offsets = [(a, b, c) for a in spans[0] for b in spans[1] for c in spans[2] if (a, b, c) != (0, 0, 0)]

    for chunk in range(chunks):
        each_move((0, 0, 0), orders[chunk], chunk, start)

    def dense_copy(k):
        return pltpu.make_async_remote_copy(
            src_ref=dense_ref.at[(me + k) % n],
            dst_ref=got_ref.at[me],
            send_sem=h_send.at[k],
            recv_sem=h_recv.at[k],
            device_id={"expert": (me + k) % n},
            device_id_type=MESH,
        )

    store = pltpu.make_async_copy(own, all_ref.at[me], local.at[2])
    store.start()
    load_dense.wait()
    store_dense = pltpu.make_async_copy(own_dense, got_ref.at[me], local.at[3])
    store_dense.start()

    arrivals = []
    for chunk in range(chunks):
        for offset in offsets:
            hops = [abs(offset[axis]) for axis in orders[chunk]]
            arrivals.append((hops[0] * WEIGHTS[0] + hops[1] * WEIGHTS[1] + hops[2] * WEIGHTS[2], chunk, offset))
    arrivals.sort()
    far = sorted(range(1, n), key=lambda k: -min(k, n - k))
    every = max(1, (len(arrivals) * SHARE // 4) // len(far))
    for count, (_, chunk, offset) in enumerate(arrivals):
        if count % every == 0 and far:
            dense_copy(far.pop(0)).start()

        def arrive(chunk=chunk, offset=offset):
            source = number([(here[i] - offset[i] + dims[i]) % dims[i] for i in range(3)])
            piece = all_ref.at[source, chunk]
            pltpu.make_async_copy(piece, piece, g_recv.at[source, chunk]).wait()
            each_move(offset, orders[chunk], chunk, start)

        on_slice(offset, arrive)
    for k in far:
        dense_copy(k).start()
    for k in range(1, n):
        dense_copy(k).wait()
    for chunk in range(chunks):
        each_move((0, 0, 0), orders[chunk], chunk, finish)
        for offset in offsets:
            if moves(offset, orders[chunk]):
                on_slice(offset, functools.partial(each_move, offset, orders[chunk], chunk, finish))
    store.wait()
    store_dense.wait()


WEIGHTS = (2, 3, 3)
SHARE = 3
LINE_ORDERS = ((0, 2, 1), (0, 1, 2), (0, 2, 1), (0, 1, 2))


def exchange(grad_rows, dense):
    n, n_tokens, hidden_width = dense.shape
    width = grad_rows.shape[1]
    dims = torus_dims(n)
    on_line = 2 in dims
    orders = [((2, 1, 0), 0), ((1, 2, 0), 1), ((0, 2, 1), 0), ((0, 1, 2), 1)]
    if on_line:
        kernel, chunks = functools.partial(line_kernel, dims, LINE_ORDERS), len(LINE_ORDERS)
    else:
        kernel, chunks = functools.partial(exchange_kernel, dims, plan(dims, orders)), len(orders)
    rows = n_tokens // chunks
    grad_chunks = grad_rows.reshape(chunks, rows, width)
    got, dense_got = pl.pallas_call(
        kernel,
        out_shape=(
            jax.ShapeDtypeStruct((n, chunks, rows, width), grad_rows.dtype),
            jax.ShapeDtypeStruct(dense.shape, dense.dtype),
        ),
        in_specs=[pl.BlockSpec(memory_space=pl.ANY)] * 2,
        out_specs=(pl.BlockSpec(memory_space=pl.ANY), pl.BlockSpec(memory_space=pl.ANY)),
        scratch_shapes=[
            pltpu.VMEM((chunks, rows, width), grad_rows.dtype),
            pltpu.VMEM((n_tokens, hidden_width), dense.dtype),
            pltpu.SemaphoreType.DMA((n, chunks, 3, 2) if on_line else (n, chunks)),
            pltpu.SemaphoreType.DMA((n, chunks)),
            pltpu.SemaphoreType.DMA((n,)),
            pltpu.SemaphoreType.DMA((n,)),
            pltpu.SemaphoreType.DMA((4,)),
        ],
        compiler_params=pltpu.CompilerParams(collective_id=0, has_side_effects=True),
        name="exchange",
    )(grad_chunks, dense)
    return got.reshape(n * n_tokens, width), dense_got.reshape(n * n_tokens, hidden_width)


def spread_kernel(n_experts, group, top, hidden_ref, weight_ref, route_ref, out_ref):
    rows, cols = n_experts * group, group * top
    row = lax.broadcasted_iota(jnp.int32, (rows, cols), 0)
    col = lax.broadcasted_iota(jnp.int32, (rows, cols), 1)
    named = (row % group == col // top) & (row // group == route_ref[0])
    mix = jnp.where(named, weight_ref[0], 0.0).astype(jnp.bfloat16)
    for e in range(n_experts):
        part = jnp.dot(
            mix[e * group : (e + 1) * group], hidden_ref[...], preferred_element_type=jnp.float32
        )
        out_ref[e] = part.astype(jnp.bfloat16)


def spread(hidden_rows, weights_low, route_ids, n_experts):
    n_tokens, top, width = hidden_rows.shape
    group = 16
    steps = n_tokens // group
    cols = group * top
    return pl.pallas_call(
        functools.partial(spread_kernel, n_experts, group, top),
        grid=(steps,),
        out_shape=jax.ShapeDtypeStruct((n_experts, n_tokens, width), jnp.bfloat16),
        in_specs=[
            pl.BlockSpec((cols, width), lambda i: (i, 0)),
            pl.BlockSpec((1, 1, cols), lambda i: (i, 0, 0)),
            pl.BlockSpec((1, 1, cols), lambda i: (i, 0, 0)),
        ],
        out_specs=pl.BlockSpec((n_experts, group, width), lambda i: (0, i, 0)),
        name="spread",
    )(
        hidden_rows.reshape(n_tokens * top, width),
        weights_low.astype(jnp.float32).reshape(steps, 1, cols),
        route_ids.reshape(steps, 1, cols),
    )


def deriv_kernel(grad_ref, hidden_ref, down_ref, out_ref):
    projected = lax.dot_general(
        grad_ref[...], down_ref[...], (((1,), (1,)), ((), ())), preferred_element_type=jnp.float32
    )
    out_ref[...] = jnp.sum(projected * hidden_ref[...].astype(jnp.float32), axis=1, keepdims=True)


def derivs_of(grads, hidden, down):
    rows, width = grads.shape
    hidden_width = hidden.shape[1]
    tile = 512
    return pl.pallas_call(
        deriv_kernel,
        grid=(rows // tile,),
        out_shape=jax.ShapeDtypeStruct((rows, 1), jnp.float32),
        in_specs=[
            pl.BlockSpec((tile, width), lambda i: (i, 0)),
            pl.BlockSpec((tile, hidden_width), lambda i: (i, 0)),
            pl.BlockSpec((hidden_width, width), lambda i: (0, 0)),
        ],
        out_specs=pl.BlockSpec((tile, 1), lambda i: (i, 0)),
        compiler_params=pltpu.CompilerParams(vmem_limit_bytes=50 * 1024 * 1024),
        cost_estimate=pl.CostEstimate(
            flops=2 * rows * width * hidden_width, bytes_accessed=2 * rows * width, transcendentals=0
        ),
        name="derivs",
    )(grads, hidden, down)


OWN, ROWS, GET, SEND = range(4)
SPREAD, KEEP, EXPAND, DERIVE, PRODUCT, CLOSE, LOGIT, PART = range(8)
SHAPE = (4, 2, 2)
ORDERS = ((0, 2, 1), (2, 0, 1), (0, 1, 2), (1, 0, 2))
WIDTHS = (9, 7, 9, 7)
RELAY_MIB, SETTLE_MIB = 62, 62
PLANES = ((1, 0, 2, 3), (1, 2, 0, 3))
GROUPS = (
    ((1, 0), (1, 1), (0, 0), (0, 1), (2, 0), (2, 1), (3, 0), (3, 1)),
    ((1, 0), (1, 1), (2, 0), (2, 1), (0, 0), (0, 1), (3, 0), (3, 1)),
)
WORK = (
    (SPREAD,),
    (KEEP,),
    (EXPAND, 0),
    (DERIVE, 0),
    (EXPAND, 2),
    (DERIVE, 2),
    (EXPAND, 1),
    (PRODUCT, 0, 2),
    (EXPAND, 4),
    (PRODUCT, 0, 3),
    (EXPAND, 6),
    (PART, 6, 2, 1, 0),
    (DERIVE, 1),
    (PRODUCT, 0, 0),
    (PRODUCT, 0, 1),
    (EXPAND, 5),
    (EXPAND, 3),
    (PRODUCT, 1, 0),
    (PRODUCT, 1, 1),
    (PRODUCT, 1, 2),
    (DERIVE, 3),
    (PRODUCT, 1, 3),
    (DERIVE, 4),
    (PRODUCT, 2, 0),
    (PART, 6, 1, 0, 0),
    (PRODUCT, 2, 1),
    (DERIVE, 5),
    (PRODUCT, 2, 2),
    (PRODUCT, 2, 3),
    (PART, 6, 0, 0, 0),
    (EXPAND, 7),
    (PART, 7, 2, 1, 0),
    (PART, 7, 1, 0, 0),
    (CLOSE, 3, 2),
    (PART, 6, 3, 0, 1),
    (PART, 7, 0, 0, 0),
    (CLOSE, 3, 0),
    (PART, 7, 3, 0, 1),
    (CLOSE, 3, 1),
    (CLOSE, 3, 3),
    (LOGIT,),
)
SCHEDULE = (
    (
        (
            (OWN, 0, 2, 1),
            (OWN, 1, 2, 1),
            (OWN, 2, 1, 1),
        ),
        (
            (OWN, 2, 0, 1),
            (ROWS, 3, 0, 0),
        ),
        (
            (GET, 1, 0, 0, 1),
            (SEND, 1, 0, 0, 1, 1, 1),
            (GET, 0, 0, 1, 0),
            (GET, 0, 1, 0, 2),
            (SEND, 0, 0, 1, 0, 1, 1),
            (SEND, 0, 1, 0, 2, 2, 1),
            (ROWS, 3, 0, 1),
            (ROWS, 3, 1, 1),
            (GET, 0, 0, 1, 1),
            (GET, 1, 1, 0, 1),
            (SEND, 0, 0, 1, 1, 0, 1),
            (SEND, 0, 0, 1, 1, 1, 1),
            (GET, 1, 0, 0, 0),
            (SEND, 1, 0, 0, 0, 2, 1),
            (SEND, 1, 0, 0, 0, 1, 1),
            (ROWS, 1, 1, 0),
            (ROWS, 2, 1, 0),
            (GET, 0, 1, 1, 2),
            (ROWS, 0, 1, 1),
            (OWN, 0, 0, 1),
            (ROWS, 2, 0, 0),
            (GET, 0, 1, 1, 0),
            (OWN, 0, 1, 1),
            (OWN, 3, 2, 1),
            (ROWS, 1, 1, 1),
            (GET, 0, 1, 1, 1),
            (GET, 1, 0, 1, 0),
            (SEND, 1, 0, 1, 0, 1, 1),
            (GET, 2, 0, 0, 3),
            (SEND, 2, 0, 0, 3, 2, 1),
            (OWN, 1, 1, 1),
            (ROWS, 0, 0, 1),
            (GET, 2, 0, 0, 1),
            (SEND, 2, 0, 0, 1, 1, 1),
            (ROWS, 1, 0, 0),
            (GET, 1, 1, 0, 0),
            (GET, 1, 0, 0, 3),
            (SEND, 1, 0, 0, 3, 2, 1),
            (GET, 0, 0, 1, 3),
            (GET, 0, 1, 0, 0),
            (OWN, 2, 2, 1),
            (GET, 1, 0, 0, 2),
            (SEND, 1, 0, 0, 2, 1, 1),
            (SEND, 1, 0, 0, 2, 2, 1),
            (GET, 2, 0, 1, 3),
            (ROWS, 3, 1, 0),
            (GET, 1, 1, 1, 0),
            (GET, 1, 0, 1, 1),
            (SEND, 1, 0, 1, 1, 1, 1),
            (GET, 1, 0, 1, 3),
            (ROWS, 1, 0, 1),
            (GET, 0, 1, 0, 1),
            (GET, 2, 0, 0, 0),
            (SEND, 2, 0, 0, 0, 2, 1),
            (SEND, 2, 0, 0, 0, 1, 1),
            (GET, 0, 0, 1, 2),
            (GET, 2, 1, 0, 1),
            (GET, 1, 1, 0, 3),
            (SEND, 1, 1, 0, 3, 2, 1),
            (GET, 1, 0, 1, 2),
            (OWN, 1, 0, 1),
            (GET, 1, 1, 0, 2),
            (SEND, 1, 1, 0, 2, 2, 1),
            (GET, 3, 0, 0, 2),
            (SEND, 3, 0, 0, 2, 2, 1),
            (GET, 1, 1, 1, 1),
            (GET, 2, 0, 1, 0),
            (SEND, 2, 0, 1, 0, 1, 1),
            (GET, 2, 0, 1, 1),
            (SEND, 2, 0, 1, 1, 1, 1),
            (GET, 2, 1, 0, 0),
            (SEND, 3, 0, 0, 2, 1, 1),
            (GET, 1, 1, 1, 3),
            (ROWS, 2, 0, 1),
            (OWN, 3, 1, 1),
            (GET, 2, 1, 1, 0),
            (GET, 1, 1, 1, 2),
            (ROWS, 0, 1, 0),
            (GET, 2, 0, 0, 2),
            (SEND, 2, 0, 0, 2, 1, 1),
            (SEND, 2, 0, 0, 2, 2, 1),
            (GET, 2, 1, 1, 1),
            (GET, 3, 0, 1, 2),
        ),
        (),
        (
            (OWN, 3, 0, 1),
        ),
        (),
        (
            (GET, 3, 1, 0, 2),
            (SEND, 3, 1, 0, 2, 2, 1),
        ),
        (),
        (
            (GET, 2, 0, 1, 2),
        ),
        (),
        (),
        (
            (GET, 0, 1, 0, 3),
            (SEND, 0, 1, 0, 3, 0, 1),
            (SEND, 0, 1, 0, 3, 2, 1),
        ),
        (),
        (),
        (
            (GET, 2, 1, 0, 3),
            (SEND, 2, 1, 0, 3, 2, 1),
        ),
        (),
        (
            (GET, 3, 1, 1, 2),
        ),
        (),
        (),
        (
            (GET, 3, 0, 1, 1),
            (SEND, 3, 0, 1, 1, 1, 1),
        ),
        (
            (GET, 0, 1, 1, 3),
        ),
        (
            (GET, 2, 1, 0, 2),
            (SEND, 2, 1, 0, 2, 2, 1),
        ),
        (
            (GET, 3, 0, 0, 0),
            (SEND, 3, 0, 0, 0, 2, 1),
            (SEND, 3, 0, 0, 0, 1, 1),
            (GET, 2, 1, 1, 3),
        ),
        (
            (GET, 3, 1, 1, 1),
            (ROWS, 2, 1, 1),
        ),
        (
            (GET, 3, 0, 0, 1),
            (SEND, 3, 0, 0, 1, 1, 1),
        ),
        (),
        (
            (GET, 2, 1, 1, 2),
        ),
        (
            (GET, 3, 1, 0, 0),
            (GET, 3, 0, 0, 3),
            (SEND, 3, 0, 0, 3, 2, 1),
        ),
        (),
        (
            (GET, 3, 1, 0, 1),
            (GET, 3, 0, 1, 0),
            (SEND, 3, 0, 1, 0, 1, 1),
        ),
        (
            (GET, 3, 1, 0, 3),
            (SEND, 3, 1, 0, 3, 2, 1),
        ),
        (),
        (),
        (),
        (
            (GET, 3, 0, 1, 3),
        ),
        (
            (GET, 3, 1, 1, 0),
        ),
        (),
        (
            (GET, 3, 1, 1, 3),
        ),
        (),
        (),
        (),
    ),
    (
        (
            (OWN, 1, 0, -1),
            (OWN, 1, 1, 1),
            (OWN, 2, 2, 1),
            (OWN, 3, 0, 1),
        ),
        (
            (OWN, 1, 0, 1),
            (OWN, 0, 0, -1),
            (ROWS, 1, 1, 1),
            (ROWS, 0, 1, 0),
            (ROWS, 2, 1, 0),
            (ROWS, 2, 0, 1),
        ),
        (
            (GET, 1, 1, 0, 1),
            (GET, 2, 0, 0, 3),
            (SEND, 2, 0, 0, 3, 0, -1),
            (SEND, 2, 0, 0, 3, 2, 1),
            (GET, 1, 0, 1, 2),
            (OWN, 1, 2, 1),
            (OWN, 0, 0, 1),
            (GET, 0, 0, 0, 2),
            (SEND, 0, 0, 0, 2, 0, 1),
            (SEND, 0, 0, 0, 2, 1, 1),
            (SEND, 0, 0, 0, 2, 2, 1),
            (GET, 2, 0, 0, 1),
            (SEND, 2, 0, 0, 1, 0, -1),
            (SEND, 2, 0, 0, 1, 1, 1),
            (GET, 2, 0, 1, 3),
            (OWN, 3, 2, 1),
            (OWN, 3, 0, -1),
            (GET, 0, 1, 0, 2),
            (SEND, 0, 1, 0, 2, 2, 1),
            (OWN, 2, 0, -1),
            (GET, 1, 0, 1, 1),
            (SEND, 1, 0, 1, 1, 0, 1),
            (SEND, 1, 0, 1, 1, 0, -1),
            (SEND, 1, 0, 1, 1, 1, 1),
            (ROWS, 3, 1, 0),
            (OWN, 2, 0, 1),
            (ROWS, 2, 1, 1),
            (GET, 2, 1, 0, 1),
            (OWN, 2, 1, 1),
            (OWN, 3, 1, 1),
            (GET, 1, 1, 1, 1),
            (GET, 0, 0, 1, 2),
            (ROWS, 3, 0, 1),
            (GET, 1, 0, 1, 3),
            (GET, 2, 0, 0, 0),
            (SEND, 2, 0, 0, 0, 0, -1),
            (SEND, 2, 0, 0, 0, 2, 1),
            (SEND, 2, 0, 0, 0, 1, 1),
            (GET, 1, 1, 0, 2),
            (SEND, 1, 1, 0, 2, 2, 1),
            (ROWS, 1, 1, 0),
            (GET, 1, 1, 0, 3),
            (SEND, 1, 1, 0, 3, 0, 1),
            (SEND, 1, 1, 0, 3, 0, -1),
            (SEND, 1, 1, 0, 3, 2, 1),
            (GET, 0, 0, 1, 1),
            (SEND, 0, 0, 1, 1, 0, 1),
            (SEND, 0, 0, 1, 1, 1, 1),
            (GET, 0, 1, 1, 2),
            (GET, 3, 0, 0, 2),
            (SEND, 3, 0, 0, 2, 0, -1),
            (SEND, 3, 0, 0, 2, 1, 1),
            (SEND, 3, 0, 0, 2, 2, 1),
            (OWN, 0, 2, 1),
            (GET, 2, 0, 1, 1),
            (SEND, 2, 0, 1, 1, 0, -1),
            (SEND, 2, 0, 1, 1, 1, 1),
            (GET, 2, 0, 1, 0),
            (SEND, 2, 0, 1, 0, 1, 1),
            (GET, 2, 1, 0, 0),
            (GET, 1, 1, 1, 2),
            (ROWS, 1, 0, 1),
            (GET, 1, 1, 1, 3),
            (ROWS, 0, 0, 1),
            (GET, 2, 0, 0, 2),
            (SEND, 2, 0, 0, 2, 0, -1),
            (SEND, 2, 0, 0, 2, 1, 1),
            (SEND, 2, 0, 0, 2, 2, 1),
            (GET, 0, 0, 0, 0),
            (SEND, 0, 0, 0, 0, 0, 1),
            (SEND, 0, 0, 0, 0, 2, 1),
            (SEND, 0, 0, 0, 0, 1, 1),
            (GET, 0, 1, 1, 1),
            (GET, 3, 0, 1, 2),
            (ROWS, 0, 0, 0),
            (GET, 3, 1, 0, 2),
            (SEND, 3, 1, 0, 2, 2, 1),
            (OWN, 0, 1, 1),
            (GET, 1, 0, 1, 0),
            (SEND, 1, 0, 1, 0, 1, 1),
            (ROWS, 0, 1, 1),
            (GET, 2, 1, 1, 1),
            (GET, 2, 1, 0, 3),
            (SEND, 2, 1, 0, 3, 0, -1),
            (SEND, 2, 1, 0, 3, 2, 1),
            (ROWS, 2, 0, 0),
            (ROWS, 3, 0, 0),
            (GET, 2, 0, 1, 2),
            (GET, 2, 1, 1, 0),
            (GET, 3, 0, 1, 1),
            (SEND, 3, 0, 1, 1, 0, -1),
            (SEND, 3, 0, 1, 1, 1, 1),
            (GET, 2, 1, 0, 2),
            (SEND, 2, 1, 0, 2, 2, 1),
            (ROWS, 3, 1, 1),
            (GET, 0, 0, 1, 0),
            (SEND, 0, 0, 1, 0, 1, 1),
            (GET, 3, 0, 0, 0),
            (SEND, 3, 0, 0, 0, 0, -1),
            (SEND, 3, 0, 0, 0, 2, 1),
            (SEND, 3, 0, 0, 0, 1, 1),
            (GET, 0, 1, 0, 0),
        ),
        (),
        (),
        (),
        (
            (GET, 3, 1, 1, 2),
            (GET, 0, 0, 0, 1),
            (SEND, 0, 0, 0, 1, 0, 1),
            (SEND, 0, 0, 0, 1, 1, 1),
            (GET, 1, 1, 0, 0),
        ),
        (),
        (),
        (),
        (
            (GET, 1, 1, 1, 0),
            (GET, 2, 1, 1, 3),
        ),
        (),
        (),
        (
            (GET, 0, 0, 0, 3),
            (SEND, 0, 0, 0, 3, 0, 1),
            (SEND, 0, 0, 0, 3, 2, 1),
            (GET, 3, 1, 1, 1),
        ),
        (),
        (
            (GET, 2, 1, 1, 2),
        ),
        (),
        (),
        (
            (GET, 0, 1, 0, 3),
            (SEND, 0, 1, 0, 3, 0, 1),
            (SEND, 0, 1, 0, 3, 2, 1),
            (GET, 3, 0, 0, 1),
            (SEND, 3, 0, 0, 1, 0, -1),
            (SEND, 3, 0, 0, 1, 1, 1),
        ),
        (
            (GET, 0, 1, 1, 0),
        ),
        (
            (GET, 3, 0, 1, 0),
            (SEND, 3, 0, 1, 0, 1, 1),
        ),
        (
            (GET, 3, 0, 0, 3),
            (SEND, 3, 0, 0, 3, 0, -1),
            (SEND, 3, 0, 0, 3, 2, 1),
        ),
        (
            (GET, 3, 1, 0, 0),
            (GET, 0, 0, 1, 3),
        ),
        (
            (GET, 3, 1, 0, 3),
            (SEND, 3, 1, 0, 3, 0, -1),
            (SEND, 3, 1, 0, 3, 2, 1),
        ),
        (
            (GET, 0, 1, 0, 1),
        ),
        (),
        (
            (GET, 0, 1, 1, 3),
        ),
        (),
        (),
        (),
        (
            (GET, 3, 1, 0, 1),
        ),
        (
            (GET, 3, 0, 1, 3),
        ),
        (),
        (),
        (),
        (
            (GET, 3, 1, 1, 3),
            (GET, 3, 1, 1, 0),
        ),
        (),
        (),
        (),
        (),
        (),
    ),
)

def near_index(z, y, x, dims):
    return (z * dims[1] + y) * dims[2] + x


def relay_kernel(
    dims, cap, grad_ref, hidden_ref, routes_ref, scores_ref, down_ref, router_ref,
    weight_ref, next_grad, next_router, next_logit,
    gall, down, hsend, hgot, meta, mgot, slots, stats, ht, acc, stage, dsend, dpart, home, logit,
    g_send, g_recv, h_send, h_recv, m_send, m_recv, d_send, d_recv, s_send, s_recv, local,
):
    n = dims[0] * dims[1] * dims[2]
    rows = grad_ref.shape[0]
    width = grad_ref.shape[1]
    hidden_width = hidden_ref.shape[1]
    cols = hidden_ref.shape[0]
    top = cols // rows
    me = lax.axis_index("expert")
    section = lax.axis_index("section")
    z, y, x = me // (dims[1] * dims[2]), (me // dims[2]) % dims[1], me % dims[2]
    lower = z < dims[0] // 2
    at_end = (z == 0) | (z == dims[0] - 1)
    sign = jnp.where(lower, 1, -1)
    pair = dims[2] * rows
    hid = ht.at[pl.ds(0, cols), pl.ds(0, hidden_width)]

    load = pltpu.make_async_copy(grad_ref, gall.at[pl.ds(me * rows, rows)], local.at[0])
    load.start()
    load_hidden = pltpu.make_async_copy(hidden_ref, hid, local.at[1])
    load_hidden.start()
    load_down = pltpu.make_async_copy(down_ref, down, local.at[2])
    load_down.start()

    barrier = pltpu.get_barrier_semaphore()
    for i in range(1, n):
        pl.semaphore_signal(barrier, inc=1, device_id={"expert": (me + i) % n}, device_id_type=MESH)
    pl.semaphore_signal(barrier, inc=1, device_id={"section": 1 - section}, device_id_type=MESH)
    pl.semaphore_wait(barrier, n)
    load.wait()

    def plane(mirrored):
        return jnp.where(lower, mirrored, dims[0] - 1 - mirrored)

    def number(rel):
        return near_index(plane(rel[0]), (y + rel[1]) % 2, (x + rel[2]) % 2, dims)

    def span(chunk):
        return sum(WIDTHS[:chunk]) * width // sum(WIDTHS), WIDTHS[chunk] * width // sum(WIDTHS)

    def piece(source, chunk):
        begin, size = span(chunk)
        return gall.at[pl.ds(source * rows, rows), pl.ds(begin, size)]

    def grad_copy(source, chunk, axis, step):
        target = [z, y, x]
        target[axis] = z + step * sign if axis == 0 else (target[axis] + 1) % 2
        block = piece(source, chunk)
        return pltpu.make_async_remote_copy(
            src_ref=block,
            dst_ref=block,
            send_sem=g_send.at[source, chunk, axis, (step + 1) // 2],
            recv_sem=g_recv.at[source, chunk],
            device_id={"expert": near_index(*target, dims)},
            device_id_type=MESH,
        )

    def hidden_copy(k):
        return pltpu.make_async_remote_copy(
            src_ref=hsend.at[pl.ds(k * cap, cap)],
            dst_ref=hgot.at[me],
            send_sem=h_send.at[k],
            recv_sem=h_recv.at[me],
            device_id={"expert": k},
            device_id_type=MESH,
        )

    def meta_copy(k):
        return pltpu.make_async_remote_copy(
            src_ref=meta.at[k],
            dst_ref=mgot.at[me],
            send_sem=m_send.at[k],
            recv_sem=m_recv.at[me],
            device_id={"expert": k},
            device_id_type=MESH,
        )

    def home_copy(k):
        return pltpu.make_async_remote_copy(
            src_ref=dsend.at[k],
            dst_ref=home.at[me],
            send_sem=d_send.at[k],
            recv_sem=d_recv.at[me],
            device_id={"expert": k},
            device_id_type=MESH,
        )

    def beside(src, dst, k):
        return pltpu.make_async_remote_copy(
            src_ref=src,
            dst_ref=dst,
            send_sem=s_send.at[k],
            recv_sem=s_recv.at[k],
            device_id={"section": 1 - section},
            device_id_type=MESH,
        )

    mine = gall.at[pl.ds(me * rows, rows)]

    def issue(event):
        if event[0] == OWN:
            grad_copy(me, event[1], event[2], event[3]).start()
        elif event[0] == ROWS:
            hidden_copy(number(event[1:])).start()
        else:
            source, chunk = number(event[1:4]), event[4]
            block = piece(source, chunk)
            if event[0] == GET:
                pltpu.make_async_copy(block, block, g_recv.at[source, chunk]).wait()
            else:
                grad_copy(source, chunk, event[5], event[6]).start()

    def events(segment):
        for kind in range(2):
            if SCHEDULE[kind][segment]:

                @pl.when(at_end if kind == 0 else jnp.logical_not(at_end))
                def _(kind=kind):
                    for event in SCHEDULE[kind][segment]:
                        issue(event)

    def tables():
        before = lax.broadcasted_iota(jnp.int32, (rows, rows), 0) < lax.broadcasted_iota(jnp.int32, (rows, rows), 1)
        score = scores_ref[...]
        route = routes_ref[...].astype(jnp.float32)
        total = jnp.sum(score, axis=0, keepdims=True)
        weight = score / total
        low = weight.astype(jnp.bfloat16).astype(jnp.float32)
        fix = weight / low
        expert = lax.broadcasted_iota(jnp.int32, (n, rows), 0).astype(jnp.float32)
        hit = [route[k : k + 1] == expert for k in range(top)]
        dense = lambda value: sum(jnp.where(hit[k], value[k : k + 1], 0.0) for k in range(top))
        named = dense(jnp.ones_like(route))
        rank = jnp.dot(
            named.astype(jnp.bfloat16),
            jnp.where(before, 1.0, 0.0).astype(jnp.bfloat16),
            preferred_element_type=jnp.float32,
        )
        score_dense = dense(score)
        stats[0] = score_dense
        stats[1] = dense(fix)
        stats[2] = score_dense / total
        place = jnp.where(named > 0.0, rank, -1.0)
        low_dense = dense(low)
        for e in range(n):
            meta[e, 0:1] = place[e : e + 1]
            meta[e, 1:2] = low_dense[e : e + 1]
        for k in range(top):
            slots[k : k + 1] = jnp.sum(jnp.where(hit[k], rank, 0.0), axis=0, keepdims=True)
        slots[top : 2 * top] = route

    def spread_rows():
        tables()
        load_hidden.wait()
        expand = jnp.where(
            lax.broadcasted_iota(jnp.int32, (rows, cols), 1) // top
            == lax.broadcasted_iota(jnp.int32, (rows, cols), 0),
            1.0,
            0.0,
        ).astype(jnp.bfloat16)
        wide = jnp.dot(slots[...].astype(jnp.bfloat16), expand, preferred_element_type=jnp.float32)
        lane = lax.broadcasted_iota(jnp.int32, (top, cols), 1) % top
        own = lane == lax.broadcasted_iota(jnp.int32, (top, cols), 0)
        slot = jnp.sum(jnp.where(own, wide[:top], 0.0), axis=0, keepdims=True)
        route = jnp.sum(jnp.where(own, wide[top:], 0.0), axis=0, keepdims=True)
        place = (route * cap + slot).astype(jnp.int32)
        block = 256 if (n * cap) % 256 == 0 else cap

        def one(b, _):
            begin = pl.multiple_of(b * block, block)
            want = lax.broadcasted_iota(jnp.int32, (block, cols), 0) + begin
            pick = jnp.where(want == place, 1.0, 0.0).astype(jnp.bfloat16)
            part = jnp.dot(pick, ht[:cols, :hidden_width], preferred_element_type=jnp.float32)
            hsend[pl.ds(begin, block), :] = part.astype(jnp.bfloat16)
            return 0

        lax.fori_loop(0, n * cap // block, one, 0)

    def keep_own():
        own = pltpu.make_async_copy(hsend.at[pl.ds(me * cap, cap)], hgot.at[me], local.at[3])
        own.start()
        own.wait()

    def group_base(group):
        table = GROUPS[0][group], GROUPS[1][group]
        zm = jnp.where(at_end, table[0][0], table[1][0])
        dy = jnp.where(at_end, table[0][1], table[1][1])
        zz = jnp.where(lower, zm, dims[0] - 1 - zm)
        return near_index(zz, (y + dy) % 2, 0, dims)

    def enlarge(group):
        first = group_base(group)
        for j in range(dims[2]):
            source = first + j

            @pl.when(source != me)
            def _(source=source):
                pltpu.make_async_copy(hgot.at[source], hgot.at[source], h_recv.at[source]).wait()
                pltpu.make_async_copy(mgot.at[source], mgot.at[source], m_recv.at[source]).wait()

            @pl.when(source == me)
            def _():
                mgot[me] = meta[me]

            info = mgot[source]
            want = lax.broadcasted_iota(jnp.int32, (cap, rows), 0).astype(jnp.float32)
            pick = jnp.where(want == info[0:1], info[1:2], 0.0).astype(jnp.bfloat16)
            full = lax.dot_general(
                hgot[source], pick, (((0,), (0,)), ((), ())), preferred_element_type=jnp.float32
            )
            ht[:, pl.ds(pl.multiple_of(source * rows, rows), rows)] = full.astype(jnp.bfloat16)

    def derive(group):
        first = group_base(group)
        begin = pl.multiple_of(first * rows, pair)
        block = 512

        def one(m, total):
            at = pl.multiple_of(m * block, block)
            projected = lax.dot_general(
                down[pl.ds(at, block), :],
                gall[pl.ds(begin, pair), :],
                (((1,), (1,)), ((), ())),
                preferred_element_type=jnp.float32,
            )
            held = ht[pl.ds(at, block), pl.ds(begin, pair)].astype(jnp.float32)
            return total + jnp.sum(projected * held, axis=0, keepdims=True)

        keep_derived(first, lax.fori_loop(0, hidden_width // block, one, jnp.zeros((1, pair), jnp.float32)))

    def derive_part(group, chunk, opening, closing):
        first = group_base(group)
        begin = pl.multiple_of(first * rows, pair)
        block = 512
        start, size = span(chunk)

        def one(m, total):
            at = pl.multiple_of(m * block, block)
            projected = lax.dot_general(
                down[pl.ds(at, block), pl.ds(start, size)],
                gall[pl.ds(begin, pair), pl.ds(start, size)],
                (((1,), (1,)), ((), ())),
                preferred_element_type=jnp.float32,
            )
            held = ht[pl.ds(at, block), pl.ds(begin, pair)].astype(jnp.float32)
            return total + jnp.sum(projected * held, axis=0, keepdims=True)

        total = lax.fori_loop(0, hidden_width // block, one, jnp.zeros((1, pair), jnp.float32))
        if not opening:
            total = total + dpart[group % 2]
        if closing:
            keep_derived(first, total)
        else:
            dpart[group % 2] = total

    def keep_derived(first, total):
        for j in range(dims[2]):
            dsend[first + j] = total[:, j * rows : (j + 1) * rows]

            @pl.when(first + j == me)
            def _(j=j):
                home[me] = total[:, j * rows : (j + 1) * rows]

    def send_home(group):
        first = group_base(group)
        for j in range(dims[2]):

            @pl.when(first + j != me)
            def _(source=first + j):
                home_copy(source).start()

    tile = stage.shape[2]
    layer = dims[1] * pair

    def plane_rows(p):
        zm = jnp.where(at_end, PLANES[0][p], PLANES[1][p])
        return pl.ds(pl.multiple_of(jnp.where(lower, zm, dims[0] - 1 - zm) * layer, layer), layer)

    def partial(p, column):
        return jnp.dot(ht[:, plane_rows(p)], gall[plane_rows(p), column], preferred_element_type=jnp.float32)

    def product(p, step):
        def one(j, _):
            column = pl.ds(pl.multiple_of((step * 2 + j) * tile, tile), tile)
            if p == 0:
                acc[:, column] = partial(p, column)
            else:
                acc[:, column] += partial(p, column)
            return 0

        lax.fori_loop(0, 2, one, 0)

    def weight_copy(j, step):
        column = pl.ds(pl.multiple_of((step * 2 + j) * tile, tile), tile)
        return pltpu.make_async_copy(stage.at[j], weight_ref.at[:, column], local.at[4 + j])

    def close(p, step, before):
        def one(j, _):
            column = pl.ds(pl.multiple_of((step * 2 + j) * tile, tile), tile)
            if before is not None:
                weight_copy(j, before).wait()
            stage[j] = (acc[:, column] + partial(p, column)).astype(stage.dtype)
            weight_copy(j, step).start()
            return 0

        lax.fori_loop(0, 2, one, 0)

    def logits():
        for i in range(1, n):
            source = (me + i) % n
            pltpu.make_async_copy(home.at[source], home.at[source], d_recv.at[source]).wait()
        weighted = home[:, 0, :] * stats[1]
        center = jnp.sum(weighted, axis=0, keepdims=True)
        logit[...] = (1.0 - stats[0]) * (weighted - stats[2] * center)
        beside(logit, next_logit, 2).start()

    beside(mine, next_grad, 0).start()
    beside(router_ref, next_router, 1).start()
    late = None
    closed = None
    for segment, op in enumerate(WORK):
        events(segment)
        if late is not None:
            send_home(late)
            late = None
        if op[0] == SPREAD:
            spread_rows()
        elif op[0] == KEEP:
            for i in range(1, n):
                meta_copy((me + i) % n).start()
            keep_own()
            load_down.wait()
        elif op[0] == EXPAND:
            enlarge(op[1])
        elif op[0] == DERIVE:
            derive(op[1])
            late = op[1]
        elif op[0] == PRODUCT:
            product(op[1], op[2])
        elif op[0] == CLOSE:
            close(op[1], op[2], closed)
            closed = op[2]
        elif op[0] == PART:
            derive_part(*op[1:])
            if op[4]:
                late = op[1]
        elif op[0] == LOGIT:
            logits()

    for i in range(1, n):
        k = (me + i) % n
        hidden_copy(k).wait_send()
        meta_copy(k).wait_send()
        home_copy(k).wait_send()
    for kind in range(2):

        @pl.when(at_end if kind == 0 else jnp.logical_not(at_end))
        def _(kind=kind):
            for segment in SCHEDULE[kind]:
                for event in segment:
                    if event[0] == OWN:
                        grad_copy(me, event[1], event[2], event[3]).wait_send()
                    elif event[0] == SEND:
                        grad_copy(number(event[1:4]), event[4], event[5], event[6]).wait_send()

    for j in range(2):
        weight_copy(j, closed).wait()
    beside(mine, next_grad, 0).wait()
    beside(router_ref, next_router, 1).wait()
    beside(logit, next_logit, 2).wait()


def relay(grad_rows, hidden_rows, routes, scores, down, router_rows, cap):
    n = router_rows.shape[0]
    n_tokens, width = grad_rows.shape
    top = routes.shape[0]
    entries, hidden_width = hidden_rows.shape
    dims = torus_dims(n)
    low = jnp.bfloat16
    any_space = pl.BlockSpec(memory_space=pl.ANY)
    vmem = pl.BlockSpec(memory_space=pltpu.VMEM)
    hbm = pl.BlockSpec(memory_space=pltpu.HBM)
    dma = pltpu.SemaphoreType.DMA
    return pl.pallas_call(
        functools.partial(relay_kernel, dims, cap),
        out_shape=(
            jax.ShapeDtypeStruct((hidden_width, width), low),
            jax.ShapeDtypeStruct((n_tokens, width), low),
            jax.ShapeDtypeStruct(router_rows.shape, low),
            jax.ShapeDtypeStruct((n, n_tokens), jnp.float32),
        ),
        in_specs=[hbm, hbm, vmem, vmem, hbm, hbm],
        out_specs=(any_space,) * 4,
        scratch_shapes=[
            pltpu.VMEM((n * n_tokens, width), low),
            pltpu.VMEM((hidden_width, width), low),
            pltpu.VMEM((n * cap, hidden_width), low),
            pltpu.VMEM((n, cap, hidden_width), low),
            pltpu.VMEM((n, 2, n_tokens), jnp.float32),
            pltpu.VMEM((n, 2, n_tokens), jnp.float32),
            pltpu.VMEM((2 * top, n_tokens), jnp.float32),
            pltpu.VMEM((3, n, n_tokens), jnp.float32),
            pltpu.VMEM((hidden_width, n * n_tokens), low),
            pltpu.VMEM((hidden_width, width), jnp.float32),
            pltpu.VMEM((2, hidden_width, 512), low),
            pltpu.VMEM((n, 1, n_tokens), jnp.float32),
            pltpu.VMEM((2, 1, dims[2] * n_tokens), jnp.float32),
            pltpu.VMEM((n, 1, n_tokens), jnp.float32),
            pltpu.VMEM((n, n_tokens), jnp.float32),
            dma((n, len(ORDERS), 3, 2)),
            dma((n, len(ORDERS))),
            dma((n,)),
            dma((n,)),
            dma((n,)),
            dma((n,)),
            dma((n,)),
            dma((n,)),
            dma((3,)),
            dma((3,)),
            dma((8,)),
        ],
        compiler_params=pltpu.CompilerParams(
            collective_id=1, has_side_effects=True, vmem_limit_bytes=RELAY_MIB * 1024 * 1024
        ),
        name="relay",
    )(grad_rows, hidden_rows, routes, scores, down, router_rows)


def settle_kernel(
    parts, weight_ref, grad_ref, router_ref, logit_ref, weight_out, handed_out, held, kept, rows, value, arrive, leave
):
    size = weight_ref.shape[0] // parts
    tile = grad_ref.shape[1] // parts
    small = [
        pltpu.make_async_copy(grad_ref, kept, arrive.at[parts]),
        pltpu.make_async_copy(router_ref, rows, arrive.at[parts + 1]),
        pltpu.make_async_copy(logit_ref, value, arrive.at[parts + 2]),
    ]
    first, second = [], []
    for i in range(parts):
        block = pl.ds(i * size, size)
        first.append(pltpu.make_async_copy(weight_ref.at[block], held.at[block], arrive.at[i]))
        second.append(pltpu.make_async_copy(held.at[block], weight_out.at[block], leave.at[i]))
    for copy in small + first:
        copy.start()
    for copy in small:
        copy.wait()
    rest = value[...]
    pieces = []
    for _ in range(3):
        pieces.append(rest.astype(jnp.bfloat16))
        rest = rest - pieces[-1].astype(jnp.float32)
    pieces = jnp.concatenate(pieces, axis=0)
    for i in range(parts):
        first[i].wait()
        second[i].start()
        column = pl.ds(i * tile, tile)
        extra = lax.dot_general(
            pieces,
            jnp.concatenate([rows[:, column]] * 3, axis=0),
            (((0,), (0,)), ((), ())),
            preferred_element_type=jnp.float32,
        )
        kept[:, column] = (kept[:, column].astype(jnp.float32) + extra).astype(kept.dtype)
    last = pltpu.make_async_copy(kept, handed_out, leave.at[parts])
    last.start()
    for copy in second:
        copy.wait()
    last.wait()


def settle(weight, next_grad, next_router, next_logit):
    parts = 8
    hbm = pl.BlockSpec(memory_space=pl.ANY)
    return pl.pallas_call(
        functools.partial(settle_kernel, parts),
        out_shape=(
            jax.ShapeDtypeStruct(weight.shape, weight.dtype),
            jax.ShapeDtypeStruct(next_grad.shape, next_grad.dtype),
        ),
        in_specs=[hbm] * 4,
        out_specs=(hbm,) * 2,
        scratch_shapes=[
            pltpu.VMEM(weight.shape, weight.dtype),
            pltpu.VMEM(next_grad.shape, next_grad.dtype),
            pltpu.VMEM(next_router.shape, next_router.dtype),
            pltpu.VMEM(next_logit.shape, next_logit.dtype),
            pltpu.SemaphoreType.DMA((parts + 3,)),
            pltpu.SemaphoreType.DMA((parts + 1,)),
        ],
        compiler_params=pltpu.CompilerParams(vmem_limit_bytes=SETTLE_MIB * 1024 * 1024),
        name="settle",
    )(weight, next_grad, next_router, next_logit)


def close_body(grad_out, saved_hidden, routes, scores, down_weight, router):
    grad_rows = grad_out[0]
    hidden_rows = saved_hidden[0]
    n_tokens, top, hidden_width = hidden_rows.shape
    n = router.shape[1]
    cap = 3 * n_tokens * top // (2 * n)
    results = relay(
        grad_rows,
        hidden_rows.reshape(n_tokens * top, hidden_width),
        routes[0].T,
        scores[0].T,
        down_weight[0, 0],
        router[0],
        cap,
    )
    weight_out, handed = settle(*results)
    return (weight_out[None, None], handed[None])


def passed_along(array, axis, by):
    size = lax.axis_size(axis)
    return lax.ppermute(array, axis, [(i, (i + by) % size) for i in range(size)])


def body(grad_out, saved_hidden, routes, scores, down_weight, router):
    grad_rows = grad_out[0]
    hidden_rows = saved_hidden[0]
    route_ids = routes[0]
    score_rows = scores[0]
    n_tokens = grad_rows.shape[0]
    n_experts = router.shape[1]
    score_total = jnp.sum(score_rows, axis=1, keepdims=True)
    weights = score_rows / score_total
    weights_low = weights.astype(jnp.bfloat16)

    next_grad = passed_along(grad_rows, "section", -1)
    next_router = passed_along(router[0], "section", -1)
    dense = spread(hidden_rows, weights_low, route_ids, n_experts)
    grads, hidden = exchange(grad_rows, dense)
    derivs = derivs_of(grads, hidden, down_weight[0, 0])
    home = lax.all_to_all(
        derivs.reshape(n_experts, n_tokens), "expert", split_axis=0, concat_axis=0, tiled=True
    )
    weight_out = lax.dot_general(
        hidden, grads, (((0,), (0,)), ((), ())), preferred_element_type=jnp.float32
    ).astype(jnp.bfloat16)

    named = route_ids.T[None] == jnp.arange(n_experts, dtype=jnp.int32)[:, None, None]
    low = weights_low.astype(jnp.float32)
    score_dense = jnp.sum(jnp.where(named, score_rows.T[None], 0.0), axis=1)
    fix_dense = jnp.sum(jnp.where(named, (weights / low).T[None], 0.0), axis=1)
    weighted = home * fix_dense
    center = jnp.sum(weighted, axis=0, keepdims=True)
    total_row = score_total.T
    logit_dense = (1.0 - score_dense) * (weighted - score_dense / total_row * center)
    next_logit = passed_along(logit_dense, "section", -1)
    handed = next_grad.astype(jnp.float32) + lax.dot_general(
        next_logit,
        next_router.astype(jnp.float32),
        (((0,), (0,)), ((), ())),
        precision=lax.Precision.HIGHEST,
    )
    return (weight_out[None, None], handed.astype(jnp.bfloat16)[None])


def solution(mesh):
    close = mesh.shape["section"] == 2 and torus_dims(mesh.shape["expert"]) == SHAPE
    return jax.shard_map(
        close_body if close else body,
        mesh=mesh,
        in_specs=(
            P("section", "expert", None),
            P("section", "expert", None, None),
            P("section", "expert", None),
            P("section", "expert", None),
            P("section", "expert", None, None),
            P("section", None, None),
        ),
        out_specs=(P("section", "expert", None, None), P("section", "expert", None)),
        check_vma=False,
    )
```
